128 devices in a mesh: tok: 64 (over z, y, x_hi, core), lay: 2 (over x_lo).
Axes of the slice: x: 4 (x_hi: 2, x_lo: 2; x = x_hi * 2 + x_lo), y: 4, z: 4, core: 2. Of those that a mesh axis runs over, the one named last changes fastest.
Arguments:
- first_acts: bfloat16 [2, 16384, 5120], P('lay', 'tok'), may hold values from -40 to 40
- second_acts: bfloat16 [2, 16384, 5120], P('lay', 'tok'), may hold values from -40 to 40
Outputs:
- whitening: float32 [2, 2, 40, 128, 128], P(None, 'lay')
- similarity: float32 [2, 2, 40], P('lay')
The draws below stay inside these ranges and needn't reach their ends.
All inputs are finite; a program needn't handle non-finite values.
Results may differ from the reference program's by a relative error of at most 0.0003.
Values may be sent and summed in bfloat16 or wider, within the bound.
A program may use at most 128 MiB of HBM per device.

```python
import math
import jax
import jax.numpy as jnp
from jax import lax

HEADS = 40
HEAD_DIM = 128
D = 5120
ITERS = 6
LAYERS = 2
TOKENS = 16384


def residual_layers(key):
    row_position = jnp.arange(TOKENS, dtype=jnp.float32) / TOKENS
    row_jitter = jax.random.uniform(jax.random.fold_in(key, 11), (TOKENS,), jnp.float32, -0.35, 0.35)
    row_scale = jnp.exp(math.log(3.0) * row_position + row_jitter)
    mixing = jnp.eye(HEAD_DIM, dtype=jnp.float32) + 0.8 / math.sqrt(HEAD_DIM) * jax.random.normal(jax.random.fold_in(key, 12), (HEADS, HEAD_DIM, HEAD_DIM), jnp.float32)
    stream = jnp.zeros((TOKENS, D), jnp.float32)
    first_list = []
    second_list = []
    for layer_idx in range(LAYERS):
        layer_key = jax.random.fold_in(key, 1000 + layer_idx)
        update = jax.random.normal(jax.random.fold_in(layer_key, 1), (TOKENS, D), jnp.float32)
        noise_part = jax.random.normal(jax.random.fold_in(layer_key, 3), (TOKENS, D), jnp.float32)
        chan_low = 0.3
        chan_high = 3.0
        stream = 0.8 * stream + 0.6 * update
        mixed_stream = jnp.einsum('thi,hij->thj', stream.reshape(TOKENS, HEADS, HEAD_DIM), mixing, precision=lax.Precision.HIGHEST).reshape(TOKENS, D)
        chan_first = jnp.exp(jax.random.uniform(jax.random.fold_in(layer_key, 4), (D,), jnp.float32, math.log(chan_low), math.log(chan_high)))
        chan_second = chan_first * jnp.exp(jax.random.uniform(jax.random.fold_in(layer_key, 5), (D,), jnp.float32, -0.35, 0.35))
        offset_first = 0.8 * jax.random.normal(jax.random.fold_in(layer_key, 6), (D,), jnp.float32)
        offset_second = offset_first + 0.3 * jax.random.normal(jax.random.fold_in(layer_key, 7), (D,), jnp.float32)
        first_layer = row_scale[:, None] * (chan_first * mixed_stream + offset_first)
        second_layer = row_scale[:, None] * (chan_second * (0.75 * mixed_stream + 0.66 * noise_part) + offset_second)
        first_list.append(jnp.clip(first_layer, -40.0, 40.0))
        second_list.append(jnp.clip(second_layer, -40.0, 40.0))
    return (jnp.stack(first_list), jnp.stack(second_list))


def draw_first_acts(key, part):
    return residual_layers(key)[0].astype(jnp.bfloat16)


def draw_second_acts(key, part):
    return residual_layers(key)[1].astype(jnp.bfloat16)


def setup_inputs(seed: int = 0) -> dict:
    arg_keys = jax.random.split(jax.random.key(seed), 3)
    return {
        "first_acts": draw_first_acts(jax.random.fold_in(arg_keys[2], 71), 0),
        "second_acts": draw_second_acts(jax.random.fold_in(arg_keys[2], 71), 0),
    }


ridge_weight = 0.05
top_precision = lax.Precision.HIGHEST

def newton_whiten(matrices):
    unit_matrix = jnp.eye(HEAD_DIM, dtype=jnp.float32)
    scale_norm = jnp.sqrt(lax.optimization_barrier(jnp.sum(matrices * matrices, axis=(-2, -1), keepdims=True)))
    square_iter = matrices / scale_norm
    inverse_iter = jnp.broadcast_to(unit_matrix, matrices.shape)
    for sweep_index in range(ITERS):
        factor_iter = 1.5 * unit_matrix - 0.5 * jnp.matmul(inverse_iter, square_iter, precision=top_precision)
        square_iter = jnp.matmul(square_iter, factor_iter, precision=top_precision)
        inverse_iter = jnp.matmul(factor_iter, inverse_iter, precision=top_precision)
    return inverse_iter / jnp.sqrt(scale_norm)

def covariance(gram_total, col_sums, token_total):
    unit_matrix = jnp.eye(HEAD_DIM, dtype=jnp.float32)
    column_mean = col_sums / token_total
    return gram_total / token_total - column_mean[..., :, None] * column_mean[..., None, :] + ridge_weight * unit_matrix

def head_view(act_block):
    return act_block.astype(jnp.float32).reshape(TOKENS, HEADS, HEAD_DIM)

def reference(first_acts, second_acts):
    gram_list = []
    sums_list = []
    for checkpoint in (first_acts, second_acts):
        for layer_idx in range(LAYERS):
            viewed = head_view(checkpoint[layer_idx])
            gram_list.append(jnp.einsum('thi,thj->hij', viewed, viewed, precision=top_precision))
            sums_list.append(lax.optimization_barrier(jnp.sum(viewed, axis=0)))
    gram_total = jnp.stack(gram_list).reshape(2, LAYERS, HEADS, HEAD_DIM, HEAD_DIM)
    col_sums = jnp.stack(sums_list).reshape(2, LAYERS, HEADS, HEAD_DIM)
    whitening = newton_whiten(covariance(gram_total, col_sums, TOKENS))
    column_mean = col_sums / TOKENS
    rows_out = []
    for first_idx in range(LAYERS):
        view_first = head_view(first_acts[first_idx])
        row_items = []
        for second_idx in range(LAYERS):
            view_second = head_view(second_acts[second_idx])
            cross_cov = jnp.einsum('thi,thj->hij', view_first, view_second, precision=top_precision) / TOKENS
            cross_cov = cross_cov - column_mean[0, first_idx][:, :, None] * column_mean[1, second_idx][:, None, :]
            left_product = jnp.matmul(whitening[0, first_idx], cross_cov, precision=top_precision)
            whitened = jnp.matmul(left_product, whitening[1, second_idx], precision=top_precision)
            row_items.append(lax.optimization_barrier(jnp.sum(whitened * whitened, axis=(-2, -1))) / HEAD_DIM)
        rows_out.append(jnp.stack(row_items))
    return (whitening, jnp.stack(rows_out))
```

```python
import functools

import jax
import jax.numpy as jnp
from jax import lax
from jax.experimental import pallas as pl
from jax.experimental.pallas import tpu as pltpu
from jax.sharding import PartitionSpec as P

HEADS = 40
HD = 128
ITERS = 6
RIDGE = 0.05
HALF = HEADS // 2
PARTS = 4
PART_HEADS = HEADS // PARTS
F32 = jnp.float32
HI = lax.Precision.HIGHEST
MESH = pl.DeviceIdType.MESH

CHAINS = {
    "pa": (72, "z"),
    "pb": (64, "y"),
    "ca": (64, "z"),
    "cb": (64, "y"),
    "da": (64, "z"),
    "db": (64, "y"),
}
GATHERS = {"wa": (72, "z"), "wb": (64, "y"), "sa": (8, "z")}


def iota(shape, dim):
    return lax.broadcasted_iota(jnp.int32, shape, dim)


def dot_t(a, b, precision=None):
    return lax.dot_general(
        a, b, (((0,), (0,)), ((), ())), precision=precision, preferred_element_type=F32
    )


def mm(a, b):
    return jnp.dot(a, b, precision=HI, preferred_element_type=F32)


def kernel(tokens, names, *refs):
    r = dict(zip(names, refs))
    tok = lax.axis_index("tok")
    lay = lax.axis_index("lay")
    c = tok % 2
    xh = (tok // 2) % 2
    y = (tok // 4) % 4
    z = tok // 16

    def dev(z_, y_, xh_, c_):
        return (((z_ * 4 + y_) * 2 + xh_) * 2 + c_, lay)

    def dev_uv(axis, u, v, xh_):
        return dev(u, v, xh_, c) if axis == "z" else dev(v, u, xh_, c)

    def uv(axis):
        return (z, y) if axis == "z" else (y, z)

    sibling = dev(z, y, xh, 1 - c)
    twin = (tok, 1 - lay)

    owner = jnp.logical_or(xh == (z + y) % 2, jnp.logical_and(z == y, xh == 1))

    def own_slot(axis):
        u, v = uv(axis)
        return jnp.where(xh == (z + y) % 2, v, 4)

    def slot_owner(axis, s):
        u, _ = uv(axis)
        vo = s if s < 4 else u
        xo = (u + vo) % 2 if s < 4 else 1
        return u, vo, xo

    def rcopy(src, dst, ssem, rsem, device):
        return pltpu.make_async_remote_copy(
            src_ref=src, dst_ref=dst, send_sem=ssem, recv_sem=rsem,
            device_id=device, device_id_type=MESH,
        )

    pending = []

    def launch(copy):
        copy.start()
        pending.append(copy)
        return copy

    def s1(name):
        q = lambda k: r[name + k]
        return rcopy(q("").at[1 - c], q("_r1"), q("_s").at[0], q("_q").at[0], sibling)

    def s1_sum(name):
        buf, r1 = r[name], r[name + "_r1"]
        s1(name).wait_recv()

        def body(i, carry):
            for s in range(5):
                buf[c, i, s] = buf[c, i, s] + r1[i, s]
            return carry

        lax.fori_loop(0, 4, body, 0)

    def s2(name, d):
        axis = CHAINS[name][1]
        u, v = uv(axis)
        to = (u + d) % 4
        q = lambda k: r[name + k]
        return rcopy(
            q("").at[c, to], q("_r2").at[d - 1], q("_s").at[d], q("_q").at[d],
            dev_uv(axis, to, v, xh),
        )

    def s2_sum(name):
        axis = CHAINS[name][1]
        u, _ = uv(axis)
        buf, r2, acc = r[name], r[name + "_r2"], r[name + "_acc"]
        for d in (1, 2, 3):
            s2(name, d).wait_recv()
        for s in range(5):
            acc[s] = (buf[c, u, s] + r2[0, s]) + (r2[1, s] + r2[2, s])

    def s3(name, s):
        axis = CHAINS[name][1]
        u, v = uv(axis)
        _, vo, xo = slot_owner(axis, s)
        slot = ((v - vo + 4) % 4) * 2 + (xh + xo) % 2
        mine = jnp.logical_and(v == vo, xh == xo)
        q = lambda k: r[name + k]
        copy = rcopy(
            q("_acc").at[s], q("_r3").at[slot], q("_s").at[4 + s], q("_q").at[4 + slot],
            dev_uv(axis, u, vo, xo),
        )
        return mine, copy

    def s3_start(name):
        for s in range(5):
            mine, copy = s3(name, s)

            @pl.when(jnp.logical_not(mine))
            def _():
                copy.start()

    def s3_total(name):
        axis = CHAINS[name][1]
        r3 = r[name + "_r3"]
        total = r[name + "_acc"][own_slot(axis)]
        for slot in range(1, 8):
            rcopy(r3.at[slot], r3.at[slot], r[name + "_s"].at[0], r[name + "_q"].at[4 + slot], twin).wait_recv()
        for slot in range(1, 8):
            total = total + r3[slot]
        return total

    def s3_drain(name):
        for s in range(5):
            mine, copy = s3(name, s)

            @pl.when(jnp.logical_not(mine))
            def _():
                copy.wait_send()

    def g1(name, i):
        axis = GATHERS[name][1]
        u, v = uv(axis)
        mine = own_slot(axis)
        place = r[name].at[c, u, mine]
        return rcopy(
            place, place, r[name + "_s"].at[i], r[name + "_q"].at[mine],
            dev_uv(axis, u, (v + i // 2) % 4, (xh + i % 2) % 2),
        )

    def g1_start(name):
        for i in range(1, 8):
            g1(name, i).start()

    def g1_wait(name):
        axis = GATHERS[name][1]
        u, _ = uv(axis)
        for s in range(5):
            place = r[name].at[c, u, s]

            @pl.when(jnp.logical_not(jnp.logical_and(owner, own_slot(axis) == s)))
            def _():
                rcopy(place, place, r[name + "_s"].at[0], r[name + "_q"].at[s], twin).wait_recv()

    def g2(name, d):
        axis = GATHERS[name][1]
        u, v = uv(axis)
        place = r[name].at[c, u]
        return rcopy(
            place, place, r[name + "_s"].at[7 + d], r[name + "_q"].at[4 + d],
            dev_uv(axis, (u + d) % 4, v, xh),
        )

    def g3(name):
        place = r[name].at[c]
        return rcopy(place, place, r[name + "_s"].at[11], r[name + "_q"].at[8], sibling)

    def exchange(e):
        cols = pl.ds(e * PART_HEADS * HD, PART_HEADS * HD)
        return rcopy(
            r["x2_hbm"].at[0, :, cols], r["x2o"].at[:, cols],
            r["x_s"].at[e], r["x_q"].at[e], twin,
        )

    barrier = pltpu.get_barrier_semaphore()
    peers = [sibling, twin]
    for i in range(1, 8):
        peers.append(dev(z, (y + i // 2) % 4, (xh + i % 2) % 2, c))
    for i in range(2, 8):
        peers.append(dev((z + i // 2) % 4, y, (xh + i % 2) % 2, c))
    for peer in peers:
        pl.semaphore_signal(barrier, inc=1, device_id=peer, device_id_type=MESH)
    load1 = pltpu.make_async_copy(r["x1_hbm"].at[0], r["x1"], r["l_s"].at[0])
    load2 = pltpu.make_async_copy(r["x2_hbm"].at[0], r["x2"], r["l_s"].at[1])
    load1.start()
    load2.start()
    pl.semaphore_wait(barrier, len(peers))

    launch(exchange(0))
    launch(exchange(1))
    load1.wait()
    load2.wait()

    ri = iota((HD, HD), 0)
    ci = iota((HD, HD), 1)
    row8 = iota((8, HD), 0)
    upper = ri <= ci
    diag = ri == ci
    eye = jnp.where(diag, 1.0, 0.0).astype(F32)
    x1, x2, x2o = r["x1"], r["x2"], r["x2o"]

    def places(h):
        k = h % HALF
        main = k < 16
        return (
            h // HALF,
            k % 4,
            k // 4,
            jnp.where(main, k // 4, k % 4),
            jnp.where(main, k % 4, 4),
        )

    def gram(h):
        ch, zz, ss, yy, rr = places(h)
        cols = pl.ds(pl.multiple_of(h * HD, HD), HD)
        ab = jnp.concatenate([x1[:, cols], x2[:, cols]], axis=1)
        g = dot_t(ab, ab)
        sums = jnp.dot(jnp.ones((8, ab.shape[0]), ab.dtype), ab, preferred_element_type=F32)
        g1_, cr, g2_ = g[:HD, :HD], g[:HD, HD:], g[HD:, HD:]
        p = jnp.where(upper, g1_, g2_)
        dg = jnp.sum(jnp.where(diag, g2_, 0.0), axis=0, keepdims=True)
        aux = jnp.where(
            row8 == 0, sums[:, :HD],
            jnp.where(row8 == 1, sums[:, HD:], jnp.where(row8 == 2, jnp.broadcast_to(dg, (8, HD)), 0.0)),
        )
        r["pa"][ch, zz, ss, 0:64] = p[:64]
        r["pa"][ch, zz, ss, 64:72] = aux
        r["pb"][ch, yy, rr] = p[64:]
        r["ca"][ch, zz, ss] = cr[:64]
        r["cb"][ch, yy, rr] = cr[64:]

    def loop(lo, n, body):
        def step(i, carry):
            body(lo + i)
            return carry

        lax.fori_loop(0, n, step, 0)

    loop((1 - c) * HALF, HALF, gram)
    for name in ("pa", "pb", "ca", "cb"):
        launch(s1(name))
    loop(c * HALF, HALF, gram)
    for name in ("pa", "pb", "ca", "cb"):
        s1_sum(name)
        for d in (1, 3, 2):
            launch(s2(name, d))
    for name in ("pa", "pb"):
        s2_sum(name)
        s3_start(name)
    launch(exchange(2))

    def unpack(top, low, aux):
        p = jnp.concatenate([top, low], axis=0)
        pt = p.T
        first = jnp.where(upper, p, pt)
        second = jnp.where(upper, jnp.where(diag, aux[2:3, :], pt), p)
        return first, second

    def only_row0(row):
        return jnp.where(row8 == 0, jnp.broadcast_to(row, (8, HD)), 0.0)

    @pl.when(owner)
    def _():
        top = s3_total("pa")
        low = s3_total("pb")
        aux = top[64:72]
        grams = unpack(top[:64], low, aux)
        ys, zs, scales = [], [], []
        for n in (0, 1):
            mean = only_row0(aux[n : n + 1, :]) / tokens
            cov = grams[n] / tokens - dot_t(mean, mean, HI) + RIDGE * eye
            sq = jnp.sum(jnp.sum(cov * cov, axis=1, keepdims=True), axis=0, keepdims=True)
            scale = jnp.sqrt(sq)
            scales.append(scale)
            ys.append(cov / scale)
        for it in range(ITERS):
            for n in (0, 1):
                if it == 0:
                    f = 1.5 * eye - 0.5 * ys[n]
                    zs.append(f)
                else:
                    f = 1.5 * eye - 0.5 * mm(zs[n], ys[n])
                    zs[n] = mm(f, zs[n])
                if it < ITERS - 1:
                    ys[n] = mm(ys[n], f)
        w1 = zs[0] / jnp.sqrt(scales[0])
        w2 = zs[1] / jnp.sqrt(scales[1])
        wp = jnp.where(upper, w1, w2)
        wd = jnp.sum(jnp.where(diag, w2, 0.0), axis=0, keepdims=True)
        slot_z, slot_y = own_slot("z"), own_slot("y")
        r["wa"][c, z, slot_z, 0:64] = wp[:64]
        r["wa"][c, z, slot_z, 64:72] = jnp.broadcast_to(wd, (8, HD))
        r["wb"][c, y, slot_y] = wp[64:]
        r["w12"][0] = w1
        r["w12"][1] = w2
        r["aux"][...] = aux
        r["w_out_x"][0:HD] = w2
        r["w_out_x"][HD : HD + 8] = aux
        g1_start("wa")
        g1_start("wb")
        rcopy(r["w_out_x"], r["w_in_x"], r["y_s"].at[0], r["y_q"].at[0], twin).start()

    launch(exchange(3))
    for name in ("ca", "cb"):
        s2_sum(name)
        s3_start(name)
    for name in ("wa", "wb"):
        g1_wait(name)
        for d in (1, 3, 2):
            launch(g2(name, d))

    def cross(h):
        ch, zz, ss, yy, rr = places(h)
        cols = pl.ds(pl.multiple_of(h * HD, HD), HD)
        cr = dot_t(x1[:, cols], x2o[:, cols])
        r["da"][ch, zz, ss] = cr[:64]
        r["db"][ch, yy, rr] = cr[64:]

    for e in range(2):
        exchange(e).wait_recv()
        loop(e * PART_HEADS, PART_HEADS, cross)
    for name in ("wa", "wb"):
        for d in (1, 3, 2):
            g2(name, d).wait_recv()
        launch(g3(name))
    for e in range(2, PARTS):
        exchange(e).wait_recv()
        loop(e * PART_HEADS, PART_HEADS, cross)
    for name in ("da", "db"):
        launch(s1(name))
    for name in ("da", "db"):
        s1_sum(name)
        for d in (1, 3, 2):
            launch(s2(name, d))

    for name in ("wa", "wb"):
        g3(name).wait_recv()

    def emit(h):
        ch, zz, ss, yy, rr = places(h)
        w1, w2 = unpack(r["wa"][ch, zz, ss, 0:64], r["wb"][ch, yy, rr], r["wa"][ch, zz, ss, 64:72])
        r["w_ref"][0, 0, h] = w1
        r["w_ref"][1, 0, h] = w2

    loop(0, HEADS, emit)

    for name in ("da", "db"):
        s2_sum(name)
        s3_start(name)

    @pl.when(owner)
    def _():
        own = jnp.concatenate([s3_total("ca"), s3_total("cb")], axis=0)
        rcopy(r["w_out_x"], r["w_in_x"], r["y_s"].at[0], r["y_q"].at[0], twin).wait()
        other = jnp.concatenate([s3_total("da"), s3_total("db")], axis=0)
        aux = r["aux"][...]
        mean1 = only_row0(aux[0:1, :]) / tokens
        sims = []
        for raw, sums, w2 in (
            (own, aux[1:2, :], r["w12"][1]),
            (other, r["w_in_x"][HD + 1 : HD + 2], r["w_in_x"][0:HD]),
        ):
            cov = raw / tokens - dot_t(mean1, only_row0(sums) / tokens, HI)
            white = mm(mm(r["w12"][0], cov), w2)
            sq = jnp.sum(jnp.sum(white * white, axis=1, keepdims=True), axis=0, keepdims=True)
            sims.append(sq / HD)
        k = jnp.where(own_slot("z") < 4, 4 * own_slot("z") + z, 16 + z)
        here = iota((8, HD), 1) == c * HALF + k
        tile = jnp.where(row8 == lay, jnp.broadcast_to(sims[0], (8, HD)), 0.0)
        tile = jnp.where(row8 == 1 - lay, jnp.broadcast_to(sims[1], (8, HD)), tile)
        r["sa"][c, z, own_slot("z")] = jnp.where(here, tile, 0.0)
        g1_start("sa")

    g1_wait("sa")
    for d in (1, 3, 2):
        launch(g2("sa", d))
    for d in (1, 2, 3):
        g2("sa", d).wait_recv()
    launch(g3("sa"))
    g3("sa").wait_recv()
    total = jnp.zeros((8, HD), F32)
    for ch in range(2):
        for i in range(4):
            for s in range(5):
                total = total + r["sa"][ch, i, s]
    r["s_ref"][0] = total[0:2, 0:HEADS]

    for copy in pending:
        copy.wait_send()
    for name in CHAINS:
        s3_drain(name)

    @pl.when(owner)
    def _():
        for name in GATHERS:
            for i in range(1, 8):
                g1(name, i).wait_send()


def local(tokens, first_acts, second_acts):
    rows, width = first_acts.shape[1:]
    names = ["x1_hbm", "x2_hbm", "w_ref", "s_ref"]
    scratch = []

    def add(name, spec):
        names.append(name)
        scratch.append(spec)

    dma = lambda n: pltpu.SemaphoreType.DMA((n,))
    for name in ("x1", "x2", "x2o"):
        add(name, pltpu.VMEM((rows, width), first_acts.dtype))
    for name, (n, _) in CHAINS.items():
        add(name, pltpu.VMEM((2, 4, 5, n, HD), F32))
        add(name + "_r1", pltpu.VMEM((4, 5, n, HD), F32))
        add(name + "_r2", pltpu.VMEM((3, 5, n, HD), F32))
        add(name + "_acc", pltpu.VMEM((5, n, HD), F32))
        add(name + "_r3", pltpu.VMEM((8, n, HD), F32))
        add(name + "_s", dma(9))
        add(name + "_q", dma(12))
    for name, (n, _) in GATHERS.items():
        add(name, pltpu.VMEM((2, 4, 5, n, HD), F32))
        add(name + "_s", dma(12))
        add(name + "_q", dma(9))
    add("w12", pltpu.VMEM((2, HD, HD), F32))
    add("aux", pltpu.VMEM((8, HD), F32))
    add("w_out_x", pltpu.VMEM((HD + 8, HD), F32))
    add("w_in_x", pltpu.VMEM((HD + 8, HD), F32))
    add("l_s", dma(2))
    add("x_s", dma(PARTS))
    add("x_q", dma(PARTS))
    add("y_s", dma(1))
    add("y_q", dma(1))
    return pl.pallas_call(
        functools.partial(kernel, tokens, names),
        out_shape=(
            jax.ShapeDtypeStruct((2, 1, HEADS, HD, HD), F32),
            jax.ShapeDtypeStruct((1, 2, HEADS), F32),
        ),
        in_specs=[pl.BlockSpec(memory_space=pl.ANY)] * 2,
        out_specs=(
            pl.BlockSpec(memory_space=pltpu.VMEM),
            pl.BlockSpec(memory_space=pltpu.VMEM),
        ),
        scratch_shapes=scratch,
        compiler_params=pltpu.CompilerParams(collective_id=0, has_side_effects=True),
    )(first_acts, second_acts)


def solution(mesh):
    def whole(first_acts, second_acts):
        tokens = first_acts.shape[1] * lax.axis_size("tok")
        return local(tokens, first_acts, second_acts)

    in_specs = (P("lay", "tok", None), P("lay", "tok", None))
    out_specs = (P(None, "lay", None, None, None), P("lay", None, None))
    return jax.shard_map(whole, mesh=mesh, in_specs=in_specs, out_specs=out_specs, check_vma=False)
```

```python
import functools

import jax
import jax.numpy as jnp
from jax import lax
from jax.experimental import pallas as pl
from jax.experimental.pallas import tpu as pltpu
from jax.sharding import PartitionSpec as P

HEADS = 40
HD = 128
ITERS = 6
RIDGE = 0.05
HALF = HEADS // 2
PARTS = 5
FROM_HBM = 3
BATCHES = (14, 19, 27)
VMEM_LIMIT = 48 * 2**20
F32 = jnp.float32
HI = lax.Precision.HIGHEST
MESH = pl.DeviceIdType.MESH

CHAINS = {"pa": (72, "z"), "pb": (64, "y"), "ca": (64, "z"), "cb": (64, "y")}
LATE = {"da": "z", "db": "y"}
GATHERS = {"wa": (72, "z"), "wb": (64, "y")}


def iota(shape, dim):
    return lax.broadcasted_iota(jnp.int32, shape, dim)


def dot_t(a, b, precision=None):
    return lax.dot_general(
        a, b, (((0,), (0,)), ((), ())), precision=precision, preferred_element_type=F32
    )


def mm(a, b):
    return jnp.dot(a, b, precision=HI, preferred_element_type=F32)


def masks():
    ri, ci = iota((HD, HD), 0), iota((HD, HD), 1)
    return ri <= ci, ri == ci


def unpack(top, low, aux):
    upper, diag = masks()
    p = jnp.concatenate([top, low], axis=0)
    pt = p.T
    first = jnp.where(upper, p, pt)
    second = jnp.where(upper, jnp.where(diag, aux[2:3, :], pt), p)
    return first, second


def head_of(z, p):
    k = 4 * ((z + p) % 4) + z
    if isinstance(p, int):
        return 16 + z if p == 4 else k
    return jnp.where(p == 4, 16 + z, k)


def places(h):
    k = h % HALF
    z = k % 4
    y = jnp.where(k < 16, k // 4, z)
    p = jnp.where(k < 16, (k // 4 - z + 4) % 4, 4)
    return h // HALF, z, y, p


def kernel(tokens, names, *refs):
    r = dict(zip(names, refs))
    tok = lax.axis_index("tok")
    lay = lax.axis_index("lay")
    c = tok % 2
    xh = (tok // 2) % 2
    y = (tok // 4) % 4
    z = tok // 16

    def dev(z_, y_, xh_, c_):
        return (((z_ * 4 + y_) * 2 + xh_) * 2 + c_, lay)

    def uv(axis):
        return (z, y) if axis == "z" else (y, z)

    def dev_uv(axis, u, v, xh_):
        return dev(u, v, xh_, c) if axis == "z" else dev(v, u, xh_, c)

    sibling = dev(z, y, xh, 1 - c)
    twin = (tok, 1 - lay)
    far = dev(z, y, 1 - xh, c)

    on_diag = z == y
    main = (y - z + 4) % 4
    owns_main = xh == main % 2
    owner = jnp.logical_or(owns_main, on_diag)
    own = jnp.where(owns_main, main, 4)
    late_owner = jnp.logical_and(on_diag, xh == 1)
    early_owner = owns_main
    extra_mine = jnp.where(owns_main, 0, 1)
    extra_give = jnp.where(owns_main, 1, 0)
    gives = jnp.logical_or(on_diag, jnp.logical_not(owns_main))
    no = jnp.logical_not

    def target(axis, p):
        u, _ = uv(axis)
        if p == 4:
            return u
        return (u + p) % 4 if axis == "z" else (u - p + 4) % 4

    def rcopy(src, dst, ssem, rsem, device):
        return pltpu.make_async_remote_copy(
            src_ref=src, dst_ref=dst, send_sem=ssem, recv_sem=rsem,
            device_id=device, device_id_type=MESH,
        )

    pending = []

    def launch(copy, cond=None):
        pending.append((cond, copy))
        if cond is None:
            copy.start()
        else:
            pl.when(cond)(lambda: copy.start())

    def arrive(ref, sem, cond=None):
        copy = rcopy(ref, ref, r["none"].at[0], sem, twin)
        if cond is None:
            copy.wait_recv()
        else:
            pl.when(cond)(lambda: copy.wait_recv())

    def loop(n, body, unroll=1):
        def step(i, carry):
            body(i)
            return carry

        lax.fori_loop(0, n, step, 0, unroll=unroll)

    def s1(name):
        launch(rcopy(r[name].at[1 - c], r[name + "_r1"], r[name + "_s"].at[0], r[name + "_q"].at[0], sibling))

    def s1_sum(name):
        buf, r1 = r[name], r[name + "_r1"]
        arrive(r1, r[name + "_q"].at[0])

        def body(i):
            for s in range(5):
                buf[c, i, s] = buf[c, i, s] + r1[i, s]

        loop(4, body)

    def s2(name):
        axis = CHAINS[name][1]
        u, v = uv(axis)
        for d in (1, 3, 2):
            to = (u + d) % 4
            launch(
                rcopy(
                    r[name].at[c, to], r[name + "_r2"].at[d - 1], r[name + "_s"].at[d],
                    r[name + "_q"].at[d], dev_uv(axis, to, v, xh),
                )
            )

    def s2_sum(name):
        u, _ = uv(CHAINS[name][1])
        buf, r2, acc = r[name], r[name + "_r2"], r[name + "_acc"]
        for d in (1, 2, 3):
            arrive(r2.at[d - 1], r[name + "_q"].at[d])
        for s in range(5):
            acc[s] = (buf[c, u, s] + r2[0, s]) + (r2[1, s] + r2[2, s])

    def s3(name, axis, slots):
        u, v = uv(axis)
        for p in slots:
            vo = target(axis, p)
            off = jnp.maximum((v - vo + 4) % 4, 1) - 1
            kind = p // 4
            launch(
                rcopy(
                    r[name + "_acc"].at[p], r[name + "_r3"].at[kind, off], r[name + "_s"].at[4 + p],
                    r[name + "_q"].at[4 + kind * 3 + off], dev_uv(axis, u, vo, xh),
                ),
                v != vo,
            )

    def s3_sum(name, extra):
        acc, r3, part = r[name + "_acc"], r[name + "_r3"], r[name + "_t"]

        def add(kind, slot):
            for off in range(3):
                arrive(r3.at[kind, off], r[name + "_q"].at[4 + kind * 3 + off])
            part[kind] = (acc[slot] + r3[kind, 0]) + (r3[kind, 1] + r3[kind, 2])

        add(0, main)
        if extra:
            pl.when(on_diag)(lambda: add(1, 4))

    def s4(name, extra):
        src = r[name + "_t"].at[extra_give] if extra else r[name + "_t"].at[0]
        cond = gives if extra else no(owns_main)
        launch(rcopy(src, r[name + "_r4"], r[name + "_s"].at[9], r[name + "_q"].at[10], far), cond)

    def s4_total(name, extra):
        arrive(r[name + "_r4"], r[name + "_q"].at[10])
        mine = r[name + "_t"][extra_mine] if extra else r[name + "_t"][0]
        return mine + r[name + "_r4"][...]

    def g1(name):
        u, _ = uv(GATHERS[name][1])
        place = r[name].at[c, u, own]
        rcopy(place, place, r[name + "_s"].at[0], r[name + "_q"].at[0], far).start()

    def g1_arrive(name):
        u, _ = uv(GATHERS[name][1])
        arrive(r[name].at[c, u, jnp.where(owns_main, 4, main)], r[name + "_q"].at[0], gives)

    def g2(name):
        axis = GATHERS[name][1]
        u, v = uv(axis)
        for d in (1, 3, 2):
            for kind in (0, 1):
                slot = 4 if kind else main
                place = r[name].at[c, u, slot]
                launch(
                    rcopy(
                        place, place, r[name + "_s"].at[kind * 3 + d], r[name + "_q"].at[1 + slot],
                        dev_uv(axis, u, (v + d) % 4, xh),
                    ),
                    on_diag if kind else None,
                )

    def g2_arrive(name):
        axis = GATHERS[name][1]
        u, v = uv(axis)
        for p in range(5):
            arrive(r[name].at[c, u, p], r[name + "_q"].at[1 + p], v != target(axis, p))

    def g3(name):
        axis = GATHERS[name][1]
        u, v = uv(axis)
        place = r[name].at[c, u]
        for d in (1, 3, 2):
            launch(
                rcopy(
                    place, place, r[name + "_s"].at[6 + d], r[name + "_q"].at[5 + d],
                    dev_uv(axis, (u + d) % 4, v, xh),
                )
            )

    def g3_arrive(name):
        u, _ = uv(GATHERS[name][1])
        for d in (1, 2, 3):
            arrive(r[name].at[c, (u - d + 4) % 4], r[name + "_q"].at[5 + d])

    def g4(name):
        place = r[name].at[c]
        launch(rcopy(place, place, r[name + "_s"].at[10], r[name + "_q"].at[9], sibling))

    def g4_arrive(name):
        arrive(r[name].at[1 - c], r[name + "_q"].at[9])

    x1, x2, x2o = r["x1"], r["x2"], r["x2o"]

    def part_head(p, j):
        half = (1 - c) if j < 4 else c
        return half, j % 4, half * HALF + head_of(j % 4, p)

    def columns(h):
        return pl.ds(pl.multiple_of(h * HD, HD), HD)

    def exchange(lo, hi):
        for n in range(lo, hi):
            p, j = n // 8, n % 8
            _, _, h = part_head(p, j)
            src = r["x2_hbm"].at[0, :, columns(h)] if n < FROM_HBM else x2.at[:, columns(h)]
            sem = 2 * p + j // 4
            rcopy(src, x2o.at[p, j], r["x_s"].at[sem], r["x_q"].at[sem], twin).start()

    load1 = pltpu.make_async_copy(r["x1_hbm"].at[0], x1, r["l_s"].at[0])
    load2 = pltpu.make_async_copy(r["x2_hbm"].at[0], x2, r["l_s"].at[1])
    load2.start()
    load1.start()
    barrier = pltpu.get_barrier_semaphore()
    peers = [sibling, twin]
    for i in range(1, 8):
        peers.append(dev(z, (y + i // 2) % 4, (xh + i % 2) % 2, c))
    for i in range(2, 8):
        peers.append(dev((z + i // 2) % 4, y, (xh + i % 2) % 2, c))
    for i in range(1, 4):
        peers.append(dev((z + i) % 4, y, xh, 1 - c))
    for peer in peers:
        pl.semaphore_signal(barrier, inc=1, device_id=peer, device_id_type=MESH)
    pl.semaphore_wait(barrier, len(peers))
    exchange(0, FROM_HBM)
    load2.wait()
    exchange(FROM_HBM, BATCHES[0])
    load1.wait()

    upper, diag = masks()
    eye = jnp.where(diag, 1.0, 0.0).astype(F32)
    row8 = iota((8, HD), 0)

    def gram(h):
        ch, zz, yy, p = places(h)
        cols = columns(h)
        ab = jnp.concatenate([x1[:, cols], x2[:, cols]], axis=1)
        g = dot_t(ab, ab)
        sums = jnp.dot(jnp.ones((8, ab.shape[0]), ab.dtype), ab, preferred_element_type=F32)
        g1_, cr, g2_ = g[:HD, :HD], g[:HD, HD:], g[HD:, HD:]
        packed = jnp.where(upper, g1_, g2_)
        dg = jnp.sum(jnp.where(diag, g2_, 0.0), axis=0, keepdims=True)
        aux = jnp.where(
            row8 == 0, sums[:, :HD],
            jnp.where(row8 == 1, sums[:, HD:], jnp.where(row8 == 2, jnp.broadcast_to(dg, (8, HD)), 0.0)),
        )
        r["pa"][ch, zz, p, 0:64] = packed[:64]
        r["pa"][ch, zz, p, 64:72] = aux
        r["pb"][ch, yy, p] = packed[64:]
        r["ca"][ch, zz, p] = cr[:64]
        r["cb"][ch, yy, p] = cr[64:]

    def cross(p, which):
        arrive(x2o.at[p, pl.ds(4 * which, 4)], r["x_q"].at[2 * p + which])
        for j in range(4 * which, 4 * which + 4):
            half, zz, h = part_head(p, j)
            yy = zz if p == 4 else (zz + p) % 4
            cr = dot_t(x1[:, columns(h)], x2o[p, j])
            r["da"][p, half, zz] = cr[:64]
            r["db"][p, half, yy] = cr[64:]
            if j == 3:
                for name in LATE:
                    launch(
                        rcopy(
                            r[name].at[p, 1 - c], r[name + "_r1"].at[p], r[name + "_s"].at[p],
                            r[name + "_q"].at[p], sibling,
                        )
                    )

    def cross_s2(p):
        for name, axis in LATE.items():
            buf, r1 = r[name], r[name + "_r1"]
            u, v = uv(axis)
            arrive(r1.at[p], r[name + "_q"].at[p])
            for i in range(4):
                buf[p, c, i] = buf[p, c, i] + r1[p, i]
            for d in (1, 3, 2):
                to = (u + d) % 4
                launch(
                    rcopy(
                        buf.at[p, c, to], r[name + "_r2"].at[p, d - 1], r[name + "_s"].at[2 + 3 * (p + 1) + d - 1],
                        r[name + "_q"].at[2 + 3 * (p + 1) + d - 1], dev_uv(axis, to, v, xh),
                    )
                )

    def cross_s2_sum(p):
        for name, axis in LATE.items():
            buf, r2 = r[name], r[name + "_r2"]
            u, _ = uv(axis)
            for d in (1, 2, 3):
                arrive(r2.at[p, d - 1], r[name + "_q"].at[2 + 3 * (p + 1) + d - 1])
            r[name + "x_acc"][p] = (buf[p, c, u] + r2[p, 0]) + (r2[p, 1] + r2[p, 2])

    def last_s3():
        for name, axis in LATE.items():
            u, v = uv(axis)
            slot = ((v - u + 4) % 4) * 2 + 1 - xh
            launch(
                rcopy(
                    r[name + "x_acc"].at[4], r[name + "_r5"].at[slot], r[name + "_s"].at[20],
                    r[name + "_q"].at[20 + slot], dev_uv(axis, u, u, 1),
                ),
                no(late_owner),
            )

    def last_total(name):
        total = r[name + "x_acc"][4]
        for slot in range(1, 8):
            arrive(r[name + "_r5"].at[slot], r[name + "_q"].at[20 + slot])
        for slot in range(1, 8):
            total = total + r[name + "_r5"][slot]
        return total

    def only_row0(row):
        return jnp.where(row8 == 0, jnp.broadcast_to(row, (8, HD)), 0.0)

    def similarity(raw, sums, w2):
        mean1 = only_row0(r["aux"][0:1, :]) / tokens
        cov = raw / tokens - dot_t(mean1, only_row0(sums) / tokens, HI)
        white = mm(mm(r["w12"][0], cov), w2)
        sq = jnp.sum(jnp.sum(white * white, axis=1, keepdims=True), axis=0, keepdims=True)
        return jnp.broadcast_to(sq / HD, (8, HD))

    def whiten():
        top = s4_total("pa", True)
        low = s4_total("pb", True)
        aux = top[64:72]
        grams = unpack(top[:64], low, aux)
        ys, zs, scales = [], [], []
        for n in (0, 1):
            mean = only_row0(aux[n : n + 1, :]) / tokens
            cov = grams[n] / tokens - dot_t(mean, mean, HI) + RIDGE * eye
            sq = jnp.sum(jnp.sum(cov * cov, axis=1, keepdims=True), axis=0, keepdims=True)
            scale = jnp.sqrt(sq)
            scales.append(scale)
            ys.append(cov / scale)
        for it in range(ITERS):
            for n in (0, 1):
                if it == 0:
                    f = 1.5 * eye - 0.5 * ys[n]
                    zs.append(f)
                else:
                    f = 1.5 * eye - 0.5 * mm(zs[n], ys[n])
                    zs[n] = mm(f, zs[n])
                if it < ITERS - 1:
                    ys[n] = mm(ys[n], f)
        w1 = zs[0] / jnp.sqrt(scales[0])
        w2 = zs[1] / jnp.sqrt(scales[1])
        wp = jnp.where(upper, w1, w2)
        wd = jnp.sum(jnp.where(diag, w2, 0.0), axis=0, keepdims=True)
        r["wa"][c, z, own, 0:64] = wp[:64]
        r["wa"][c, z, own, 64:72] = jnp.broadcast_to(wd, (8, HD))
        r["wb"][c, y, own] = wp[64:]
        g1("wa")
        g1("wb")
        r["w12"][0] = w1
        r["w12"][1] = w2
        r["aux"][...] = aux
        r["w_out_x"][0:HD] = w2
        r["w_out_x"][HD : HD + 8] = aux
        rcopy(r["w_out_x"], r["w_in_x"], r["y_s"].at[0], r["y_q"].at[0], twin).start()

    def both(p):
        cross(p, 0)
        cross(p, 1)

    loop(HALF, lambda i: gram((1 - c) * HALF + i), unroll=2)
    for name in CHAINS:
        s1(name)
    loop(HALF, lambda i: gram(c * HALF + i), unroll=2)
    for name in ("pa", "pb"):
        s1_sum(name)
        s2(name)
    for name in ("ca", "cb"):
        s1_sum(name)
    both(0)
    for name in ("pa", "pb"):
        s2_sum(name)
        s3(name, CHAINS[name][1], range(5))
    for name in ("pa", "pb"):
        s3_sum(name, True)
        s4(name, True)
    exchange(BATCHES[0], BATCHES[1])
    for name in ("ca", "cb"):
        s2(name)
    pl.when(owner)(whiten)
    exchange(BATCHES[1], BATCHES[2])
    for name in GATHERS:
        g1_arrive(name)
        g2(name)
    both(1)
    cross_s2(0)
    for name in ("ca", "cb"):
        s2_sum(name)
        s3(name, CHAINS[name][1], range(5))
    for name in GATHERS:
        g2_arrive(name)
        g3(name)
    for name in ("ca", "cb"):
        s3_sum(name, True)
        s4(name, True)
    exchange(BATCHES[2], 8 * PARTS)
    cross_s2(1)
    both(2)
    cross_s2_sum(0)

    lane_head = c * HALF + jnp.where(own == 4, 16 + z, head_of(z, own))
    here = iota((8, HD), 1) == lane_head
    sa_mine = r["sa"].at[c, z, own]

    def own_similarity():
        raw = jnp.concatenate([s4_total("ca", True), s4_total("cb", True)], axis=0)
        sim = similarity(raw, r["aux"][1:2, :], r["w12"][1])
        sa_mine[...] = jnp.where(jnp.logical_and(here, row8 == lay), sim, 0.0)
        arrive(r["w_in_x"], r["y_q"].at[0])

    def other_similarity(raw):
        sim = similarity(raw, r["w_in_x"][HD + 1 : HD + 2], r["w_in_x"][0:HD])
        sa_mine[...] = jnp.where(jnp.logical_and(here, row8 == 1 - lay), sim, sa_mine[...])
        for i in range(1, 8):
            rcopy(
                sa_mine, sa_mine, r["sa_s"].at[i], r["sa_q"].at[own],
                dev(z, (y + i // 2) % 4, (xh + i % 2) % 2, c),
            ).start()

    def emit(h):
        ch, zz, yy, p = places(h)
        w1, w2 = unpack(r["wa"][ch, zz, p, 0:64], r["wb"][ch, yy, p], r["wa"][ch, zz, p, 64:72])
        r["w"][0, h] = w1
        r["w"][1, h] = w2

    pl.when(owner)(own_similarity)
    cross_s2(2)
    cross_s2_sum(1)
    for name in GATHERS:
        g3_arrive(name)
        g4(name)
    both(3)
    cross_s2_sum(2)
    cross_s2(3)
    for name in GATHERS:
        g4_arrive(name)
    loop(HEADS, emit, unroll=2)
    cross_s2_sum(3)
    for name, axis in LATE.items():
        s3(name + "x", axis, range(4))
    for name in LATE:
        s3_sum(name + "x", False)
        s4(name + "x", False)
    cross(4, 0)
    cross(4, 1)
    cross_s2(4)
    cross_s2_sum(4)
    last_s3()

    @pl.when(early_owner)
    def _():
        other_similarity(jnp.concatenate([s4_total("dax", False), s4_total("dbx", False)], axis=0))

    @pl.when(late_owner)
    def _():
        other_similarity(jnp.concatenate([last_total("da"), last_total("db")], axis=0))

    for p in range(5):
        arrive(r["sa"].at[c, z, p], r["sa_q"].at[p], no(jnp.logical_and(owner, own == p)))
    mine = r["sa"].at[c, z]
    for i in range(1, 8):
        launch(
            rcopy(
                mine, mine, r["sa_s"].at[7 + i], r["sa_q"].at[4 + i],
                dev((z + i // 2) % 4, y, xh, (c + i % 2) % 2),
            )
        )
    for i in range(1, 8):
        arrive(r["sa"].at[(c + i % 2) % 2, (z - i // 2 + 4) % 4], r["sa_q"].at[4 + i])

    total = jnp.zeros((8, HD), F32)
    for ch in range(2):
        for i in range(4):
            for s in range(5):
                total = total + r["sa"][ch, i, s]
    r["sim"][...] = total

    for cond, copy in pending:
        if cond is None:
            copy.wait_send()
        else:
            pl.when(cond)(lambda copy=copy: copy.wait_send())
    for i in range(2 * PARTS):
        part = x2o.at[i // 2, pl.ds(4 * (i % 2), 4)]
        rcopy(part, part, r["x_s"].at[i], r["x_q"].at[i], twin).wait_send()

    @pl.when(owner)
    def _():
        for name in GATHERS:
            u, _ = uv(GATHERS[name][1])
            place = r[name].at[c, u, own]
            rcopy(place, place, r[name + "_s"].at[0], r[name + "_q"].at[0], far).wait_send()
        rcopy(r["w_out_x"], r["w_in_x"], r["y_s"].at[0], r["y_q"].at[0], twin).wait_send()
        for i in range(1, 8):
            rcopy(sa_mine, sa_mine, r["sa_s"].at[i], r["sa_q"].at[own], far).wait_send()


def gather_kernel(tokens, first_acts, second_acts):
    rows, width = first_acts.shape[1:]
    names = ["x1_hbm", "x2_hbm", "w", "sim"]
    scratch = []

    def add(name, spec):
        names.append(name)
        scratch.append(spec)

    dma = lambda n: pltpu.SemaphoreType.DMA((n,))
    for name in ("x1", "x2"):
        add(name, pltpu.VMEM((rows, width), first_acts.dtype))
    add("x2o", pltpu.VMEM((PARTS, 8, rows, HD), first_acts.dtype))
    for name, (n, _) in CHAINS.items():
        add(name, pltpu.VMEM((2, 4, 5, n, HD), F32))
        add(name + "_r1", pltpu.VMEM((4, 5, n, HD), F32))
        add(name + "_r2", pltpu.VMEM((3, 5, n, HD), F32))
    for name in LATE:
        add(name, pltpu.VMEM((PARTS, 2, 4, 64, HD), F32))
        add(name + "_r1", pltpu.VMEM((PARTS, 4, 64, HD), F32))
        add(name + "_r2", pltpu.VMEM((PARTS, 3, 64, HD), F32))
        add(name + "_r5", pltpu.VMEM((8, 64, HD), F32))
        add(name + "_s", dma(21))
        add(name + "_q", dma(28))
    for name, n in [(k, v[0]) for k, v in CHAINS.items()] + [(k + "x", 64) for k in LATE]:
        add(name + "_acc", pltpu.VMEM((5, n, HD), F32))
        add(name + "_r3", pltpu.VMEM((2, 3, n, HD), F32))
        add(name + "_t", pltpu.VMEM((2, n, HD), F32))
        add(name + "_r4", pltpu.VMEM((n, HD), F32))
        add(name + "_s", dma(10))
        add(name + "_q", dma(11))
    add("sa", pltpu.VMEM((2, 4, 5, 8, HD), F32))
    for name, (n, _) in GATHERS.items():
        add(name, pltpu.VMEM((2, 4, 5, n, HD), F32))
        add(name + "_s", dma(11))
        add(name + "_q", dma(10))
    add("sa_s", dma(15))
    add("sa_q", dma(12))
    add("w12", pltpu.VMEM((2, HD, HD), F32))
    add("aux", pltpu.VMEM((8, HD), F32))
    add("w_out_x", pltpu.VMEM((HD + 8, HD), F32))
    add("w_in_x", pltpu.VMEM((HD + 8, HD), F32))
    add("l_s", dma(2))
    add("x_s", dma(2 * PARTS))
    add("x_q", dma(2 * PARTS))
    add("y_s", dma(1))
    add("y_q", dma(1))
    add("none", dma(1))
    return pl.pallas_call(
        functools.partial(kernel, tokens, names),
        out_shape=(
            pltpu.VMEM((2, HEADS, HD, HD), F32),
            pltpu.VMEM((8, HD), F32),
        ),
        in_specs=[pl.BlockSpec(memory_space=pltpu.HBM)] * 2,
        out_specs=[pl.BlockSpec(memory_space=pltpu.VMEM)] * 2,
        scratch_shapes=scratch,
        compiler_params=pltpu.CompilerParams(
            collective_id=0, has_side_effects=True, vmem_limit_bytes=VMEM_LIMIT
        ),
    )(
        pltpu.with_memory_space_constraint(first_acts, pltpu.HBM),
        pltpu.with_memory_space_constraint(second_acts, pltpu.HBM),
    )


def store_kernel(w, sim, w_hbm, s_ref, sem):
    copy = pltpu.make_async_copy(w, w_hbm.at[:, 0], sem.at[0])
    copy.start()
    s_ref[0] = sim[0:2, 0:HEADS]
    copy.wait()


def store(w, sim):
    vmem = pl.BlockSpec(memory_space=pltpu.VMEM)
    return pl.pallas_call(
        store_kernel,
        out_shape=(
            jax.ShapeDtypeStruct((2, 1, HEADS, HD, HD), F32),
            jax.ShapeDtypeStruct((1, 2, HEADS), F32),
        ),
        in_specs=[vmem] * 2,
        out_specs=(pl.BlockSpec(memory_space=pltpu.HBM), vmem),
        scratch_shapes=[pltpu.SemaphoreType.DMA((1,))],
        compiler_params=pltpu.CompilerParams(vmem_limit_bytes=16 * 2**20),
    )(w, sim)


def solution(mesh):
    def whole(first_acts, second_acts):
        tokens = first_acts.shape[1] * lax.axis_size("tok")
        return store(*gather_kernel(tokens, first_acts, second_acts))

    in_specs = (P("lay", "tok", None), P("lay", "tok", None))
    out_specs = (P(None, "lay", None, None, None), P("lay", None, None))
    return jax.shard_map(whole, mesh=mesh, in_specs=in_specs, out_specs=out_specs, check_vma=False)
```

```python
import functools

import jax
import jax.numpy as jnp
from jax import lax
from jax.experimental import pallas as pl
from jax.experimental.pallas import tpu as pltpu
from jax.sharding import PartitionSpec as P

HEADS = 40
HD = 128
ITERS = 6
RIDGE = 0.05
HALF = HEADS // 2
PARTS = 5
FROM_HBM = 3
BATCHES = (14, 19, 27)
VMEM_LIMIT = 48 * 2**20
F32 = jnp.float32
HI = lax.Precision.HIGHEST
MESH = pl.DeviceIdType.MESH

CHAINS = {"pa": (72, "z"), "pb": (64, "y"), "ca": (64, "z"), "cb": (64, "y")}
LATE = {"da": "z", "db": "y"}
GATHERS = {"wa": (72, "z"), "wb": (64, "y")}


def iota(shape, dim):
    return lax.broadcasted_iota(jnp.int32, shape, dim)


def dot_t(a, b, precision=None):
    return lax.dot_general(
        a, b, (((0,), (0,)), ((), ())), precision=precision, preferred_element_type=F32
    )


def mm(a, b):
    return jnp.dot(a, b, precision=HI, preferred_element_type=F32)


def masks():
    ri, ci = iota((HD, HD), 0), iota((HD, HD), 1)
    return ri <= ci, ri == ci


def unpack(top, low, aux):
    upper, diag = masks()
    p = jnp.concatenate([top, low], axis=0)
    pt = p.T
    first = jnp.where(upper, p, pt)
    second = jnp.where(upper, jnp.where(diag, aux[2:3, :], pt), p)
    return first, second


def head_of(z, p):
    k = 4 * ((z + p) % 4) + z
    if isinstance(p, int):
        return 16 + z if p == 4 else k
    return jnp.where(p == 4, 16 + z, k)


def places(h):
    k = h % HALF
    z = k % 4
    y = jnp.where(k < 16, k // 4, z)
    p = jnp.where(k < 16, (k // 4 - z + 4) % 4, 4)
    return h // HALF, z, y, p


def kernel(tokens, names, *refs):
    r = dict(zip(names, refs))
    tok = lax.axis_index("tok")
    lay = lax.axis_index("lay")
    c = tok % 2
    xh = (tok // 2) % 2
    y = (tok // 4) % 4
    z = tok // 16

    def dev(z_, y_, xh_, c_):
        return (((z_ * 4 + y_) * 2 + xh_) * 2 + c_, lay)

    def uv(axis):
        return (z, y) if axis == "z" else (y, z)

    def dev_uv(axis, u, v, xh_):
        return dev(u, v, xh_, c) if axis == "z" else dev(v, u, xh_, c)

    sibling = dev(z, y, xh, 1 - c)
    twin = (tok, 1 - lay)
    far = dev(z, y, 1 - xh, c)

    on_diag = z == y
    main = (y - z + 4) % 4
    owns_main = xh == main % 2
    owner = jnp.logical_or(owns_main, on_diag)
    own = jnp.where(owns_main, main, 4)
    late_owner = jnp.logical_and(on_diag, xh == 1)
    early_owner = owns_main
    extra_mine = jnp.where(owns_main, 0, 1)
    extra_give = jnp.where(owns_main, 1, 0)
    gives = jnp.logical_or(on_diag, jnp.logical_not(owns_main))
    no = jnp.logical_not

    def target(axis, p):
        u, _ = uv(axis)
        if p == 4:
            return u
        return (u + p) % 4 if axis == "z" else (u - p + 4) % 4

    def rcopy(src, dst, ssem, rsem, device):
        return pltpu.make_async_remote_copy(
            src_ref=src, dst_ref=dst, send_sem=ssem, recv_sem=rsem,
            device_id=device, device_id_type=MESH,
        )

    others = lax.axis_size("tok") - 1
    pending = []

    def launch(copy, cond=None):
        pending.append((cond, copy))
        if cond is None:
            copy.start()
        else:
            pl.when(cond)(lambda: copy.start())

    def arrive(ref, sem, cond=None):
        copy = rcopy(ref, ref, r["none"].at[0], sem, twin)
        if cond is None:
            copy.wait_recv()
        else:
            pl.when(cond)(lambda: copy.wait_recv())

    def loop(n, body, unroll=1):
        def step(i, carry):
            body(i)
            return carry

        lax.fori_loop(0, n, step, 0, unroll=unroll)

    def s1(name):
        launch(rcopy(r[name].at[1 - c], r[name + "_r1"], r[name + "_s"].at[0], r[name + "_q"].at[0], sibling))

    def s1_sum(name):
        buf, r1 = r[name], r[name + "_r1"]
        arrive(r1, r[name + "_q"].at[0])

        def body(i):
            for s in range(5):
                buf[c, i, s] = buf[c, i, s] + r1[i, s]

        loop(4, body)

    def s2(name):
        axis = CHAINS[name][1]
        u, v = uv(axis)
        for d in (1, 3, 2):
            to = (u + d) % 4
            launch(
                rcopy(
                    r[name].at[c, to], r[name + "_r2"].at[d - 1], r[name + "_s"].at[d],
                    r[name + "_q"].at[d], dev_uv(axis, to, v, xh),
                )
            )

    def s2_sum(name):
        u, _ = uv(CHAINS[name][1])
        buf, r2, acc = r[name], r[name + "_r2"], r[name + "_acc"]
        for d in (1, 2, 3):
            arrive(r2.at[d - 1], r[name + "_q"].at[d])
        for s in range(5):
            acc[s] = (buf[c, u, s] + r2[0, s]) + (r2[1, s] + r2[2, s])

    def s3(name, axis, slots):
        u, v = uv(axis)
        for p in slots:
            vo = target(axis, p)
            off = jnp.maximum((v - vo + 4) % 4, 1) - 1
            kind = p // 4
            launch(
                rcopy(
                    r[name + "_acc"].at[p], r[name + "_r3"].at[kind, off], r[name + "_s"].at[4 + p],
                    r[name + "_q"].at[4 + kind * 3 + off], dev_uv(axis, u, vo, xh),
                ),
                v != vo,
            )

    def s3_sum(name, extra):
        acc, r3, part = r[name + "_acc"], r[name + "_r3"], r[name + "_t"]

        def add(kind, slot):
            for off in range(3):
                arrive(r3.at[kind, off], r[name + "_q"].at[4 + kind * 3 + off])
            part[kind] = (acc[slot] + r3[kind, 0]) + (r3[kind, 1] + r3[kind, 2])

        add(0, main)
        if extra:
            pl.when(on_diag)(lambda: add(1, 4))

    def s4(name, extra):
        src = r[name + "_t"].at[extra_give] if extra else r[name + "_t"].at[0]
        cond = gives if extra else no(owns_main)
        launch(rcopy(src, r[name + "_r4"], r[name + "_s"].at[9], r[name + "_q"].at[10], far), cond)

    def s4_total(name, extra):
        arrive(r[name + "_r4"], r[name + "_q"].at[10])
        mine = r[name + "_t"][extra_mine] if extra else r[name + "_t"][0]
        return mine + r[name + "_r4"][...]

    def g1(name):
        u, _ = uv(GATHERS[name][1])
        place = r[name].at[c, u, own]
        rcopy(place, place, r[name + "_s"].at[0], r[name + "_q"].at[0], far).start()

    def g1_arrive(name):
        u, _ = uv(GATHERS[name][1])
        arrive(r[name].at[c, u, jnp.where(owns_main, 4, main)], r[name + "_q"].at[0], gives)

    def g2(name):
        axis = GATHERS[name][1]
        u, v = uv(axis)
        for d in (1, 3, 2):
            for kind in (0, 1):
                slot = 4 if kind else main
                place = r[name].at[c, u, slot]
                launch(
                    rcopy(
                        place, place, r[name + "_s"].at[kind * 3 + d], r[name + "_q"].at[1 + slot],
                        dev_uv(axis, u, (v + d) % 4, xh),
                    ),
                    on_diag if kind else None,
                )

    def g2_arrive(name):
        axis = GATHERS[name][1]
        u, v = uv(axis)
        for p in range(5):
            arrive(r[name].at[c, u, p], r[name + "_q"].at[1 + p], v != target(axis, p))

    def g3(name):
        axis = GATHERS[name][1]
        u, v = uv(axis)
        place = r[name].at[c, u]
        for d in (1, 3, 2):
            launch(
                rcopy(
                    place, place, r[name + "_s"].at[6 + d], r[name + "_q"].at[5 + d],
                    dev_uv(axis, (u + d) % 4, v, xh),
                )
            )

    def g3_arrive(name):
        u, _ = uv(GATHERS[name][1])
        for d in (1, 2, 3):
            arrive(r[name].at[c, (u - d + 4) % 4], r[name + "_q"].at[5 + d])

    def g4(name):
        place = r[name].at[c]
        launch(rcopy(place, place, r[name + "_s"].at[10], r[name + "_q"].at[9], sibling))

    def g4_arrive(name):
        arrive(r[name].at[1 - c], r[name + "_q"].at[9])

    x1, x2, x2o = r["x1"], r["x2"], r["x2o"]

    def part_head(p, j):
        half = (1 - c) if j < 4 else c
        return half, j % 4, half * HALF + head_of(j % 4, p)

    def columns(h):
        return pl.ds(pl.multiple_of(h * HD, HD), HD)

    def exchange(lo, hi):
        for n in range(lo, hi):
            p, j = n // 8, n % 8
            _, _, h = part_head(p, j)
            src = r["x2_hbm"].at[0, :, columns(h)] if n < FROM_HBM else x2.at[:, columns(h)]
            sem = 2 * p + j // 4
            rcopy(src, x2o.at[p, j], r["x_s"].at[sem], r["x_q"].at[sem], twin).start()

    load1 = pltpu.make_async_copy(r["x1_hbm"].at[0], x1, r["l_s"].at[0])
    load2 = pltpu.make_async_copy(r["x2_hbm"].at[0], x2, r["l_s"].at[1])
    load2.start()
    load1.start()
    barrier = pltpu.get_barrier_semaphore()
    peers = [sibling, twin]
    for i in range(1, 8):
        peers.append(dev(z, (y + i // 2) % 4, (xh + i % 2) % 2, c))
    for i in range(2, 8):
        peers.append(dev((z + i // 2) % 4, y, (xh + i % 2) % 2, c))
    for peer in peers:
        pl.semaphore_signal(barrier, inc=1, device_id=peer, device_id_type=MESH)
    pl.semaphore_wait(barrier, len(peers))
    exchange(0, FROM_HBM)
    load2.wait()
    exchange(FROM_HBM, BATCHES[0])
    load1.wait()

    upper, diag = masks()
    eye = jnp.where(diag, 1.0, 0.0).astype(F32)
    row8 = iota((8, HD), 0)

    def gram(h):
        ch, zz, yy, p = places(h)
        cols = columns(h)
        ab = jnp.concatenate([x1[:, cols], x2[:, cols]], axis=1)
        g = dot_t(ab, ab)
        sums = jnp.dot(jnp.ones((8, ab.shape[0]), ab.dtype), ab, preferred_element_type=F32)
        g1_, cr, g2_ = g[:HD, :HD], g[:HD, HD:], g[HD:, HD:]
        packed = jnp.where(upper, g1_, g2_)
        dg = jnp.sum(jnp.where(diag, g2_, 0.0), axis=0, keepdims=True)
        aux = jnp.where(
            row8 == 0, sums[:, :HD],
            jnp.where(row8 == 1, sums[:, HD:], jnp.where(row8 == 2, jnp.broadcast_to(dg, (8, HD)), 0.0)),
        )
        r["pa"][ch, zz, p, 0:64] = packed[:64]
        r["pa"][ch, zz, p, 64:72] = aux
        r["pb"][ch, yy, p] = packed[64:]
        r["ca"][ch, zz, p] = cr[:64]
        r["cb"][ch, yy, p] = cr[64:]

    def cross(p, which):
        arrive(x2o.at[p, pl.ds(4 * which, 4)], r["x_q"].at[2 * p + which])
        for j in range(4 * which, 4 * which + 4):
            half, zz, h = part_head(p, j)
            yy = zz if p == 4 else (zz + p) % 4
            cr = dot_t(x1[:, columns(h)], x2o[p, j])
            r["da"][p, half, zz] = cr[:64]
            r["db"][p, half, yy] = cr[64:]
            if j == 3:
                for name in LATE:
                    launch(
                        rcopy(
                            r[name].at[p, 1 - c], r[name + "_r1"].at[p], r[name + "_s"].at[p],
                            r[name + "_q"].at[p], sibling,
                        )
                    )

    def cross_s2(p):
        for name, axis in LATE.items():
            buf, r1 = r[name], r[name + "_r1"]
            u, v = uv(axis)
            arrive(r1.at[p], r[name + "_q"].at[p])
            for i in range(4):
                buf[p, c, i] = buf[p, c, i] + r1[p, i]
            for d in (1, 3, 2):
                to = (u + d) % 4
                launch(
                    rcopy(
                        buf.at[p, c, to], r[name + "_r2"].at[p, d - 1], r[name + "_s"].at[2 + 3 * (p + 1) + d - 1],
                        r[name + "_q"].at[2 + 3 * (p + 1) + d - 1], dev_uv(axis, to, v, xh),
                    )
                )

    def cross_s2_sum(p):
        for name, axis in LATE.items():
            buf, r2 = r[name], r[name + "_r2"]
            u, _ = uv(axis)
            for d in (1, 2, 3):
                arrive(r2.at[p, d - 1], r[name + "_q"].at[2 + 3 * (p + 1) + d - 1])
            r[name + "x_acc"][p] = (buf[p, c, u] + r2[p, 0]) + (r2[p, 1] + r2[p, 2])

    def last_s3():
        for name, axis in LATE.items():
            u, v = uv(axis)
            slot = ((v - u + 4) % 4) * 2 + 1 - xh
            launch(
                rcopy(
                    r[name + "x_acc"].at[4], r[name + "_r5"].at[slot], r[name + "_s"].at[20],
                    r[name + "_q"].at[20 + slot], dev_uv(axis, u, u, 1),
                ),
                no(late_owner),
            )

    def last_total(name):
        total = r[name + "x_acc"][4]
        for slot in range(1, 8):
            arrive(r[name + "_r5"].at[slot], r[name + "_q"].at[20 + slot])
        for slot in range(1, 8):
            total = total + r[name + "_r5"][slot]
        return total

    def only_row0(row):
        return jnp.where(row8 == 0, jnp.broadcast_to(row, (8, HD)), 0.0)

    def similarity(raw, sums, w2):
        mean1 = only_row0(r["aux"][0:1, :]) / tokens
        cov = raw / tokens - dot_t(mean1, only_row0(sums) / tokens, HI)
        white = mm(mm(r["w12"][0], cov), w2)
        sq = jnp.sum(jnp.sum(white * white, axis=1, keepdims=True), axis=0, keepdims=True)
        return jnp.broadcast_to(sq / HD, (8, HD))

    def whiten():
        top = s4_total("pa", True)
        low = s4_total("pb", True)
        aux = top[64:72]
        grams = unpack(top[:64], low, aux)
        ys, zs, scales = [], [], []
        for n in (0, 1):
            mean = only_row0(aux[n : n + 1, :]) / tokens
            cov = grams[n] / tokens - dot_t(mean, mean, HI) + RIDGE * eye
            sq = jnp.sum(jnp.sum(cov * cov, axis=1, keepdims=True), axis=0, keepdims=True)
            scale = jnp.sqrt(sq)
            scales.append(scale)
            ys.append(cov / scale)
        for it in range(ITERS):
            for n in (0, 1):
                if it == 0:
                    f = 1.5 * eye - 0.5 * ys[n]
                    zs.append(f)
                else:
                    f = 1.5 * eye - 0.5 * mm(zs[n], ys[n])
                    zs[n] = mm(f, zs[n])
                if it < ITERS - 1:
                    ys[n] = mm(ys[n], f)
        w1 = zs[0] / jnp.sqrt(scales[0])
        w2 = zs[1] / jnp.sqrt(scales[1])
        wp = jnp.where(upper, w1, w2)
        wd = jnp.sum(jnp.where(diag, w2, 0.0), axis=0, keepdims=True)
        r["wa"][c, z, own, 0:64] = wp[:64]
        r["wa"][c, z, own, 64:72] = jnp.broadcast_to(wd, (8, HD))
        r["wb"][c, y, own] = wp[64:]
        g1("wa")
        g1("wb")
        r["w12"][0] = w1
        r["w12"][1] = w2
        r["aux"][...] = aux
        r["w_out_x"][0:HD] = w2
        r["w_out_x"][HD : HD + 8] = aux
        rcopy(r["w_out_x"], r["w_in_x"], r["y_s"].at[0], r["y_q"].at[0], twin).start()

    def both(p):
        cross(p, 0)
        cross(p, 1)

    loop(HALF, lambda i: gram((1 - c) * HALF + i), unroll=2)
    for name in CHAINS:
        s1(name)
    loop(HALF, lambda i: gram(c * HALF + i), unroll=2)
    for name in ("pa", "pb"):
        s1_sum(name)
        s2(name)
    for name in ("ca", "cb"):
        s1_sum(name)
    both(0)
    for name in ("pa", "pb"):
        s2_sum(name)
        s3(name, CHAINS[name][1], range(5))
    for name in ("pa", "pb"):
        s3_sum(name, True)
        s4(name, True)
    exchange(BATCHES[0], BATCHES[1])
    for name in ("ca", "cb"):
        s2(name)
    pl.when(owner)(whiten)
    exchange(BATCHES[1], BATCHES[2])
    for name in GATHERS:
        g1_arrive(name)
        g2(name)
    both(1)
    cross_s2(0)
    for name in ("ca", "cb"):
        s2_sum(name)
        s3(name, CHAINS[name][1], range(5))
    for name in GATHERS:
        g2_arrive(name)
        g3(name)
    for name in ("ca", "cb"):
        s3_sum(name, True)
        s4(name, True)
    exchange(BATCHES[2], 8 * PARTS)
    cross_s2(1)
    both(2)
    cross_s2_sum(0)

    lane_head = c * HALF + jnp.where(own == 4, 16 + z, head_of(z, own))
    here = iota((8, HD), 1) == lane_head
    sa_mine = r["sa"].at[(c * 4 + z) * 5 + own]

    def own_similarity():
        raw = jnp.concatenate([s4_total("ca", True), s4_total("cb", True)], axis=0)
        sim = similarity(raw, r["aux"][1:2, :], r["w12"][1])
        sa_mine[...] = jnp.where(jnp.logical_and(here, row8 == lay), sim, 0.0)
        arrive(r["w_in_x"], r["y_q"].at[0])

    def other_similarity(raw):
        sim = similarity(raw, r["w_in_x"][HD + 1 : HD + 2], r["w_in_x"][0:HD])
        sa_mine[...] = jnp.where(jnp.logical_and(here, row8 == 1 - lay), sim, sa_mine[...])

        def send(t):
            @pl.when(t != tok)
            def _():
                rcopy(sa_mine, sa_mine, r["sa_s"].at[0], r["sa_q"].at[0], (t, lay)).start()

        loop(lax.axis_size("tok"), send)

    def emit(h):
        ch, zz, yy, p = places(h)
        w1, w2 = unpack(r["wa"][ch, zz, p, 0:64], r["wb"][ch, yy, p], r["wa"][ch, zz, p, 64:72])
        r["w"][0, h] = w1
        r["w"][1, h] = w2

    pl.when(owner)(own_similarity)
    cross_s2(2)
    cross_s2_sum(1)
    for name in GATHERS:
        g3_arrive(name)
        g4(name)
    both(3)
    cross_s2_sum(2)
    cross_s2(3)
    for name in GATHERS:
        g4_arrive(name)
    loop(HEADS, emit, unroll=2)
    cross_s2_sum(3)
    for name, axis in LATE.items():
        s3(name + "x", axis, range(4))
    cross(4, 0)
    cross(4, 1)
    cross_s2(4)
    for name in LATE:
        s3_sum(name + "x", False)
        s4(name + "x", False)
    cross_s2_sum(4)
    last_s3()

    @pl.when(early_owner)
    def _():
        other_similarity(jnp.concatenate([s4_total("dax", False), s4_total("dbx", False)], axis=0))

    @pl.when(late_owner)
    def _():
        other_similarity(jnp.concatenate([last_total("da"), last_total("db")], axis=0))

    pl.when(owner)(lambda: arrive(r["sa"].at[pl.ds(0, HEADS - 1)], r["sa_q"].at[0]))
    pl.when(no(owner))(lambda: arrive(r["sa"].at[pl.ds(0, HEADS)], r["sa_q"].at[0]))
    total = r["sa"][0]
    for i in range(1, HEADS):
        total = total + r["sa"][i]
    r["sim"][...] = total[0:2, 0:HEADS]

    for cond, copy in pending:
        if cond is None:
            copy.wait_send()
        else:
            pl.when(cond)(lambda copy=copy: copy.wait_send())
    for i in range(2 * PARTS):
        part = x2o.at[i // 2, pl.ds(4 * (i % 2), 4)]
        rcopy(part, part, r["x_s"].at[i], r["x_q"].at[i], twin).wait_send()

    @pl.when(owner)
    def _():
        for name in GATHERS:
            u, _ = uv(GATHERS[name][1])
            place = r[name].at[c, u, own]
            rcopy(place, place, r[name + "_s"].at[0], r[name + "_q"].at[0], far).wait_send()
        rcopy(r["w_out_x"], r["w_in_x"], r["y_s"].at[0], r["y_q"].at[0], twin).wait_send()
        sent = r["sa"].at[pl.ds(0, others)]
        rcopy(sent, sent, r["sa_s"].at[0], r["sa_q"].at[0], far).wait_send()


def gather_kernel(tokens, first_acts, second_acts):
    rows, width = first_acts.shape[1:]
    names = ["x1_hbm", "x2_hbm", "w", "sim"]
    scratch = []

    def add(name, spec):
        names.append(name)
        scratch.append(spec)

    dma = lambda n: pltpu.SemaphoreType.DMA((n,))
    for name in ("x1", "x2"):
        add(name, pltpu.VMEM((rows, width), first_acts.dtype))
    add("x2o", pltpu.VMEM((PARTS, 8, rows, HD), first_acts.dtype))
    for name, (n, _) in CHAINS.items():
        add(name, pltpu.VMEM((2, 4, 5, n, HD), F32))
        add(name + "_r1", pltpu.VMEM((4, 5, n, HD), F32))
        add(name + "_r2", pltpu.VMEM((3, 5, n, HD), F32))
    for name in LATE:
        add(name, pltpu.VMEM((PARTS, 2, 4, 64, HD), F32))
        add(name + "_r1", pltpu.VMEM((PARTS, 4, 64, HD), F32))
        add(name + "_r2", pltpu.VMEM((PARTS, 3, 64, HD), F32))
        add(name + "_r5", pltpu.VMEM((8, 64, HD), F32))
        add(name + "_s", dma(21))
        add(name + "_q", dma(28))
    for name, n in [(k, v[0]) for k, v in CHAINS.items()] + [(k + "x", 64) for k in LATE]:
        add(name + "_acc", pltpu.VMEM((5, n, HD), F32))
        add(name + "_r3", pltpu.VMEM((2, 3, n, HD), F32))
        add(name + "_t", pltpu.VMEM((2, n, HD), F32))
        add(name + "_r4", pltpu.VMEM((n, HD), F32))
        add(name + "_s", dma(10))
        add(name + "_q", dma(11))
    add("sa", pltpu.VMEM((64, 8, HD), F32))
    for name, (n, _) in GATHERS.items():
        add(name, pltpu.VMEM((2, 4, 5, n, HD), F32))
        add(name + "_s", dma(11))
        add(name + "_q", dma(10))
    add("sa_s", dma(1))
    add("sa_q", dma(1))
    add("w12", pltpu.VMEM((2, HD, HD), F32))
    add("aux", pltpu.VMEM((8, HD), F32))
    add("w_out_x", pltpu.VMEM((HD + 8, HD), F32))
    add("w_in_x", pltpu.VMEM((HD + 8, HD), F32))
    add("l_s", dma(2))
    add("x_s", dma(2 * PARTS))
    add("x_q", dma(2 * PARTS))
    add("y_s", dma(1))
    add("y_q", dma(1))
    add("none", dma(1))
    return pl.pallas_call(
        functools.partial(kernel, tokens, names),
        out_shape=(
            pltpu.VMEM((2, HEADS, HD, HD), F32),
            pltpu.VMEM((2, HEADS), F32),
        ),
        in_specs=[pl.BlockSpec(memory_space=pltpu.HBM)] * 2,
        out_specs=[pl.BlockSpec(memory_space=pltpu.VMEM)] * 2,
        scratch_shapes=scratch,
        compiler_params=pltpu.CompilerParams(
            collective_id=0, has_side_effects=True, vmem_limit_bytes=VMEM_LIMIT
        ),
    )(
        pltpu.with_memory_space_constraint(first_acts, pltpu.HBM),
        pltpu.with_memory_space_constraint(second_acts, pltpu.HBM),
    )


PIECES = 4


def store_kernel(w, sim, w_hbm, s_hbm, sems):
    step = HEADS // PIECES
    copies = [
        pltpu.make_async_copy(
            w.at[n, pl.ds(q * step, step)], w_hbm.at[n, 0, pl.ds(q * step, step)], sems.at[n * PIECES + q]
        )
        for n in range(2)
        for q in range(PIECES)
    ]
    copies.append(pltpu.make_async_copy(sim, s_hbm.at[0], sems.at[2 * PIECES]))
    for copy in copies:
        copy.start()
    for copy in copies:
        copy.wait()


def store(w, sim):
    vmem, hbm = pl.BlockSpec(memory_space=pltpu.VMEM), pl.BlockSpec(memory_space=pltpu.HBM)
    return pl.pallas_call(
        store_kernel,
        out_shape=(
            jax.ShapeDtypeStruct((2, 1, HEADS, HD, HD), F32),
            jax.ShapeDtypeStruct((1, 2, HEADS), F32),
        ),
        in_specs=[vmem] * 2,
        out_specs=(hbm, hbm),
        scratch_shapes=[pltpu.SemaphoreType.DMA((2 * PIECES + 1,))],
        compiler_params=pltpu.CompilerParams(vmem_limit_bytes=16 * 2**20),
    )(w, sim)


def solution(mesh):
    def whole(first_acts, second_acts):
        tokens = first_acts.shape[1] * lax.axis_size("tok")
        return store(*gather_kernel(tokens, first_acts, second_acts))

    in_specs = (P("lay", "tok", None), P("lay", "tok", None))
    out_specs = (P(None, "lay", None, None, None), P("lay", None, None))
    return jax.shard_map(whole, mesh=mesh, in_specs=in_specs, out_specs=out_specs, check_vma=False)
```

```python
import functools

import jax
import jax.numpy as jnp
from jax import lax
from jax.experimental import pallas as pl
from jax.experimental.pallas import tpu as pltpu
from jax.sharding import PartitionSpec as P

HEADS = 40
HD = 128
ITERS = 6
RIDGE = 0.05
HALF = HEADS // 2
PARTS = 5
FROM_HBM = 3
BATCHES = (14, 21, 32)
VMEM_LIMIT = 48 * 2**20
F32 = jnp.float32
HI = lax.Precision.HIGHEST
MESH = pl.DeviceIdType.MESH

CHAINS = {"pa": (72, "z"), "pb": (64, "y"), "ca": (64, "z"), "cb": (64, "y")}
LATE = {"da": "z", "db": "y"}
GATHERS = {"wa": (72, "z"), "wb": (64, "y")}


def iota(shape, dim):
    return lax.broadcasted_iota(jnp.int32, shape, dim)


def dot_t(a, b, precision=None):
    return lax.dot_general(
        a, b, (((0,), (0,)), ((), ())), precision=precision, preferred_element_type=F32
    )


def mm(a, b):
    return jnp.dot(a, b, precision=HI, preferred_element_type=F32)


def masks():
    ri, ci = iota((HD, HD), 0), iota((HD, HD), 1)
    return ri <= ci, ri == ci


def unpack(top, low, aux):
    upper, diag = masks()
    p = jnp.concatenate([top, low], axis=0)
    pt = p.T
    first = jnp.where(upper, p, pt)
    second = jnp.where(upper, jnp.where(diag, aux[2:3, :], pt), p)
    return first, second


def head_of(z, p):
    k = 4 * ((z + p) % 4) + z
    if isinstance(p, int):
        return 16 + z if p == 4 else k
    return jnp.where(p == 4, 16 + z, k)


def places(h):
    k = h % HALF
    z = k % 4
    y = jnp.where(k < 16, k // 4, z)
    p = jnp.where(k < 16, (k // 4 - z + 4) % 4, 4)
    return h // HALF, z, y, p


def kernel(tokens, names, *refs):
    r = dict(zip(names, refs))
    tok = lax.axis_index("tok")
    lay = lax.axis_index("lay")
    c = tok % 2
    xh = (tok // 2) % 2
    y = (tok // 4) % 4
    z = tok // 16

    def dev(z_, y_, xh_, c_):
        return (((z_ * 4 + y_) * 2 + xh_) * 2 + c_, lay)

    def uv(axis):
        return (z, y) if axis == "z" else (y, z)

    def dev_uv(axis, u, v, xh_):
        return dev(u, v, xh_, c) if axis == "z" else dev(v, u, xh_, c)

    sibling = dev(z, y, xh, 1 - c)
    twin = (tok, 1 - lay)
    far = dev(z, y, 1 - xh, c)

    on_diag = z == y
    main = (y - z + 4) % 4
    owns_main = xh == main % 2
    owner = jnp.logical_or(owns_main, on_diag)
    own = jnp.where(owns_main, main, 4)
    late_owner = jnp.logical_and(on_diag, xh == 1)
    early_owner = owns_main
    extra_mine = jnp.where(owns_main, 0, 1)
    extra_give = jnp.where(owns_main, 1, 0)
    gives = jnp.logical_or(on_diag, jnp.logical_not(owns_main))
    no = jnp.logical_not

    def target(axis, p):
        u, _ = uv(axis)
        if p == 4:
            return u
        return (u + p) % 4 if axis == "z" else (u - p + 4) % 4

    def rcopy(src, dst, ssem, rsem, device):
        return pltpu.make_async_remote_copy(
            src_ref=src, dst_ref=dst, send_sem=ssem, recv_sem=rsem,
            device_id=device, device_id_type=MESH,
        )

    others = lax.axis_size("tok") - 1
    pending = []

    def launch(copy, cond=None):
        pending.append((cond, copy))
        if cond is None:
            copy.start()
        else:
            pl.when(cond)(lambda: copy.start())

    def arrive(ref, sem, cond=None):
        copy = rcopy(ref, ref, r["none"].at[0], sem, twin)
        if cond is None:
            copy.wait_recv()
        else:
            pl.when(cond)(lambda: copy.wait_recv())

    def loop(n, body, unroll=1):
        def step(i, carry):
            body(i)
            return carry

        lax.fori_loop(0, n, step, 0, unroll=unroll)

    def s1(name):
        launch(rcopy(r[name].at[1 - c], r[name + "_r1"], r[name + "_s"].at[0], r[name + "_q"].at[0], sibling))

    def s1_sum(name):
        buf, r1 = r[name], r[name + "_r1"]
        arrive(r1, r[name + "_q"].at[0])

        def body(i):
            for s in range(5):
                buf[c, i, s] = buf[c, i, s] + r1[i, s]

        loop(4, body)

    def s2(name):
        axis = CHAINS[name][1]
        u, v = uv(axis)
        for d in (1, 3, 2):
            to = (u + d) % 4
            launch(
                rcopy(
                    r[name].at[c, to], r[name + "_r2"].at[d - 1], r[name + "_s"].at[d],
                    r[name + "_q"].at[d], dev_uv(axis, to, v, xh),
                )
            )

    def s2_sum(name):
        u, _ = uv(CHAINS[name][1])
        buf, r2, acc = r[name], r[name + "_r2"], r[name + "_acc"]
        for d in (1, 2, 3):
            arrive(r2.at[d - 1], r[name + "_q"].at[d])
        for s in range(5):
            acc[s] = (buf[c, u, s] + r2[0, s]) + (r2[1, s] + r2[2, s])

    def s3(name, axis, slots):
        u, v = uv(axis)
        for p in slots:
            vo = target(axis, p)
            off = jnp.maximum((v - vo + 4) % 4, 1) - 1
            kind = p // 4
            launch(
                rcopy(
                    r[name + "_acc"].at[p], r[name + "_r3"].at[kind, off], r[name + "_s"].at[4 + p],
                    r[name + "_q"].at[4 + kind * 3 + off], dev_uv(axis, u, vo, xh),
                ),
                v != vo,
            )

    def s3_sum(name, extra):
        acc, r3, part = r[name + "_acc"], r[name + "_r3"], r[name + "_t"]

        def add(kind, slot):
            for off in range(3):
                arrive(r3.at[kind, off], r[name + "_q"].at[4 + kind * 3 + off])
            part[kind] = (acc[slot] + r3[kind, 0]) + (r3[kind, 1] + r3[kind, 2])

        add(0, main)
        if extra:
            pl.when(on_diag)(lambda: add(1, 4))

    def s4(name, extra):
        src = r[name + "_t"].at[extra_give] if extra else r[name + "_t"].at[0]
        cond = gives if extra else no(owns_main)
        launch(rcopy(src, r[name + "_r4"], r[name + "_s"].at[9], r[name + "_q"].at[10], far), cond)

    def s4_total(name, extra):
        arrive(r[name + "_r4"], r[name + "_q"].at[10])
        mine = r[name + "_t"][extra_mine] if extra else r[name + "_t"][0]
        return mine + r[name + "_r4"][...]

    def g1(name):
        u, _ = uv(GATHERS[name][1])
        place = r[name].at[c, u, own]
        rcopy(place, place, r[name + "_s"].at[0], r[name + "_q"].at[0], far).start()

    def g1_arrive(name):
        u, _ = uv(GATHERS[name][1])
        arrive(r[name].at[c, u, jnp.where(owns_main, 4, main)], r[name + "_q"].at[0], gives)

    def g2(name):
        axis = GATHERS[name][1]
        u, v = uv(axis)
        for d in (1, 3, 2):
            for kind in (0, 1):
                slot = 4 if kind else main
                place = r[name].at[c, u, slot]
                launch(
                    rcopy(
                        place, place, r[name + "_s"].at[kind * 3 + d], r[name + "_q"].at[1 + slot],
                        dev_uv(axis, u, (v + d) % 4, xh),
                    ),
                    on_diag if kind else None,
                )

    def g2_arrive(name):
        axis = GATHERS[name][1]
        u, v = uv(axis)
        for p in range(5):
            arrive(r[name].at[c, u, p], r[name + "_q"].at[1 + p], v != target(axis, p))

    def g3(name):
        axis = GATHERS[name][1]
        u, v = uv(axis)
        place = r[name].at[c, u]
        for d in (1, 3, 2):
            launch(
                rcopy(
                    place, place, r[name + "_s"].at[6 + d], r[name + "_q"].at[5 + d],
                    dev_uv(axis, (u + d) % 4, v, xh),
                )
            )

    def g3_arrive(name):
        u, _ = uv(GATHERS[name][1])
        for d in (1, 2, 3):
            arrive(r[name].at[c, (u - d + 4) % 4], r[name + "_q"].at[5 + d])

    def g4(name):
        place = r[name].at[c]
        launch(rcopy(place, place, r[name + "_s"].at[10], r[name + "_q"].at[9], sibling))

    def g4_arrive(name):
        arrive(r[name].at[1 - c], r[name + "_q"].at[9])

    x1, x2, x2o = r["x1"], r["x2"], r["x2o"]

    def part_head(p, j):
        half = (1 - c) if j < 4 else c
        return half, j % 4, half * HALF + head_of(j % 4, p)

    def last_head(z_, c_):
        return c_ * HALF + 16 + z_

    def columns(h):
        return pl.ds(pl.multiple_of(h * HD, HD), HD)

    def exchange(lo, hi):
        for n in range(lo, hi):
            p, j = n // 8, n % 8
            _, _, h = part_head(p, j)
            src = r["x2_hbm"].at[0, :, columns(h)] if n < FROM_HBM else x2.at[:, columns(h)]
            if p == 4:
                src = x2.at[:, columns(last_head(z, c))] if j == 0 else r["m2"].at[j - 1]
            sem = 2 * p + j // 4
            rcopy(src, x2o.at[p, j], r["x_s"].at[sem], r["x_q"].at[sem], twin).start()

    def collect():
        for dz in (1, 3, 2, 0):
            for dc in (0, 1):
                j = 2 * dz + dc
                if j:
                    z_, c_ = (z + dz) % 4, (c + dc) % 2
                    cols = columns(last_head(z_, c_))
                    for n, x in ((1, x2), (0, x1)):
                        launch(
                            rcopy(
                                x.at[:, cols], r["m%d" % (n + 1)].at[j - 1], r["m_s"].at[7 * n + j - 1],
                                r["m_q"].at[7 * n + j - 1], dev(z_, y, xh, c_),
                            )
                        )

    def collected(n):
        for j in range(1, 8):
            arrive(r["m%d" % (n + 1)].at[j - 1], r["m_q"].at[7 * n + j - 1])

    def last_cross(which):
        arrive(x2o.at[4, pl.ds(4 * which, 4)], r["x_q"].at[8 + which])
        total = None
        for j in range(4 * which, 4 * which + 4):
            left = r["m1"][j - 1] if j else x1[:, columns(last_head(z, c))]
            cr = dot_t(left, x2o[4, j])
            total = cr if total is None else total + cr
        r["d4"][...] = r["d4"][...] + total if which else total

    load1 = pltpu.make_async_copy(r["x1_hbm"].at[0], x1, r["l_s"].at[0])
    load2 = pltpu.make_async_copy(r["x2_hbm"].at[0], x2, r["l_s"].at[1])
    load2.start()
    load1.start()
    barrier = pltpu.get_barrier_semaphore()
    peers = [sibling, twin, far]
    for d in range(1, 4):
        peers.append(dev((z + d) % 4, y, xh, c))
        peers.append(dev(z, (y + d) % 4, xh, c))
    for peer in peers:
        pl.semaphore_signal(barrier, inc=1, device_id=peer, device_id_type=MESH)
    pl.semaphore_wait(barrier, len(peers))
    exchange(0, FROM_HBM)
    load2.wait()
    exchange(FROM_HBM, BATCHES[0])
    load1.wait()

    upper, diag = masks()
    eye = jnp.where(diag, 1.0, 0.0).astype(F32)
    row8 = iota((8, HD), 0)

    def gram(h):
        ch, zz, yy, p = places(h)
        cols = columns(h)
        ab = jnp.concatenate([x1[:, cols], x2[:, cols]], axis=1)
        g = dot_t(ab, ab)
        sums = jnp.dot(jnp.ones((8, ab.shape[0]), ab.dtype), ab, preferred_element_type=F32)
        g1_, cr, g2_ = g[:HD, :HD], g[:HD, HD:], g[HD:, HD:]
        packed = jnp.where(upper, g1_, g2_)
        dg = jnp.sum(jnp.where(diag, g2_, 0.0), axis=0, keepdims=True)
        aux = jnp.where(
            row8 == 0, sums[:, :HD],
            jnp.where(row8 == 1, sums[:, HD:], jnp.where(row8 == 2, jnp.broadcast_to(dg, (8, HD)), 0.0)),
        )
        r["pa"][ch, zz, p, 0:64] = packed[:64]
        r["pa"][ch, zz, p, 64:72] = aux
        r["pb"][ch, yy, p] = packed[64:]
        r["ca"][ch, zz, p] = cr[:64]
        r["cb"][ch, yy, p] = cr[64:]

    def cross(p, which):
        arrive(x2o.at[p, pl.ds(4 * which, 4)], r["x_q"].at[2 * p + which])
        for j in range(4 * which, 4 * which + 4):
            half, zz, h = part_head(p, j)
            yy = (zz + p) % 4
            cr = dot_t(x1[:, columns(h)], x2o[p, j])
            r["da"][p, half, zz] = cr[:64]
            r["db"][p, half, yy] = cr[64:]
            if j == 3:
                for name in LATE:
                    launch(
                        rcopy(
                            r[name].at[p, 1 - c], r[name + "_r1"].at[p], r[name + "_s"].at[p],
                            r[name + "_q"].at[p], sibling,
                        )
                    )

    def cross_s2(p):
        for name, axis in LATE.items():
            buf, r1 = r[name], r[name + "_r1"]
            u, v = uv(axis)
            arrive(r1.at[p], r[name + "_q"].at[p])
            for i in range(4):
                buf[p, c, i] = buf[p, c, i] + r1[p, i]
            for d in (1, 3, 2):
                to = (u + d) % 4
                launch(
                    rcopy(
                        buf.at[p, c, to], r[name + "_r2"].at[p, d - 1], r[name + "_s"].at[2 + 3 * (p + 1) + d - 1],
                        r[name + "_q"].at[2 + 3 * (p + 1) + d - 1], dev_uv(axis, to, v, xh),
                    )
                )

    def cross_s2_sum(p):
        for name, axis in LATE.items():
            buf, r2 = r[name], r[name + "_r2"]
            u, _ = uv(axis)
            for d in (1, 2, 3):
                arrive(r2.at[p, d - 1], r[name + "_q"].at[2 + 3 * (p + 1) + d - 1])
            r[name + "x_acc"][p] = (buf[p, c, u] + r2[p, 0]) + (r2[p, 1] + r2[p, 2])

    def last_s3():
        slot = ((y - z + 4) % 4) * 2 + 1 - xh
        launch(
            rcopy(r["d4"], r["r5"].at[slot], r["d4_s"].at[0], r["d4_q"].at[slot], dev(z, z, 1, c)),
            no(late_owner),
        )

    def last_total():
        for slot in range(1, 8):
            arrive(r["r5"].at[slot], r["d4_q"].at[slot])
        total = r["d4"][...] + r["r5"][1]
        for slot in range(2, 8):
            total = total + r["r5"][slot]
        return total

    def only_row0(row):
        return jnp.where(row8 == 0, jnp.broadcast_to(row, (8, HD)), 0.0)

    def mean_term(sums):
        mean1 = only_row0(r["aux"][0:1, :]) / tokens
        return dot_t(mean1, only_row0(sums) / tokens, HI)

    def similarity(raw, means, w2):
        white = mm(mm(r["w12"][0], raw / tokens - means), w2)
        sq = jnp.sum(jnp.sum(white * white, axis=1, keepdims=True), axis=0, keepdims=True)
        return jnp.broadcast_to(sq / HD, (8, HD))

    def whiten():
        top = s4_total("pa", True)
        low = s4_total("pb", True)
        aux = top[64:72]
        grams = unpack(top[:64], low, aux)
        ys, zs, scales = [], [], []
        for n in (0, 1):
            mean = only_row0(aux[n : n + 1, :]) / tokens
            cov = grams[n] / tokens - dot_t(mean, mean, HI) + RIDGE * eye
            sq = jnp.sum(jnp.sum(cov * cov, axis=1, keepdims=True), axis=0, keepdims=True)
            scale = jnp.sqrt(sq)
            scales.append(scale)
            ys.append(cov / scale)
        for it in range(ITERS):
            for n in (0, 1):
                if it == 0:
                    f = 1.5 * eye - 0.5 * ys[n]
                    zs.append(f)
                else:
                    f = 1.5 * eye - 0.5 * mm(zs[n], ys[n])
                    zs[n] = mm(f, zs[n])
                if it < ITERS - 1:
                    ys[n] = mm(ys[n], f)
        w1 = zs[0] / jnp.sqrt(scales[0])
        w2 = zs[1] / jnp.sqrt(scales[1])
        wp = jnp.where(upper, w1, w2)
        wd = jnp.sum(jnp.where(diag, w2, 0.0), axis=0, keepdims=True)
        r["wa"][c, z, own, 0:64] = wp[:64]
        r["wa"][c, z, own, 64:72] = jnp.broadcast_to(wd, (8, HD))
        r["wb"][c, y, own] = wp[64:]
        g1("wa")
        g1("wb")
        r["w12"][0] = w1
        r["w12"][1] = w2
        r["aux"][...] = aux
        r["w_out_x"][0:HD] = w2
        r["w_out_x"][HD : HD + 8] = aux
    def both(p):
        cross(p, 0)
        cross(p, 1)

    loop(HALF, lambda i: gram((1 - c) * HALF + i), unroll=2)
    for name in CHAINS:
        s1(name)
    loop(HALF, lambda i: gram(c * HALF + i), unroll=2)
    for name in ("pa", "pb"):
        s1_sum(name)
        s2(name)
    for name in ("ca", "cb"):
        s1_sum(name)
    both(0)
    for name in ("pa", "pb"):
        s2_sum(name)
        s3(name, CHAINS[name][1], range(5))
    collect()
    for name in ("pa", "pb"):
        s3_sum(name, True)
        s4(name, True)
    exchange(BATCHES[0], BATCHES[1])
    for name in ("ca", "cb"):
        s2(name)
    pl.when(owner)(whiten)
    exchange(BATCHES[1], BATCHES[2])
    for name in GATHERS:
        g1_arrive(name)
        g2(name)
    both(1)
    cross_s2(0)
    for name in ("ca", "cb"):
        s2_sum(name)
        s3(name, CHAINS[name][1], range(5))
    for name in GATHERS:
        g2_arrive(name)
        g3(name)
    collected(1)
    exchange(BATCHES[2], 8 * PARTS)
    for name in ("ca", "cb"):
        s3_sum(name, True)
        s4(name, True)

    @pl.when(owner)
    def _():
        rcopy(r["w_out_x"], r["w_in_x"], r["y_s"].at[0], r["y_q"].at[0], twin).start()

    cross_s2(1)
    both(2)
    cross_s2_sum(0)

    lane_head = c * HALF + jnp.where(own == 4, 16 + z, head_of(z, own))
    here = iota((8, HD), 1) == lane_head
    sa_mine = r["sa"].at[(c * 4 + z) * 5 + own]

    def own_similarity():
        raw = jnp.concatenate([s4_total("ca", True), s4_total("cb", True)], axis=0)
        sim = similarity(raw, mean_term(r["aux"][1:2, :]), r["w12"][1])
        sa_mine[...] = jnp.where(jnp.logical_and(here, row8 == lay), sim, 0.0)
        arrive(r["w_in_x"], r["y_q"].at[0])
        r["means"][...] = mean_term(r["w_in_x"][HD + 1 : HD + 2])

    def other_similarity(raw):
        sim = similarity(raw, r["means"][...], r["w_in_x"][0:HD])
        sa_mine[...] = jnp.where(jnp.logical_and(here, row8 == 1 - lay), sim, sa_mine[...])

        def send(i):
            to = (tok + 1 + (25 + i) % others) % (others + 1)
            rcopy(sa_mine, sa_mine, r["sa_s"].at[0], r["sa_q"].at[0], (to, lay)).start()

        loop(others, send, unroll=9)

    def emit(h):
        ch, zz, yy, p = places(h)
        w1, w2 = unpack(r["wa"][ch, zz, p, 0:64], r["wb"][ch, yy, p], r["wa"][ch, zz, p, 64:72])
        r["w"][0, h] = w1
        r["w"][1, h] = w2

    cross_s2(2)
    cross_s2_sum(1)
    for name in GATHERS:
        g3_arrive(name)
        g4(name)
    both(3)
    cross_s2_sum(2)
    cross_s2(3)
    for name in GATHERS:
        g4_arrive(name)
    loop(HEADS, emit, unroll=2)
    cross_s2_sum(3)
    for name, axis in LATE.items():
        s3(name + "x", axis, range(4))
    collected(0)
    last_cross(0)
    last_cross(1)
    last_s3()
    for name in LATE:
        s3_sum(name + "x", False)
        s4(name + "x", False)
    pl.when(owner)(own_similarity)

    @pl.when(early_owner)
    def _():
        other_similarity(jnp.concatenate([s4_total("dax", False), s4_total("dbx", False)], axis=0))

    @pl.when(late_owner)
    def _():
        other_similarity(last_total())

    pl.when(owner)(lambda: arrive(r["sa"].at[pl.ds(0, HEADS - 1)], r["sa_q"].at[0]))
    pl.when(no(owner))(lambda: arrive(r["sa"].at[pl.ds(0, HEADS)], r["sa_q"].at[0]))
    total = r["sa"][0]
    for i in range(1, HEADS):
        total = total + r["sa"][i]
    r["sim"][...] = total[0:2, 0:HEADS]

    for cond, copy in pending:
        if cond is None:
            copy.wait_send()
        else:
            pl.when(cond)(lambda copy=copy: copy.wait_send())
    for i in range(2 * PARTS):
        part = x2o.at[i // 2, pl.ds(4 * (i % 2), 4)]
        rcopy(part, part, r["x_s"].at[i], r["x_q"].at[i], twin).wait_send()

    @pl.when(owner)
    def _():
        for name in GATHERS:
            u, _ = uv(GATHERS[name][1])
            place = r[name].at[c, u, own]
            rcopy(place, place, r[name + "_s"].at[0], r[name + "_q"].at[0], far).wait_send()
        rcopy(r["w_out_x"], r["w_in_x"], r["y_s"].at[0], r["y_q"].at[0], twin).wait_send()
        sent = r["sa"].at[pl.ds(0, others)]
        rcopy(sent, sent, r["sa_s"].at[0], r["sa_q"].at[0], far).wait_send()


def gather_kernel(tokens, first_acts, second_acts):
    rows, width = first_acts.shape[1:]
    names = ["x1_hbm", "x2_hbm", "w", "sim"]
    scratch = []

    def add(name, spec):
        names.append(name)
        scratch.append(spec)

    dma = lambda n: pltpu.SemaphoreType.DMA((n,))
    for name in ("x1", "x2"):
        add(name, pltpu.VMEM((rows, width), first_acts.dtype))
    add("x2o", pltpu.VMEM((PARTS, 8, rows, HD), first_acts.dtype))
    for name, (n, _) in CHAINS.items():
        add(name, pltpu.VMEM((2, 4, 5, n, HD), F32))
        add(name + "_r1", pltpu.VMEM((4, 5, n, HD), F32))
        add(name + "_r2", pltpu.VMEM((3, 5, n, HD), F32))
    for name in LATE:
        add(name, pltpu.VMEM((PARTS - 1, 2, 4, 64, HD), F32))
        add(name + "_r1", pltpu.VMEM((PARTS - 1, 4, 64, HD), F32))
        add(name + "_r2", pltpu.VMEM((PARTS - 1, 3, 64, HD), F32))
        add(name + "_s", dma(17))
        add(name + "_q", dma(17))
    for name in ("m1", "m2"):
        add(name, pltpu.VMEM((7, rows, HD), first_acts.dtype))
    add("m_s", dma(14))
    add("m_q", dma(14))
    add("d4", pltpu.VMEM((HD, HD), F32))
    add("r5", pltpu.VMEM((8, HD, HD), F32))
    add("d4_s", dma(1))
    add("d4_q", dma(8))
    add("means", pltpu.VMEM((HD, HD), F32))
    for name, n in [(k, v[0]) for k, v in CHAINS.items()] + [(k + "x", 64) for k in LATE]:
        add(name + "_acc", pltpu.VMEM((5, n, HD), F32))
        add(name + "_r3", pltpu.VMEM((2, 3, n, HD), F32))
        add(name + "_t", pltpu.VMEM((2, n, HD), F32))
        add(name + "_r4", pltpu.VMEM((n, HD), F32))
        add(name + "_s", dma(10))
        add(name + "_q", dma(11))
    add("sa", pltpu.VMEM((64, 8, HD), F32))
    for name, (n, _) in GATHERS.items():
        add(name, pltpu.VMEM((2, 4, 5, n, HD), F32))
        add(name + "_s", dma(11))
        add(name + "_q", dma(10))
    add("sa_s", dma(1))
    add("sa_q", dma(1))
    add("w12", pltpu.VMEM((2, HD, HD), F32))
    add("aux", pltpu.VMEM((8, HD), F32))
    add("w_out_x", pltpu.VMEM((HD + 8, HD), F32))
    add("w_in_x", pltpu.VMEM((HD + 8, HD), F32))
    add("l_s", dma(2))
    add("x_s", dma(2 * PARTS))
    add("x_q", dma(2 * PARTS))
    add("y_s", dma(1))
    add("y_q", dma(1))
    add("none", dma(1))
    return pl.pallas_call(
        functools.partial(kernel, tokens, names),
        out_shape=(
            pltpu.VMEM((2, HEADS, HD, HD), F32),
            pltpu.VMEM((2, HEADS), F32),
        ),
        in_specs=[pl.BlockSpec(memory_space=pltpu.HBM)] * 2,
        out_specs=[pl.BlockSpec(memory_space=pltpu.VMEM)] * 2,
        scratch_shapes=scratch,
        compiler_params=pltpu.CompilerParams(
            collective_id=0, has_side_effects=True, vmem_limit_bytes=VMEM_LIMIT
        ),
    )(
        pltpu.with_memory_space_constraint(first_acts, pltpu.HBM),
        pltpu.with_memory_space_constraint(second_acts, pltpu.HBM),
    )


PIECES = 4


def store_kernel(w, sim, w_hbm, s_hbm, sems):
    step = HEADS // PIECES
    copies = [
        pltpu.make_async_copy(
            w.at[n, pl.ds(q * step, step)], w_hbm.at[n, 0, pl.ds(q * step, step)], sems.at[n * PIECES + q]
        )
        for n in range(2)
        for q in range(PIECES)
    ]
    copies.append(pltpu.make_async_copy(sim, s_hbm.at[0], sems.at[2 * PIECES]))
    for copy in copies:
        copy.start()
    for copy in copies:
        copy.wait()


def store(w, sim):
    vmem, hbm = pl.BlockSpec(memory_space=pltpu.VMEM), pl.BlockSpec(memory_space=pltpu.HBM)
    return pl.pallas_call(
        store_kernel,
        out_shape=(
            jax.ShapeDtypeStruct((2, 1, HEADS, HD, HD), F32),
            jax.ShapeDtypeStruct((1, 2, HEADS), F32),
        ),
        in_specs=[vmem] * 2,
        out_specs=(hbm, hbm),
        scratch_shapes=[pltpu.SemaphoreType.DMA((2 * PIECES + 1,))],
        compiler_params=pltpu.CompilerParams(vmem_limit_bytes=16 * 2**20),
    )(w, sim)


def solution(mesh):
    def whole(first_acts, second_acts):
        tokens = first_acts.shape[1] * lax.axis_size("tok")
        return store(*gather_kernel(tokens, first_acts, second_acts))

    in_specs = (P("lay", "tok", None), P("lay", "tok", None))
    out_specs = (P(None, "lay", None, None, None), P("lay", None, None))
    return jax.shard_map(whole, mesh=mesh, in_specs=in_specs, out_specs=out_specs, check_vma=False)
```

```python
import functools

import jax
import jax.numpy as jnp
from jax import lax
from jax.experimental import pallas as pl
from jax.experimental.pallas import tpu as pltpu
from jax.sharding import PartitionSpec as P

HEADS = 40
HD = 128
ITERS = 6
RIDGE = 0.05
HALF = HEADS // 2
PARTS = 5
FROM_HBM = 3
BATCHES = (14, 21, 32)
VMEM_LIMIT = 48 * 2**20
F32 = jnp.float32
HI = lax.Precision.HIGHEST
MESH = pl.DeviceIdType.MESH

CHAINS = {"pa": (72, "z"), "pb": (64, "y"), "ca": (64, "z"), "cb": (64, "y")}
LATE = {"da": "z", "db": "y"}
GATHERS = {"wa": (72, "z"), "wb": (64, "y")}


def iota(shape, dim):
    return lax.broadcasted_iota(jnp.int32, shape, dim)


def dot_t(a, b, precision=None):
    return lax.dot_general(
        a, b, (((0,), (0,)), ((), ())), precision=precision, preferred_element_type=F32
    )


def mm(a, b):
    return jnp.dot(a, b, precision=HI, preferred_element_type=F32)


def masks():
    ri, ci = iota((HD, HD), 0), iota((HD, HD), 1)
    return ri <= ci, ri == ci


def unpack(top, low, aux):
    upper, diag = masks()
    p = jnp.concatenate([top, low], axis=0)
    pt = p.T
    first = jnp.where(upper, p, pt)
    second = jnp.where(upper, jnp.where(diag, aux[2:3, :], pt), p)
    return first, second


def head_of(z, p):
    k = 4 * ((z + p) % 4) + z
    if isinstance(p, int):
        return 16 + z if p == 4 else k
    return jnp.where(p == 4, 16 + z, k)


def places(h):
    k = h % HALF
    z = k % 4
    y = jnp.where(k < 16, k // 4, z)
    p = jnp.where(k < 16, (k // 4 - z + 4) % 4, 4)
    return h // HALF, z, y, p


def kernel(tokens, names, *refs):
    r = dict(zip(names, refs))
    tok = lax.axis_index("tok")
    lay = lax.axis_index("lay")
    c = tok % 2
    xh = (tok // 2) % 2
    y = (tok // 4) % 4
    z = tok // 16

    def dev(z_, y_, xh_, c_):
        return (((z_ * 4 + y_) * 2 + xh_) * 2 + c_, lay)

    def uv(axis):
        return (z, y) if axis == "z" else (y, z)

    def dev_uv(axis, u, v, xh_):
        return dev(u, v, xh_, c) if axis == "z" else dev(v, u, xh_, c)

    sibling = dev(z, y, xh, 1 - c)
    twin = (tok, 1 - lay)
    far = dev(z, y, 1 - xh, c)

    on_diag = z == y
    main = (y - z + 4) % 4
    owns_main = xh == main % 2
    owner = jnp.logical_or(owns_main, on_diag)
    own = jnp.where(owns_main, main, 4)
    late_owner = jnp.logical_and(on_diag, xh == 1)
    early_owner = owns_main
    extra_mine = jnp.where(owns_main, 0, 1)
    extra_give = jnp.where(owns_main, 1, 0)
    gives = jnp.logical_or(on_diag, jnp.logical_not(owns_main))
    no = jnp.logical_not

    def target(axis, p):
        u, _ = uv(axis)
        if p == 4:
            return u
        return (u + p) % 4 if axis == "z" else (u - p + 4) % 4

    def rcopy(src, dst, ssem, rsem, device):
        return pltpu.make_async_remote_copy(
            src_ref=src, dst_ref=dst, send_sem=ssem, recv_sem=rsem,
            device_id=device, device_id_type=MESH,
        )

    others = lax.axis_size("tok") - 1
    pending = []

    def launch(copy, cond=None):
        pending.append((cond, copy))
        if cond is None:
            copy.start()
        else:
            pl.when(cond)(lambda: copy.start())

    def arrive(ref, sem, cond=None):
        copy = rcopy(ref, ref, r["none"].at[0], sem, twin)
        if cond is None:
            copy.wait_recv()
        else:
            pl.when(cond)(lambda: copy.wait_recv())

    def loop(n, body, unroll=1):
        def step(i, carry):
            body(i)
            return carry

        lax.fori_loop(0, n, step, 0, unroll=unroll)

    def s1(name):
        launch(rcopy(r[name].at[1 - c], r[name + "_r1"], r[name + "_s"].at[0], r[name + "_q"].at[0], sibling))

    def s1_sum(name):
        buf, r1 = r[name], r[name + "_r1"]
        arrive(r1, r[name + "_q"].at[0])

        def body(i):
            for s in range(5):
                buf[c, i, s] = buf[c, i, s] + r1[i, s]

        loop(4, body)

    def s2(name, offsets=(1, 3, 2)):
        axis = CHAINS[name][1]
        u, v = uv(axis)
        for d in offsets:
            to = (u + d) % 4
            launch(
                rcopy(
                    r[name].at[c, to], r[name + "_r2"].at[d - 1], r[name + "_s"].at[d],
                    r[name + "_q"].at[d], dev_uv(axis, to, v, xh),
                )
            )

    def s2_sum(name):
        u, _ = uv(CHAINS[name][1])
        buf, r2, acc = r[name], r[name + "_r2"], r[name + "_acc"]
        for d in (1, 2, 3):
            arrive(r2.at[d - 1], r[name + "_q"].at[d])
        for s in range(5):
            acc[s] = (buf[c, u, s] + r2[0, s]) + (r2[1, s] + r2[2, s])

    def s3(name, axis, slots):
        u, v = uv(axis)
        for p in slots:
            vo = target(axis, p)
            off = jnp.maximum((v - vo + 4) % 4, 1) - 1
            kind = p // 4
            launch(
                rcopy(
                    r[name + "_acc"].at[p], r[name + "_r3"].at[kind, off], r[name + "_s"].at[4 + p],
                    r[name + "_q"].at[4 + kind * 3 + off], dev_uv(axis, u, vo, xh),
                ),
                v != vo,
            )

    def s3_sum(name, extra):
        acc, r3, part = r[name + "_acc"], r[name + "_r3"], r[name + "_t"]

        def add(kind, slot):
            for off in range(3):
                arrive(r3.at[kind, off], r[name + "_q"].at[4 + kind * 3 + off])
            part[kind] = (acc[slot] + r3[kind, 0]) + (r3[kind, 1] + r3[kind, 2])

        add(0, main)
        if extra:
            pl.when(on_diag)(lambda: add(1, 4))

    def s4(name, extra):
        src = r[name + "_t"].at[extra_give] if extra else r[name + "_t"].at[0]
        cond = gives if extra else no(owns_main)
        launch(rcopy(src, r[name + "_r4"], r[name + "_s"].at[9], r[name + "_q"].at[10], far), cond)

    def s4_total(name, extra):
        arrive(r[name + "_r4"], r[name + "_q"].at[10])
        mine = r[name + "_t"][extra_mine] if extra else r[name + "_t"][0]
        return mine + r[name + "_r4"][...]

    def g1(name):
        u, _ = uv(GATHERS[name][1])
        place = r[name].at[c, u, own]
        rcopy(place, place, r[name + "_s"].at[0], r[name + "_q"].at[0], far).start()

    def g1_arrive(name):
        u, _ = uv(GATHERS[name][1])
        arrive(r[name].at[c, u, jnp.where(owns_main, 4, main)], r[name + "_q"].at[0], gives)

    def g2(name):
        axis = GATHERS[name][1]
        u, v = uv(axis)
        for d in (1, 3, 2):
            for kind in (0, 1):
                slot = 4 if kind else main
                place = r[name].at[c, u, slot]
                launch(
                    rcopy(
                        place, place, r[name + "_s"].at[kind * 3 + d], r[name + "_q"].at[1 + slot],
                        dev_uv(axis, u, (v + d) % 4, xh),
                    ),
                    on_diag if kind else None,
                )

    def g2_arrive(name):
        axis = GATHERS[name][1]
        u, v = uv(axis)
        for p in range(5):
            arrive(r[name].at[c, u, p], r[name + "_q"].at[1 + p], v != target(axis, p))

    def g3(name):
        axis = GATHERS[name][1]
        u, v = uv(axis)
        place = r[name].at[c, u]
        for d in (1, 3, 2):
            launch(
                rcopy(
                    place, place, r[name + "_s"].at[6 + d], r[name + "_q"].at[5 + d],
                    dev_uv(axis, (u + d) % 4, v, xh),
                )
            )

    def g3_arrive(name):
        u, _ = uv(GATHERS[name][1])
        for d in (1, 2, 3):
            arrive(r[name].at[c, (u - d + 4) % 4], r[name + "_q"].at[5 + d])

    def g4(name):
        place = r[name].at[c]
        launch(rcopy(place, place, r[name + "_s"].at[10], r[name + "_q"].at[9], sibling))

    def g4_arrive(name):
        arrive(r[name].at[1 - c], r[name + "_q"].at[9])

    x1, x2, x2o = r["x1"], r["x2"], r["x2o"]

    def part_head(p, j):
        half = (1 - c) if j < 4 else c
        return half, j % 4, half * HALF + head_of(j % 4, p)

    own_last = jnp.where(c == 0, z, y)

    def last_head(z_, c_):
        return c_ * HALF + 16 + z_

    def columns(h):
        return pl.ds(pl.multiple_of(h * HD, HD), HD)

    def exchange(lo, hi):
        for n in range(lo, hi):
            p, j = n // 8, n % 8
            _, _, h = part_head(p, j)
            src = r["x2_hbm"].at[0, :, columns(h)] if n < FROM_HBM else x2.at[:, columns(h)]
            if p == 4:
                src = x2.at[:, columns(last_head(own_last, c))] if j == 0 else r["m2"].at[j - 1]
            sem = 2 * p + j // 4
            rcopy(src, x2o.at[p, j], r["x_s"].at[sem], r["x_q"].at[sem], twin).start()

    def collect():
        for d in (1, 3, 2, 0):
            for c_ in (0, 1):
                if c_ == 0:
                    w_, to, other = (z + d) % 4, dev((z + d) % 4, y, xh, 0), c
                else:
                    w_, to, other = (y + d) % 4, dev(z, (y + d) % 4, xh, 1), 1 - c
                slot = jnp.maximum(2 * d + other, 1) - 1
                cols = columns(last_head(w_, c_))
                for n, x in ((1, x2), (0, x1)):
                    launch(
                        rcopy(
                            x.at[:, cols], r["m%d" % (n + 1)].at[slot], r["m_s"].at[8 * n + 2 * d + c_],
                            r["m_q"].at[7 * n + slot], to,
                        ),
                        None if d else other == 1,
                    )

    def collected(n):
        for j in range(1, 8):
            arrive(r["m%d" % (n + 1)].at[j - 1], r["m_q"].at[7 * n + j - 1])

    def last_cross(which):
        arrive(x2o.at[4, pl.ds(4 * which, 4)], r["x_q"].at[8 + which])
        total = None
        for j in range(4 * which, 4 * which + 4):
            left = r["m1"][j - 1] if j else x1[:, columns(last_head(own_last, c))]
            cr = dot_t(left, x2o[4, j])
            total = cr if total is None else total + cr
        r["d4"][...] = r["d4"][...] + total if which else total

    load1 = pltpu.make_async_copy(r["x1_hbm"].at[0], x1, r["l_s"].at[0])
    load2 = pltpu.make_async_copy(r["x2_hbm"].at[0], x2, r["l_s"].at[1])
    load2.start()
    load1.start()
    barrier = pltpu.get_barrier_semaphore()
    peers = [sibling, twin, far]
    for d in range(1, 4):
        for c_ in (c, 1 - c):
            peers.append(dev((z + d) % 4, y, xh, c_))
            peers.append(dev(z, (y + d) % 4, xh, c_))
    for peer in peers:
        pl.semaphore_signal(barrier, inc=1, device_id=peer, device_id_type=MESH)
    pl.semaphore_wait(barrier, len(peers))
    exchange(0, FROM_HBM)
    load2.wait()
    exchange(FROM_HBM, BATCHES[0])
    load1.wait()
    collect()

    upper, diag = masks()
    eye = jnp.where(diag, 1.0, 0.0).astype(F32)
    row8 = iota((8, HD), 0)

    def gram(h):
        ch, zz, yy, p = places(h)
        cols = columns(h)
        ab = jnp.concatenate([x1[:, cols], x2[:, cols]], axis=1)
        g = dot_t(ab, ab)
        sums = jnp.dot(jnp.ones((8, ab.shape[0]), ab.dtype), ab, preferred_element_type=F32)
        g1_, cr, g2_ = g[:HD, :HD], g[:HD, HD:], g[HD:, HD:]
        packed = jnp.where(upper, g1_, g2_)
        dg = jnp.sum(jnp.where(diag, g2_, 0.0), axis=0, keepdims=True)
        aux = jnp.where(
            row8 == 0, sums[:, :HD],
            jnp.where(row8 == 1, sums[:, HD:], jnp.where(row8 == 2, jnp.broadcast_to(dg, (8, HD)), 0.0)),
        )
        r["pa"][ch, zz, p, 0:64] = packed[:64]
        r["pa"][ch, zz, p, 64:72] = aux
        r["pb"][ch, yy, p] = packed[64:]
        r["ca"][ch, zz, p] = cr[:64]
        r["cb"][ch, yy, p] = cr[64:]

    def cross(p, which):
        arrive(x2o.at[p, pl.ds(4 * which, 4)], r["x_q"].at[2 * p + which])
        for j in range(4 * which, 4 * which + 4):
            half, zz, h = part_head(p, j)
            yy = (zz + p) % 4
            cr = dot_t(x1[:, columns(h)], x2o[p, j])
            r["da"][p, half, zz] = cr[:64]
            r["db"][p, half, yy] = cr[64:]
            if j == 3:
                for name in LATE:
                    launch(
                        rcopy(
                            r[name].at[p, 1 - c], r[name + "_r1"].at[p], r[name + "_s"].at[p],
                            r[name + "_q"].at[p], sibling,
                        )
                    )

    def cross_s2(p):
        for name, axis in LATE.items():
            buf, r1 = r[name], r[name + "_r1"]
            u, v = uv(axis)
            arrive(r1.at[p], r[name + "_q"].at[p])
            for i in range(4):
                buf[p, c, i] = buf[p, c, i] + r1[p, i]
            for d in (1, 3, 2):
                to = (u + d) % 4
                launch(
                    rcopy(
                        buf.at[p, c, to], r[name + "_r2"].at[p, d - 1], r[name + "_s"].at[2 + 3 * (p + 1) + d - 1],
                        r[name + "_q"].at[2 + 3 * (p + 1) + d - 1], dev_uv(axis, to, v, xh),
                    )
                )

    def cross_s2_sum(p):
        for name, axis in LATE.items():
            buf, r2 = r[name], r[name + "_r2"]
            u, _ = uv(axis)
            for d in (1, 2, 3):
                arrive(r2.at[p, d - 1], r[name + "_q"].at[2 + 3 * (p + 1) + d - 1])
            r[name + "x_acc"][p] = (buf[p, c, u] + r2[p, 0]) + (r2[p, 1] + r2[p, 2])

    def last_s3():
        away = jnp.where(c == 0, y - z + 4, z - y + 4) % 4
        slot = away * 2 + 1 - xh
        launch(
            rcopy(
                r["d4"], r["r5"].at[slot], r["d4_s"].at[0], r["d4_q"].at[slot],
                dev(own_last, own_last, 1, c),
            ),
            no(late_owner),
        )

    def last_total():
        for slot in range(1, 8):
            arrive(r["r5"].at[slot], r["d4_q"].at[slot])
        total = r["d4"][...] + r["r5"][1]
        for slot in range(2, 8):
            total = total + r["r5"][slot]
        return total

    def only_row0(row):
        return jnp.where(row8 == 0, jnp.broadcast_to(row, (8, HD)), 0.0)

    def mean_term(sums):
        mean1 = only_row0(r["aux"][0:1, :]) / tokens
        return dot_t(mean1, only_row0(sums) / tokens, HI)

    def similarity(raw, means, w2):
        white = mm(mm(r["w12"][0], raw / tokens - means), w2)
        sq = jnp.sum(jnp.sum(white * white, axis=1, keepdims=True), axis=0, keepdims=True)
        return jnp.broadcast_to(sq / HD, (8, HD))

    def whiten():
        top = s4_total("pa", True)
        low = s4_total("pb", True)
        aux = top[64:72]
        grams = unpack(top[:64], low, aux)
        ys, zs, scales = [], [], []
        for n in (0, 1):
            mean = only_row0(aux[n : n + 1, :]) / tokens
            cov = grams[n] / tokens - dot_t(mean, mean, HI) + RIDGE * eye
            sq = jnp.sum(jnp.sum(cov * cov, axis=1, keepdims=True), axis=0, keepdims=True)
            scale = jnp.sqrt(sq)
            scales.append(scale)
            ys.append(cov / scale)
        for it in range(ITERS):
            for n in (0, 1):
                if it == 0:
                    f = 1.5 * eye - 0.5 * ys[n]
                    zs.append(f)
                else:
                    f = 1.5 * eye - 0.5 * mm(zs[n], ys[n])
                    zs[n] = mm(f, zs[n])
                if it < ITERS - 1:
                    ys[n] = mm(ys[n], f)
        w1 = zs[0] / jnp.sqrt(scales[0])
        w2 = zs[1] / jnp.sqrt(scales[1])
        wp = jnp.where(upper, w1, w2)
        wd = jnp.sum(jnp.where(diag, w2, 0.0), axis=0, keepdims=True)
        r["wa"][c, z, own, 0:64] = wp[:64]
        r["wa"][c, z, own, 64:72] = jnp.broadcast_to(wd, (8, HD))
        r["wb"][c, y, own] = wp[64:]
        g1("wa")
        g1("wb")
        r["w12"][0] = w1
        r["w12"][1] = w2
        r["aux"][...] = aux
        r["w_out_x"][0:HD] = w2
        r["w_out_x"][HD : HD + 8] = aux
    def both(p):
        cross(p, 0)
        cross(p, 1)

    loop(HALF, lambda i: gram((1 - c) * HALF + i), unroll=2)
    for name in CHAINS:
        s1(name)
    loop(HALF, lambda i: gram(c * HALF + i), unroll=2)
    for name in ("pa", "pb"):
        s1_sum(name)
        s2(name)
    for name in ("ca", "cb"):
        s1_sum(name)
    both(0)
    for name in ("pa", "pb"):
        s2_sum(name)
        s3(name, CHAINS[name][1], range(5))
    for name in ("pa", "pb"):
        s3_sum(name, True)
        s4(name, True)
    exchange(BATCHES[0], BATCHES[1])
    for name in ("ca", "cb"):
        s2(name)
    cross_s2(0)
    pl.when(owner)(whiten)
    exchange(BATCHES[1], BATCHES[2])
    for name in GATHERS:
        g1_arrive(name)
        g2(name)
    both(1)
    cross_s2(1)
    for name in ("ca", "cb"):
        s2_sum(name)
        s3(name, CHAINS[name][1], range(5))
    for name in GATHERS:
        g2_arrive(name)
        g3(name)
    collected(1)
    exchange(BATCHES[2], 8 * PARTS)

    @pl.when(owner)
    def _():
        rcopy(r["w_out_x"], r["w_in_x"], r["y_s"].at[0], r["y_q"].at[0], twin).start()

    both(2)
    cross_s2(2)
    cross_s2_sum(0)
    cross_s2_sum(1)

    lane_head = c * HALF + jnp.where(own == 4, 16 + z, head_of(z, own))
    here = iota((8, HD), 1) == lane_head
    sa_mine = r["sa"].at[(c * 4 + z) * 5 + own]

    def own_similarity():
        raw = jnp.concatenate([s4_total("ca", True), s4_total("cb", True)], axis=0)
        sim = similarity(raw, mean_term(r["aux"][1:2, :]), r["w12"][1])
        sa_mine[...] = jnp.where(jnp.logical_and(here, row8 == lay), sim, 0.0)
        arrive(r["w_in_x"], r["y_q"].at[0])
        r["means"][...] = mean_term(r["w_in_x"][HD + 1 : HD + 2])

    def other_similarity(raw):
        sim = similarity(raw, r["means"][...], r["w_in_x"][0:HD])
        sa_mine[...] = jnp.where(jnp.logical_and(here, row8 == 1 - lay), sim, sa_mine[...])

        def send(i):
            to = (tok + 1 + (25 + i) % others) % (others + 1)
            rcopy(sa_mine, sa_mine, r["sa_s"].at[0], r["sa_q"].at[0], (to, lay)).start()

        loop(others, send, unroll=9)

    def emit(h):
        ch, zz, yy, p = places(h)
        w1, w2 = unpack(r["wa"][ch, zz, p, 0:64], r["wb"][ch, yy, p], r["wa"][ch, zz, p, 64:72])
        r["w"][0, h] = w1
        r["w"][1, h] = w2

    both(3)
    for name in GATHERS:
        g3_arrive(name)
        g4(name)
    cross_s2(3)
    cross_s2_sum(2)
    for name, axis in LATE.items():
        s3(name + "x", axis, range(3))
    for name in ("ca", "cb"):
        s3_sum(name, True)
        s4(name, True)
    for name in GATHERS:
        g4_arrive(name)
    loop(HEADS, emit, unroll=2)
    cross_s2_sum(3)
    for name, axis in LATE.items():
        s3(name + "x", axis, (3,))
    collected(0)
    last_cross(0)
    last_cross(1)
    last_s3()
    for name in LATE:
        s3_sum(name + "x", False)
        s4(name + "x", False)
    pl.when(owner)(own_similarity)

    @pl.when(early_owner)
    def _():
        other_similarity(jnp.concatenate([s4_total("dax", False), s4_total("dbx", False)], axis=0))

    @pl.when(late_owner)
    def _():
        other_similarity(last_total())

    pl.when(owner)(lambda: arrive(r["sa"].at[pl.ds(0, HEADS - 1)], r["sa_q"].at[0]))
    pl.when(no(owner))(lambda: arrive(r["sa"].at[pl.ds(0, HEADS)], r["sa_q"].at[0]))
    total = r["sa"][0]
    for i in range(1, HEADS):
        total = total + r["sa"][i]
    r["sim"][...] = total[0:2, 0:HEADS]

    for cond, copy in pending:
        if cond is None:
            copy.wait_send()
        else:
            pl.when(cond)(lambda copy=copy: copy.wait_send())
    for i in range(2 * PARTS):
        part = x2o.at[i // 2, pl.ds(4 * (i % 2), 4)]
        rcopy(part, part, r["x_s"].at[i], r["x_q"].at[i], twin).wait_send()

    @pl.when(owner)
    def _():
        for name in GATHERS:
            u, _ = uv(GATHERS[name][1])
            place = r[name].at[c, u, own]
            rcopy(place, place, r[name + "_s"].at[0], r[name + "_q"].at[0], far).wait_send()
        rcopy(r["w_out_x"], r["w_in_x"], r["y_s"].at[0], r["y_q"].at[0], twin).wait_send()
        sent = r["sa"].at[pl.ds(0, others)]
        rcopy(sent, sent, r["sa_s"].at[0], r["sa_q"].at[0], far).wait_send()


def gather_kernel(tokens, first_acts, second_acts):
    rows, width = first_acts.shape[1:]
    names = ["x1_hbm", "x2_hbm", "w", "sim"]
    scratch = []

    def add(name, spec):
        names.append(name)
        scratch.append(spec)

    dma = lambda n: pltpu.SemaphoreType.DMA((n,))
    for name in ("x1", "x2"):
        add(name, pltpu.VMEM((rows, width), first_acts.dtype))
    add("x2o", pltpu.VMEM((PARTS, 8, rows, HD), first_acts.dtype))
    for name, (n, _) in CHAINS.items():
        add(name, pltpu.VMEM((2, 4, 5, n, HD), F32))
        add(name + "_r1", pltpu.VMEM((4, 5, n, HD), F32))
        add(name + "_r2", pltpu.VMEM((3, 5, n, HD), F32))
    for name in LATE:
        add(name, pltpu.VMEM((PARTS - 1, 2, 4, 64, HD), F32))
        add(name + "_r1", pltpu.VMEM((PARTS - 1, 4, 64, HD), F32))
        add(name + "_r2", pltpu.VMEM((PARTS - 1, 3, 64, HD), F32))
        add(name + "_s", dma(17))
        add(name + "_q", dma(17))
    for name in ("m1", "m2"):
        add(name, pltpu.VMEM((7, rows, HD), first_acts.dtype))
    add("m_s", dma(16))
    add("m_q", dma(14))
    add("d4", pltpu.VMEM((HD, HD), F32))
    add("r5", pltpu.VMEM((8, HD, HD), F32))
    add("d4_s", dma(1))
    add("d4_q", dma(8))
    add("means", pltpu.VMEM((HD, HD), F32))
    for name, n in [(k, v[0]) for k, v in CHAINS.items()] + [(k + "x", 64) for k in LATE]:
        add(name + "_acc", pltpu.VMEM((5, n, HD), F32))
        add(name + "_r3", pltpu.VMEM((2, 3, n, HD), F32))
        add(name + "_t", pltpu.VMEM((2, n, HD), F32))
        add(name + "_r4", pltpu.VMEM((n, HD), F32))
        add(name + "_s", dma(10))
        add(name + "_q", dma(11))
    add("sa", pltpu.VMEM((64, 8, HD), F32))
    for name, (n, _) in GATHERS.items():
        add(name, pltpu.VMEM((2, 4, 5, n, HD), F32))
        add(name + "_s", dma(11))
        add(name + "_q", dma(10))
    add("sa_s", dma(1))
    add("sa_q", dma(1))
    add("w12", pltpu.VMEM((2, HD, HD), F32))
    add("aux", pltpu.VMEM((8, HD), F32))
    add("w_out_x", pltpu.VMEM((HD + 8, HD), F32))
    add("w_in_x", pltpu.VMEM((HD + 8, HD), F32))
    add("l_s", dma(2))
    add("x_s", dma(2 * PARTS))
    add("x_q", dma(2 * PARTS))
    add("y_s", dma(1))
    add("y_q", dma(1))
    add("none", dma(1))
    return pl.pallas_call(
        functools.partial(kernel, tokens, names),
        out_shape=(
            pltpu.VMEM((2, HEADS, HD, HD), F32),
            pltpu.VMEM((2, HEADS), F32),
        ),
        in_specs=[pl.BlockSpec(memory_space=pltpu.HBM)] * 2,
        out_specs=[pl.BlockSpec(memory_space=pltpu.VMEM)] * 2,
        scratch_shapes=scratch,
        compiler_params=pltpu.CompilerParams(
            collective_id=0, has_side_effects=True, vmem_limit_bytes=VMEM_LIMIT
        ),
    )(
        pltpu.with_memory_space_constraint(first_acts, pltpu.HBM),
        pltpu.with_memory_space_constraint(second_acts, pltpu.HBM),
    )


PIECES = 4


def store_kernel(w, sim, w_hbm, s_hbm, sems):
    step = HEADS // PIECES
    copies = [
        pltpu.make_async_copy(
            w.at[n, pl.ds(q * step, step)], w_hbm.at[n, 0, pl.ds(q * step, step)], sems.at[n * PIECES + q]
        )
        for n in range(2)
        for q in range(PIECES)
    ]
    copies.append(pltpu.make_async_copy(sim, s_hbm.at[0], sems.at[2 * PIECES]))
    for copy in copies:
        copy.start()
    for copy in copies:
        copy.wait()


def store(w, sim):
    vmem, hbm = pl.BlockSpec(memory_space=pltpu.VMEM), pl.BlockSpec(memory_space=pltpu.HBM)
    return pl.pallas_call(
        store_kernel,
        out_shape=(
            jax.ShapeDtypeStruct((2, 1, HEADS, HD, HD), F32),
            jax.ShapeDtypeStruct((1, 2, HEADS), F32),
        ),
        in_specs=[vmem] * 2,
        out_specs=(hbm, hbm),
        scratch_shapes=[pltpu.SemaphoreType.DMA((2 * PIECES + 1,))],
        compiler_params=pltpu.CompilerParams(vmem_limit_bytes=16 * 2**20),
    )(w, sim)


def solution(mesh):
    def whole(first_acts, second_acts):
        tokens = first_acts.shape[1] * lax.axis_size("tok")
        return store(*gather_kernel(tokens, first_acts, second_acts))

    in_specs = (P("lay", "tok", None), P("lay", "tok", None))
    out_specs = (P(None, "lay", None, None, None), P("lay", None, None))
    return jax.shard_map(whole, mesh=mesh, in_specs=in_specs, out_specs=out_specs, check_vma=False)
```

```python
import functools

import jax
import jax.numpy as jnp
from jax import lax
from jax.experimental import pallas as pl
from jax.experimental.pallas import tpu as pltpu
from jax.sharding import PartitionSpec as P

HEADS = 40
HD = 128
ITERS = 6
RIDGE = 0.05
HALF = HEADS // 2
PARTS = 5
FROM_HBM = 3
BATCHES = (14, 21, 32)
VMEM_LIMIT = 48 * 2**20
F32 = jnp.float32
HI = lax.Precision.HIGHEST
MESH = pl.DeviceIdType.MESH

CHAINS = {"pa": (72, "z"), "pb": (64, "y"), "ca": (64, "z"), "cb": (64, "y")}
LATE = {"da": "z", "db": "y"}
GATHERS = {"wa": (72, "z"), "wb": (64, "y")}


def iota(shape, dim):
    return lax.broadcasted_iota(jnp.int32, shape, dim)


def dot_t(a, b, precision=None):
    return lax.dot_general(
        a, b, (((0,), (0,)), ((), ())), precision=precision, preferred_element_type=F32
    )


def mm(a, b):
    return jnp.dot(a, b, precision=HI, preferred_element_type=F32)


def masks():
    ri, ci = iota((HD, HD), 0), iota((HD, HD), 1)
    return ri <= ci, ri == ci


def unpack(top, low, aux):
    upper, diag = masks()
    p = jnp.concatenate([top, low], axis=0)
    pt = p.T
    first = jnp.where(upper, p, pt)
    second = jnp.where(upper, jnp.where(diag, aux[2:3, :], pt), p)
    return first, second


def head_of(z, p):
    k = 4 * ((z + p) % 4) + z
    if isinstance(p, int):
        return 16 + z if p == 4 else k
    return jnp.where(p == 4, 16 + z, k)


def places(h):
    k = h % HALF
    z = k % 4
    half = h // HALF
    y = jnp.where(k < 16, k // 4, (z + 2 * half) % 4)
    p = jnp.where(k < 16, (k // 4 - z + 4) % 4, 4)
    return half, z, y, p


def kernel(tokens, names, *refs):
    r = dict(zip(names, refs))
    tok = lax.axis_index("tok")
    lay = lax.axis_index("lay")
    c = tok % 2
    xh = (tok // 2) % 2
    y = (tok // 4) % 4
    z = tok // 16

    def dev(z_, y_, xh_, c_):
        return (((z_ * 4 + y_) * 2 + xh_) * 2 + c_, lay)

    def uv(axis):
        return (z, y) if axis == "z" else (y, z)

    def dev_uv(axis, u, v, xh_):
        return dev(u, v, xh_, c) if axis == "z" else dev(v, u, xh_, c)

    sibling = dev(z, y, xh, 1 - c)
    twin = (tok, 1 - lay)
    far = dev(z, y, 1 - xh, c)

    on_diag = y == (z + 2 * c) % 4
    main = (y - z + 4) % 4
    owns_main = xh == main % 2
    owner = jnp.logical_or(owns_main, on_diag)
    own = jnp.where(owns_main, main, 4)
    late_owner = jnp.logical_and(on_diag, xh == 1)
    early_owner = owns_main
    extra_mine = jnp.where(owns_main, 0, 1)
    extra_give = jnp.where(owns_main, 1, 0)
    gives = jnp.logical_or(on_diag, jnp.logical_not(owns_main))
    no = jnp.logical_not

    def target(axis, p):
        u, _ = uv(axis)
        if p == 4:
            return (u + 2 * c) % 4
        return (u + p) % 4 if axis == "z" else (u - p + 4) % 4

    def rcopy(src, dst, ssem, rsem, device):
        return pltpu.make_async_remote_copy(
            src_ref=src, dst_ref=dst, send_sem=ssem, recv_sem=rsem,
            device_id=device, device_id_type=MESH,
        )

    others = lax.axis_size("tok") - 1
    pending = []

    def launch(copy, cond=None):
        pending.append((cond, copy))
        if cond is None:
            copy.start()
        else:
            pl.when(cond)(lambda: copy.start())

    def drain(copies):
        for cond, copy in copies:
            if cond is None:
                copy.wait_send()
            else:
                pl.when(cond)(lambda copy=copy: copy.wait_send())

    def arrive(ref, sem, cond=None):
        copy = rcopy(ref, ref, r["none"].at[0], sem, twin)
        if cond is None:
            copy.wait_recv()
        else:
            pl.when(cond)(lambda: copy.wait_recv())

    def loop(n, body, unroll=1):
        def step(i, carry):
            body(i)
            return carry

        lax.fori_loop(0, n, step, 0, unroll=unroll)

    def s1(name):
        launch(rcopy(r[name].at[1 - c], r[name + "_r1"], r[name + "_s"].at[0], r[name + "_q"].at[0], sibling))

    def s1_sum(name):
        buf, r1 = r[name], r[name + "_r1"]
        arrive(r1, r[name + "_q"].at[0])

        def body(i):
            for s in range(5):
                buf[c, i, s] = buf[c, i, s] + r1[i, s]

        loop(4, body)

    def s2(name, offsets=(1, 3, 2)):
        axis = CHAINS[name][1]
        u, v = uv(axis)
        for d in offsets:
            to = (u + d) % 4
            launch(
                rcopy(
                    r[name].at[c, to], r[name + "_r2"].at[d - 1], r[name + "_s"].at[d],
                    r[name + "_q"].at[d], dev_uv(axis, to, v, xh),
                )
            )

    def s2_sum(name):
        u, _ = uv(CHAINS[name][1])
        buf, r2, acc = r[name], r[name + "_r2"], r[name + "_acc"]
        for d in (1, 2, 3):
            arrive(r2.at[d - 1], r[name + "_q"].at[d])
        for s in range(5):
            acc[s] = (buf[c, u, s] + r2[0, s]) + (r2[1, s] + r2[2, s])

    def s3(name, axis, slots):
        u, v = uv(axis)
        for p in slots:
            vo = target(axis, p)
            off = jnp.maximum((v - vo + 4) % 4, 1) - 1
            kind = p // 4
            launch(
                rcopy(
                    r[name + "_acc"].at[p], r[name + "_r3"].at[kind, off], r[name + "_s"].at[4 + p],
                    r[name + "_q"].at[4 + kind * 3 + off], dev_uv(axis, u, vo, xh),
                ),
                v != vo,
            )

    def s3_sum(name, extra):
        acc, r3, part = r[name + "_acc"], r[name + "_r3"], r[name + "_t"]

        def add(kind, slot):
            for off in range(3):
                arrive(r3.at[kind, off], r[name + "_q"].at[4 + kind * 3 + off])
            part[kind] = (acc[slot] + r3[kind, 0]) + (r3[kind, 1] + r3[kind, 2])

        add(0, main)
        if extra:
            pl.when(on_diag)(lambda: add(1, 4))

    def s4(name, extra):
        src = r[name + "_t"].at[extra_give] if extra else r[name + "_t"].at[0]
        cond = gives if extra else no(owns_main)
        launch(rcopy(src, r[name + "_r4"], r[name + "_s"].at[9], r[name + "_q"].at[10], far), cond)

    def s4_total(name, extra):
        arrive(r[name + "_r4"], r[name + "_q"].at[10])
        mine = r[name + "_t"][extra_mine] if extra else r[name + "_t"][0]
        return mine + r[name + "_r4"][...]

    def g1(name):
        u, _ = uv(GATHERS[name][1])
        place = r[name].at[c, u, own]
        rcopy(place, place, r[name + "_s"].at[0], r[name + "_q"].at[0], far).start()

    def g1_arrive(name):
        u, _ = uv(GATHERS[name][1])
        arrive(r[name].at[c, u, jnp.where(owns_main, 4, main)], r[name + "_q"].at[0], gives)

    def g2(name):
        axis = GATHERS[name][1]
        u, v = uv(axis)
        for d in (1, 3, 2):
            for kind in (0, 1):
                slot = 4 if kind else main
                place = r[name].at[c, u, slot]
                launch(
                    rcopy(
                        place, place, r[name + "_s"].at[kind * 3 + d], r[name + "_q"].at[1 + slot],
                        dev_uv(axis, u, (v + d) % 4, xh),
                    ),
                    on_diag if kind else None,
                )

    def g2_arrive(name):
        axis = GATHERS[name][1]
        u, v = uv(axis)
        for p in range(5):
            arrive(r[name].at[c, u, p], r[name + "_q"].at[1 + p], v != target(axis, p))

    def g3(name):
        axis = GATHERS[name][1]
        u, v = uv(axis)
        place = r[name].at[c, u]
        for d in (1, 3, 2):
            launch(
                rcopy(
                    place, place, r[name + "_s"].at[6 + d], r[name + "_q"].at[5 + d],
                    dev_uv(axis, (u + d) % 4, v, xh),
                )
            )

    def g3_arrive(name):
        u, _ = uv(GATHERS[name][1])
        for d in (1, 2, 3):
            arrive(r[name].at[c, (u - d + 4) % 4], r[name + "_q"].at[5 + d])

    def g4(name):
        place = r[name].at[c]
        launch(rcopy(place, place, r[name + "_s"].at[10], r[name + "_q"].at[9], sibling))

    def g4_arrive(name):
        arrive(r[name].at[1 - c], r[name + "_q"].at[9])

    x1, x2, x2o = r["x1"], r["x2"], r["x2o"]

    def part_head(p, j):
        half = (1 - c) if j < 4 else c
        return half, j % 4, half * HALF + head_of(j % 4, p)

    own_last = jnp.where(c == 0, z, (y + 2) % 4)

    def last_head(z_, c_):
        return c_ * HALF + 16 + z_

    def columns(h):
        return pl.ds(pl.multiple_of(h * HD, HD), HD)

    def exchange(lo, hi):
        for n in range(lo, hi):
            p, j = n // 8, n % 8
            _, _, h = part_head(p, j)
            src = r["x2_hbm"].at[0, :, columns(h)] if n < FROM_HBM else x2.at[:, columns(h)]
            if p == 4:
                src = x2.at[:, columns(last_head(own_last, c))] if j == 0 else r["m2"].at[j - 1]
            sem = 2 * p + j // 4
            rcopy(src, x2o.at[p, j], r["x_s"].at[sem], r["x_q"].at[sem], twin).start()

    def collect():
        for d in (1, 3, 2, 0):
            for c_ in (0, 1):
                if c_ == 0:
                    w_, to, other = (z + d) % 4, dev((z + d) % 4, y, xh, 0), c
                else:
                    w_, to, other = (y + d + 2) % 4, dev(z, (y + d) % 4, xh, 1), 1 - c
                slot = jnp.maximum(2 * d + other, 1) - 1
                cols = columns(last_head(w_, c_))
                for n, x in ((1, x2), (0, x1)):
                    launch(
                        rcopy(
                            x.at[:, cols], r["m%d" % (n + 1)].at[slot], r["m_s"].at[8 * n + 2 * d + c_],
                            r["m_q"].at[7 * n + slot], to,
                        ),
                        None if d else other == 1,
                    )

    def collected(n):
        for j in range(1, 8):
            arrive(r["m%d" % (n + 1)].at[j - 1], r["m_q"].at[7 * n + j - 1])

    def last_cross(which):
        arrive(x2o.at[4, pl.ds(4 * which, 4)], r["x_q"].at[8 + which])
        total = None
        for j in range(4 * which, 4 * which + 4):
            left = r["m1"][j - 1] if j else x1[:, columns(last_head(own_last, c))]
            cr = dot_t(left, x2o[4, j])
            total = cr if total is None else total + cr
        r["d4"][...] = r["d4"][...] + total if which else total

    def exchange_sent(i):
        part = x2o.at[i // 2, pl.ds(4 * (i % 2), 4)]
        rcopy(part, part, r["x_s"].at[i], r["x_q"].at[i], twin).wait_send()

    load1 = pltpu.make_async_copy(r["x1_hbm"].at[0], x1, r["l_s"].at[0])
    load2 = pltpu.make_async_copy(r["x2_hbm"].at[0], x2, r["l_s"].at[1])
    load2.start()
    load1.start()
    barrier = pltpu.get_barrier_semaphore()
    peers = [sibling, twin, far]
    for d in range(1, 4):
        for c_ in (c, 1 - c):
            peers.append(dev((z + d) % 4, y, xh, c_))
            peers.append(dev(z, (y + d) % 4, xh, c_))
    for peer in peers:
        pl.semaphore_signal(barrier, inc=1, device_id=peer, device_id_type=MESH)
    pl.semaphore_wait(barrier, len(peers))
    exchange(0, FROM_HBM)
    load2.wait()
    exchange(FROM_HBM, BATCHES[0])
    load1.wait()
    collect()

    upper, diag = masks()
    eye = jnp.where(diag, 1.0, 0.0).astype(F32)
    row8 = iota((8, HD), 0)

    def gram(h):
        ch, zz, yy, p = places(h)
        cols = columns(h)
        ab = jnp.concatenate([x1[:, cols], x2[:, cols]], axis=1)
        g = dot_t(ab, ab)
        sums = jnp.dot(jnp.ones((8, ab.shape[0]), ab.dtype), ab, preferred_element_type=F32)
        g1_, cr, g2_ = g[:HD, :HD], g[:HD, HD:], g[HD:, HD:]
        packed = jnp.where(upper, g1_, g2_)
        dg = jnp.sum(jnp.where(diag, g2_, 0.0), axis=0, keepdims=True)
        aux = jnp.where(
            row8 == 0, sums[:, :HD],
            jnp.where(row8 == 1, sums[:, HD:], jnp.where(row8 == 2, jnp.broadcast_to(dg, (8, HD)), 0.0)),
        )
        r["pa"][ch, zz, p, 0:64] = packed[:64]
        r["pa"][ch, zz, p, 64:72] = aux
        r["pb"][ch, yy, p] = packed[64:]
        r["ca"][ch, zz, p] = cr[:64]
        r["cb"][ch, yy, p] = cr[64:]

    def cross(p, which):
        arrive(x2o.at[p, pl.ds(4 * which, 4)], r["x_q"].at[2 * p + which])
        for j in range(4 * which, 4 * which + 4):
            half, zz, h = part_head(p, j)
            yy = (zz + p) % 4
            cr = dot_t(x1[:, columns(h)], x2o[p, j])
            r["da"][p, half, zz] = cr[:64]
            r["db"][p, half, yy] = cr[64:]
            if j == 3:
                for name in LATE:
                    launch(
                        rcopy(
                            r[name].at[p, 1 - c], r[name + "_r1"].at[p], r[name + "_s"].at[p],
                            r[name + "_q"].at[p], sibling,
                        )
                    )

    def cross_s2(p):
        for name, axis in LATE.items():
            buf, r1 = r[name], r[name + "_r1"]
            u, v = uv(axis)
            arrive(r1.at[p], r[name + "_q"].at[p])
            for i in range(4):
                buf[p, c, i] = buf[p, c, i] + r1[p, i]
            for d in (1, 3, 2):
                to = (u + d) % 4
                launch(
                    rcopy(
                        buf.at[p, c, to], r[name + "_r2"].at[p, d - 1], r[name + "_s"].at[2 + 3 * (p + 1) + d - 1],
                        r[name + "_q"].at[2 + 3 * (p + 1) + d - 1], dev_uv(axis, to, v, xh),
                    )
                )

    def cross_s2_sum(p):
        for name, axis in LATE.items():
            buf, r2 = r[name], r[name + "_r2"]
            u, _ = uv(axis)
            for d in (1, 2, 3):
                arrive(r2.at[p, d - 1], r[name + "_q"].at[2 + 3 * (p + 1) + d - 1])
            r[name + "x_acc"][p] = (buf[p, c, u] + r2[p, 0]) + (r2[p, 1] + r2[p, 2])

    def last_s3():
        away = jnp.where(c == 0, y - z + 4, z - own_last + 4) % 4
        slot = away * 2 + 1 - xh
        launch(
            rcopy(
                r["d4"], r["r5"].at[slot], r["d4_s"].at[0], r["d4_q"].at[slot],
                dev(own_last, (own_last + 2 * c) % 4, 1, c),
            ),
            no(late_owner),
        )

    def last_total():
        for slot in range(1, 8):
            arrive(r["r5"].at[slot], r["d4_q"].at[slot])
        total = r["d4"][...] + r["r5"][1]
        for slot in range(2, 8):
            total = total + r["r5"][slot]
        return total

    def only_row0(row):
        return jnp.where(row8 == 0, jnp.broadcast_to(row, (8, HD)), 0.0)

    def mean_term(sums):
        mean1 = only_row0(r["aux"][0:1, :]) / tokens
        return dot_t(mean1, only_row0(sums) / tokens, HI)

    def similarity(raw, means, w2):
        white = mm(mm(r["w12"][0], raw / tokens - means), w2)
        sq = jnp.sum(jnp.sum(white * white, axis=1, keepdims=True), axis=0, keepdims=True)
        return jnp.broadcast_to(sq / HD, (1, HD))

    def whiten():
        top = s4_total("pa", True)
        low = s4_total("pb", True)
        aux = top[64:72]
        grams = unpack(top[:64], low, aux)
        ys, zs, scales = [], [], []
        for n in (0, 1):
            mean = only_row0(aux[n : n + 1, :]) / tokens
            cov = grams[n] / tokens - dot_t(mean, mean, HI) + RIDGE * eye
            sq = jnp.sum(jnp.sum(cov * cov, axis=1, keepdims=True), axis=0, keepdims=True)
            scale = jnp.sqrt(sq)
            scales.append(scale)
            ys.append(cov / scale)
        for it in range(ITERS):
            for n in (0, 1):
                if it == 0:
                    f = 1.5 * eye - 0.5 * ys[n]
                    zs.append(f)
                else:
                    f = 1.5 * eye - 0.5 * mm(zs[n], ys[n])
                    zs[n] = mm(f, zs[n])
                if it < ITERS - 1:
                    ys[n] = mm(ys[n], f)
        w1 = zs[0] / jnp.sqrt(scales[0])
        w2 = zs[1] / jnp.sqrt(scales[1])
        wp = jnp.where(upper, w1, w2)
        wd = jnp.sum(jnp.where(diag, w2, 0.0), axis=0, keepdims=True)
        r["wa"][c, z, own, 0:64] = wp[:64]
        r["wa"][c, z, own, 64:72] = jnp.broadcast_to(wd, (8, HD))
        r["wb"][c, y, own] = wp[64:]
        g1("wa")
        g1("wb")
        r["w12"][0] = w1
        r["w12"][1] = w2
        r["aux"][...] = aux
        r["w_out_x"][0:HD] = w2
        r["w_out_x"][HD : HD + 8] = aux
    def both(p):
        cross(p, 0)
        cross(p, 1)

    loop(HALF, lambda i: gram((1 - c) * HALF + i), unroll=2)
    for name in CHAINS:
        s1(name)
    loop(HALF, lambda i: gram(c * HALF + i), unroll=2)
    for name in ("pa", "pb"):
        s1_sum(name)
        s2(name)
    for name in ("ca", "cb"):
        s1_sum(name)
    both(0)
    for name in ("pa", "pb"):
        s2_sum(name)
        s3(name, CHAINS[name][1], range(5))
    for name in ("pa", "pb"):
        s3_sum(name, True)
        s4(name, True)
    exchange(BATCHES[0], BATCHES[1])
    for name in ("ca", "cb"):
        s2(name)
    cross_s2(0)
    pl.when(owner)(whiten)
    exchange(BATCHES[1], BATCHES[2])
    for name in GATHERS:
        g1_arrive(name)
        g2(name)
    both(1)
    cross_s2(1)
    for name in ("ca", "cb"):
        s2_sum(name)
        s3(name, CHAINS[name][1], range(5))
    for name in GATHERS:
        g2_arrive(name)
        g3(name)
    collected(1)
    exchange(BATCHES[2], 8 * PARTS)

    @pl.when(owner)
    def _():
        rcopy(r["w_out_x"], r["w_in_x"], r["y_s"].at[0], r["y_q"].at[0], twin).start()

    both(2)
    cross_s2(2)
    cross_s2_sum(0)
    cross_s2_sum(1)

    lane_head = c * HALF + jnp.where(own == 4, 16 + z, head_of(z, own))
    lanes = iota((1, HD), 1)
    sa_mine = r["sa"].at[(c * 4 + z) * 5 + own]

    def own_similarity():
        raw = jnp.concatenate([s4_total("ca", True), s4_total("cb", True)], axis=0)
        sim = similarity(raw, mean_term(r["aux"][1:2, :]), r["w12"][1])
        sa_mine[...] = jnp.where(lanes == 64 * lay + lane_head, sim, 0.0)
        arrive(r["w_in_x"], r["y_q"].at[0])
        r["means"][...] = mean_term(r["w_in_x"][HD + 1 : HD + 2])

    def other_similarity(raw):
        sim = similarity(raw, r["means"][...], r["w_in_x"][0:HD])
        sa_mine[...] = jnp.where(lanes == 64 * (1 - lay) + lane_head, sim, sa_mine[...])
        steps = (2, 1, 3, 0)
        z_at = [(z + d) % 4 * 16 for d in range(4)]
        y_at = [(y + d) % 4 * 4 for d in range(4)]
        x_at = [(xh + d) % 2 * 2 for d in range(2)]
        c_at = [(c + d) % 2 for d in range(2)]
        for dx in (1, 0):
            for dz in steps:
                for dy in steps:
                    for dc in (1, 0):
                        if dx or dz or dy or dc:
                            to = z_at[dz] + y_at[dy] + (x_at[dx] + c_at[dc])
                            rcopy(sa_mine, sa_mine, r["sa_s"].at[0], r["sa_q"].at[0], (to, lay)).start()

    def emit(h):
        ch, zz, yy, p = places(h)
        w1, w2 = unpack(r["wa"][ch, zz, p, 0:64], r["wb"][ch, yy, p], r["wa"][ch, zz, p, 64:72])
        r["w"][0, h] = w1
        r["w"][1, h] = w2

    both(3)
    for name in GATHERS:
        g3_arrive(name)
        g4(name)
    cross_s2(3)
    cross_s2_sum(2)
    for name, axis in LATE.items():
        s3(name + "x", axis, range(3))
    for name in ("ca", "cb"):
        s3_sum(name, True)
    early = list(pending)
    pending.clear()
    for name in ("ca", "cb"):
        s4(name, True)
    for name in GATHERS:
        g4_arrive(name)
    loop(HEADS, emit, unroll=2)
    cross_s2_sum(3)
    for name, axis in LATE.items():
        s3(name + "x", axis, (3,))
    collected(0)
    drain(early)
    for i in range(2 * PARTS - 2):
        exchange_sent(i)
    last_cross(0)
    last_cross(1)
    last_s3()
    for name in LATE:
        s3_sum(name + "x", False)
        s4(name + "x", False)
    pl.when(owner)(own_similarity)

    @pl.when(early_owner)
    def _():
        other_similarity(jnp.concatenate([s4_total("dax", False), s4_total("dbx", False)], axis=0))

    @pl.when(late_owner)
    def _():
        other_similarity(last_total())

    pl.when(owner)(lambda: arrive(r["sa"].at[pl.ds(0, HEADS - 1)], r["sa_q"].at[0]))
    pl.when(no(owner))(lambda: arrive(r["sa"].at[pl.ds(0, HEADS)], r["sa_q"].at[0]))
    total = r["sa"][0]
    for i in range(1, HEADS):
        total = total + r["sa"][i]
    r["sim"][0:1, :] = total[:, 0:HEADS]
    r["sim"][1:2, :] = total[:, 64 : 64 + HEADS]

    drain(pending)
    for i in (2 * PARTS - 2, 2 * PARTS - 1):
        exchange_sent(i)

    @pl.when(owner)
    def _():
        for name in GATHERS:
            u, _ = uv(GATHERS[name][1])
            place = r[name].at[c, u, own]
            rcopy(place, place, r[name + "_s"].at[0], r[name + "_q"].at[0], far).wait_send()
        rcopy(r["w_out_x"], r["w_in_x"], r["y_s"].at[0], r["y_q"].at[0], twin).wait_send()
        sent = r["sa"].at[pl.ds(0, others)]
        rcopy(sent, sent, r["sa_s"].at[0], r["sa_q"].at[0], far).wait_send()


def gather_kernel(tokens, first_acts, second_acts):
    rows, width = first_acts.shape[1:]
    names = ["x1_hbm", "x2_hbm", "w", "sim"]
    scratch = []

    def add(name, spec):
        names.append(name)
        scratch.append(spec)

    dma = lambda n: pltpu.SemaphoreType.DMA((n,))
    for name in ("x1", "x2"):
        add(name, pltpu.VMEM((rows, width), first_acts.dtype))
    add("x2o", pltpu.VMEM((PARTS, 8, rows, HD), first_acts.dtype))
    for name, (n, _) in CHAINS.items():
        add(name, pltpu.VMEM((2, 4, 5, n, HD), F32))
        add(name + "_r1", pltpu.VMEM((4, 5, n, HD), F32))
        add(name + "_r2", pltpu.VMEM((3, 5, n, HD), F32))
    for name in LATE:
        add(name, pltpu.VMEM((PARTS - 1, 2, 4, 64, HD), F32))
        add(name + "_r1", pltpu.VMEM((PARTS - 1, 4, 64, HD), F32))
        add(name + "_r2", pltpu.VMEM((PARTS - 1, 3, 64, HD), F32))
        add(name + "_s", dma(17))
        add(name + "_q", dma(17))
    for name in ("m1", "m2"):
        add(name, pltpu.VMEM((7, rows, HD), first_acts.dtype))
    add("m_s", dma(16))
    add("m_q", dma(14))
    add("d4", pltpu.VMEM((HD, HD), F32))
    add("r5", pltpu.VMEM((8, HD, HD), F32))
    add("d4_s", dma(1))
    add("d4_q", dma(8))
    add("means", pltpu.VMEM((HD, HD), F32))
    for name, n in [(k, v[0]) for k, v in CHAINS.items()] + [(k + "x", 64) for k in LATE]:
        add(name + "_acc", pltpu.VMEM((5, n, HD), F32))
        add(name + "_r3", pltpu.VMEM((2, 3, n, HD), F32))
        add(name + "_t", pltpu.VMEM((2, n, HD), F32))
        add(name + "_r4", pltpu.VMEM((n, HD), F32))
        add(name + "_s", dma(10))
        add(name + "_q", dma(11))
    add("sa", pltpu.VMEM((64, 1, HD), F32))
    for name, (n, _) in GATHERS.items():
        add(name, pltpu.VMEM((2, 4, 5, n, HD), F32))
        add(name + "_s", dma(11))
        add(name + "_q", dma(10))
    add("sa_s", dma(1))
    add("sa_q", dma(1))
    add("w12", pltpu.VMEM((2, HD, HD), F32))
    add("aux", pltpu.VMEM((8, HD), F32))
    add("w_out_x", pltpu.VMEM((HD + 8, HD), F32))
    add("w_in_x", pltpu.VMEM((HD + 8, HD), F32))
    add("l_s", dma(2))
    add("x_s", dma(2 * PARTS))
    add("x_q", dma(2 * PARTS))
    add("y_s", dma(1))
    add("y_q", dma(1))
    add("none", dma(1))
    return pl.pallas_call(
        functools.partial(kernel, tokens, names),
        out_shape=(
            pltpu.VMEM((2, HEADS, HD, HD), F32),
            pltpu.VMEM((2, HEADS), F32),
        ),
        in_specs=[pl.BlockSpec(memory_space=pltpu.HBM)] * 2,
        out_specs=[pl.BlockSpec(memory_space=pltpu.VMEM)] * 2,
        scratch_shapes=scratch,
        compiler_params=pltpu.CompilerParams(
            collective_id=0, has_side_effects=True, vmem_limit_bytes=VMEM_LIMIT
        ),
    )(
        pltpu.with_memory_space_constraint(first_acts, pltpu.HBM),
        pltpu.with_memory_space_constraint(second_acts, pltpu.HBM),
    )


PIECES = 4


def store_kernel(w, sim, w_hbm, s_hbm, sems):
    step = HEADS // PIECES
    copies = [
        pltpu.make_async_copy(
            w.at[n, pl.ds(q * step, step)], w_hbm.at[n, 0, pl.ds(q * step, step)], sems.at[n * PIECES + q]
        )
        for n in range(2)
        for q in range(PIECES)
    ]
    copies.append(pltpu.make_async_copy(sim, s_hbm.at[0], sems.at[2 * PIECES]))
    for copy in copies:
        copy.start()
    for copy in copies:
        copy.wait()


def store(w, sim):
    vmem, hbm = pl.BlockSpec(memory_space=pltpu.VMEM), pl.BlockSpec(memory_space=pltpu.HBM)
    return pl.pallas_call(
        store_kernel,
        out_shape=(
            jax.ShapeDtypeStruct((2, 1, HEADS, HD, HD), F32),
            jax.ShapeDtypeStruct((1, 2, HEADS), F32),
        ),
        in_specs=[vmem] * 2,
        out_specs=(hbm, hbm),
        scratch_shapes=[pltpu.SemaphoreType.DMA((2 * PIECES + 1,))],
        compiler_params=pltpu.CompilerParams(vmem_limit_bytes=16 * 2**20),
    )(w, sim)


def solution(mesh):
    def whole(first_acts, second_acts):
        tokens = first_acts.shape[1] * lax.axis_size("tok")
        return store(*gather_kernel(tokens, first_acts, second_acts))

    in_specs = (P("lay", "tok", None), P("lay", "tok", None))
    out_specs = (P(None, "lay", None, None, None), P("lay", None, None))
    return jax.shard_map(whole, mesh=mesh, in_specs=in_specs, out_specs=out_specs, check_vma=False)
```

```python
import functools

import jax
import jax.numpy as jnp
from jax import lax
from jax.experimental import pallas as pl
from jax.experimental.pallas import tpu as pltpu
from jax.sharding import PartitionSpec as P

HEADS = 40
HD = 128
ITERS = 6
RIDGE = 0.05
HALF = HEADS // 2
PARTS = 5
FROM_HBM = 3
BATCHES = (14, 21, 32)
CARRIED = (3, 7)
VMEM_LIMIT = 48 * 2**20
F32 = jnp.float32
HI = lax.Precision.HIGHEST
MESH = pl.DeviceIdType.MESH

CHAINS = {"pa": (72, "z"), "pb": (64, "y"), "ca": (64, "z"), "cb": (64, "y")}
LATE = {"da": "z", "db": "y"}
GATHERS = {"wa": (72, "z"), "wb": (64, "y")}


def iota(shape, dim):
    return lax.broadcasted_iota(jnp.int32, shape, dim)


def dot_t(a, b, precision=None):
    return lax.dot_general(
        a, b, (((0,), (0,)), ((), ())), precision=precision, preferred_element_type=F32
    )


def mm(a, b):
    return jnp.dot(a, b, precision=HI, preferred_element_type=F32)


def masks():
    ri, ci = iota((HD, HD), 0), iota((HD, HD), 1)
    return ri <= ci, ri == ci


def unpack(top, low, aux):
    upper, diag = masks()
    p = jnp.concatenate([top, low], axis=0)
    pt = p.T
    first = jnp.where(upper, p, pt)
    second = jnp.where(upper, jnp.where(diag, aux[2:3, :], pt), p)
    return first, second


def fold(w):
    row, lane = iota((64, HD), 0), iota((64, HD), 1)
    lower = jnp.logical_and(lane < 64, row > lane)
    return jnp.where(lower, pltpu.roll(w[64:], 64, 1), w[:64])


def unfold(folded, diagonal):
    row, lane = iota((HD, HD), 0), iota((HD, HD), 1)
    q = jnp.concatenate([folded, pltpu.roll(folded, 64, 1)], axis=0)
    top = jnp.logical_and(row < 64, row <= lane)
    low = jnp.logical_and(lane >= 64, row > lane)
    out = jnp.where(jnp.logical_or(top, low), q, q.T)
    return jnp.where(jnp.logical_and(row == lane, row >= 64), diagonal, out)


def head_of(z, p):
    k = 4 * ((z + p) % 4) + z
    if isinstance(p, int):
        return 16 + z if p == 4 else k
    return jnp.where(p == 4, 16 + z, k)


def places(h):
    k = h % HALF
    z = k % 4
    half = h // HALF
    y = jnp.where(k < 16, k // 4, (z + 2 * half) % 4)
    p = jnp.where(k < 16, (k // 4 - z + 4) % 4, 4)
    return half, z, y, p


def kernel(tokens, names, *refs):
    r = dict(zip(names, refs))
    tok = lax.axis_index("tok")
    lay = lax.axis_index("lay")
    c = tok % 2
    xh = (tok // 2) % 2
    y = (tok // 4) % 4
    z = tok // 16

    def dev(z_, y_, xh_, c_):
        return (((z_ * 4 + y_) * 2 + xh_) * 2 + c_, lay)

    def uv(axis):
        return (z, y) if axis == "z" else (y, z)

    def dev_uv(axis, u, v, xh_):
        return dev(u, v, xh_, c) if axis == "z" else dev(v, u, xh_, c)

    sibling = dev(z, y, xh, 1 - c)
    twin = (tok, 1 - lay)
    far = dev(z, y, 1 - xh, c)

    on_diag = y == (z + 2 * c) % 4
    main = (y - z + 4) % 4
    owns_main = xh == main % 2
    owner = jnp.logical_or(owns_main, on_diag)
    own = jnp.where(owns_main, main, 4)
    late_owner = jnp.logical_and(on_diag, xh == 1)
    early_owner = owns_main
    extra_mine = jnp.where(owns_main, 0, 1)
    extra_give = jnp.where(owns_main, 1, 0)
    gives = jnp.logical_or(on_diag, jnp.logical_not(owns_main))
    no = jnp.logical_not

    def target(axis, p):
        u, _ = uv(axis)
        if p == 4:
            return (u + 2 * c) % 4
        return (u + p) % 4 if axis == "z" else (u - p + 4) % 4

    def rcopy(src, dst, ssem, rsem, device):
        return pltpu.make_async_remote_copy(
            src_ref=src, dst_ref=dst, send_sem=ssem, recv_sem=rsem,
            device_id=device, device_id_type=MESH,
        )

    others = lax.axis_size("tok") - 1
    pending = []

    def launch(copy, cond=None):
        pending.append((cond, copy))
        if cond is None:
            copy.start()
        else:
            pl.when(cond)(lambda: copy.start())

    def drain(copies):
        for cond, copy in copies:
            if cond is None:
                copy.wait_send()
            else:
                pl.when(cond)(lambda copy=copy: copy.wait_send())

    def arrive(ref, sem, cond=None):
        copy = rcopy(ref, ref, r["none"].at[0], sem, twin)
        if cond is None:
            copy.wait_recv()
        else:
            pl.when(cond)(lambda: copy.wait_recv())

    def loop(n, body, unroll=1):
        def step(i, carry):
            body(i)
            return carry

        lax.fori_loop(0, n, step, 0, unroll=unroll)

    def s1(name):
        launch(rcopy(r[name].at[1 - c], r[name + "_r1"], r[name + "_s"].at[0], r[name + "_q"].at[0], sibling))

    def s1_sum(name):
        buf, r1 = r[name], r[name + "_r1"]
        arrive(r1, r[name + "_q"].at[0])

        def body(i):
            for s in range(5):
                buf[c, i, s] = buf[c, i, s] + r1[i, s]

        loop(4, body)

    def s2(name, offsets=(1, 3, 2)):
        axis = CHAINS[name][1]
        u, v = uv(axis)
        for d in offsets:
            to = (u + d) % 4
            launch(
                rcopy(
                    r[name].at[c, to], r[name + "_r2"].at[d - 1], r[name + "_s"].at[d],
                    r[name + "_q"].at[d], dev_uv(axis, to, v, xh),
                )
            )

    def s2_sum(name):
        u, _ = uv(CHAINS[name][1])
        buf, r2, acc = r[name], r[name + "_r2"], r[name + "_acc"]
        for d in (1, 2, 3):
            arrive(r2.at[d - 1], r[name + "_q"].at[d])
        for s in range(5):
            acc[s] = (buf[c, u, s] + r2[0, s]) + (r2[1, s] + r2[2, s])

    def s3(name, axis, slots):
        u, v = uv(axis)
        for p in slots:
            vo = target(axis, p)
            off = jnp.maximum((v - vo + 4) % 4, 1) - 1
            kind = p // 4
            launch(
                rcopy(
                    r[name + "_acc"].at[p], r[name + "_r3"].at[kind, off], r[name + "_s"].at[4 + p],
                    r[name + "_q"].at[4 + kind * 3 + off], dev_uv(axis, u, vo, xh),
                ),
                v != vo,
            )

    def s3_sum(name, extra):
        acc, r3, part = r[name + "_acc"], r[name + "_r3"], r[name + "_t"]

        def add(kind, slot):
            for off in range(3):
                arrive(r3.at[kind, off], r[name + "_q"].at[4 + kind * 3 + off])
            part[kind] = (acc[slot] + r3[kind, 0]) + (r3[kind, 1] + r3[kind, 2])

        add(0, main)
        if extra:
            pl.when(on_diag)(lambda: add(1, 4))

    def s4(name, extra):
        src = r[name + "_t"].at[extra_give] if extra else r[name + "_t"].at[0]
        cond = gives if extra else no(owns_main)
        launch(rcopy(src, r[name + "_r4"], r[name + "_s"].at[9], r[name + "_q"].at[10], far), cond)

    def s4_total(name, extra):
        arrive(r[name + "_r4"], r[name + "_q"].at[10])
        mine = r[name + "_t"][extra_mine] if extra else r[name + "_t"][0]
        return mine + r[name + "_r4"][...]

    def g1(name):
        u, _ = uv(GATHERS[name][1])
        place = r[name].at[c, u, own]
        rcopy(place, place, r[name + "_s"].at[0], r[name + "_q"].at[0], far).start()

    def g1_arrive(name):
        u, _ = uv(GATHERS[name][1])
        arrive(r[name].at[c, u, jnp.where(owns_main, 4, main)], r[name + "_q"].at[0], gives)

    def g2(name):
        axis = GATHERS[name][1]
        u, v = uv(axis)
        for d in (1, 3, 2):
            for kind in (0, 1):
                slot = 4 if kind else main
                place = r[name].at[c, u, slot]
                launch(
                    rcopy(
                        place, place, r[name + "_s"].at[kind * 3 + d], r[name + "_q"].at[1 + slot],
                        dev_uv(axis, u, (v + d) % 4, xh),
                    ),
                    on_diag if kind else None,
                )

    def g2_arrive(name):
        axis = GATHERS[name][1]
        u, v = uv(axis)
        for p in range(5):
            arrive(r[name].at[c, u, p], r[name + "_q"].at[1 + p], v != target(axis, p))

    def g3(name):
        axis = GATHERS[name][1]
        u, v = uv(axis)
        place = r[name].at[c, u]
        for d in (1, 3, 2):
            launch(
                rcopy(
                    place, place, r[name + "_s"].at[6 + d], r[name + "_q"].at[5 + d],
                    dev_uv(axis, (u + d) % 4, v, xh),
                )
            )

    def g3_arrive(name):
        u, _ = uv(GATHERS[name][1])
        for d in (1, 2, 3):
            arrive(r[name].at[c, (u - d + 4) % 4], r[name + "_q"].at[5 + d])

    def g4(name):
        place = r[name].at[c]
        launch(rcopy(place, place, r[name + "_s"].at[10], r[name + "_q"].at[9], sibling))

    def g4_arrive(name):
        arrive(r[name].at[1 - c], r[name + "_q"].at[9])

    x1, x2, x2o = r["x1"], r["x2"], r["x2o"]

    def part_head(p, j):
        half = (1 - c) if j < 4 else c
        return half, j % 4, half * HALF + head_of(j % 4, p)

    own_last = jnp.where(c == 0, z, (y + 2) % 4)

    def last_head(z_, c_):
        return c_ * HALF + 16 + z_

    def columns(h):
        return pl.ds(pl.multiple_of(h * HD, HD), HD)

    def exchange(lo, hi):
        for n in range(lo, hi):
            p, j = n // 8, n % 8
            _, _, h = part_head(p, j)
            src = r["x2_hbm"].at[0, :, columns(h)] if n < FROM_HBM else x2.at[:, columns(h)]
            if p == 4:
                src = x2.at[:, columns(last_head(own_last, c))] if j == 0 else r["m2"].at[j - 1]
            sem = 2 * p + j // 4
            copy = rcopy(src, x2o.at[p, j], r["x_s"].at[sem], r["x_q"].at[sem], twin)
            if p == 4 and j in CARRIED:
                pl.when(c == 1)(lambda copy=copy: copy.start())
            else:
                copy.start()
            if n == 8 * PARTS - 5:
                for i, k in enumerate(CARRIED):
                    launch(
                        rcopy(
                            r["m3"].at[i], x2o.at[4, k], r["m3_s"].at[2 + i], r["x_q"].at[8 + k // 4],
                            (jnp.maximum(tok, 1) - 1, 1 - lay),
                        ),
                        c == 1,
                    )

    def collect():
        for d in (1, 3, 2, 0):
            for c_ in (0, 1):
                if c_ == 0:
                    w_, to, other = (z + d) % 4, dev((z + d) % 4, y, xh, 0), c
                else:
                    w_, to, other = (y + d + 2) % 4, dev(z, (y + d) % 4, xh, 1), 1 - c
                slot = jnp.maximum(2 * d + other, 1) - 1
                cols = columns(last_head(w_, c_))
                for n, x in ((1, x2), (0, x1)):
                    cond = None if d else other == 1
                    carried = n == 1 and c_ == 0 and 2 * d + 1 in CARRIED
                    if carried:
                        i = CARRIED.index(2 * d + 1)
                        launch(
                            rcopy(
                                x.at[:, cols], r["m3"].at[i], r["m3_s"].at[i], r["m3_q"].at[i],
                                dev(w_, y, xh, 1),
                            ),
                            c == 1,
                        )
                        cond = c == 0
                    launch(
                        rcopy(
                            x.at[:, cols], r["m%d" % (n + 1)].at[slot], r["m_s"].at[8 * n + 2 * d + c_],
                            r["m_q"].at[7 * n + slot], to,
                        ),
                        cond,
                    )

    def collected(n):
        for j in range(1, 8):
            carried = n == 1 and j in CARRIED
            arrive(r["m%d" % (n + 1)].at[j - 1], r["m_q"].at[7 * n + j - 1], c == 1 if carried else None)
        if n == 1:
            for i in range(2):
                arrive(r["m3"].at[i], r["m3_q"].at[i], c == 1)

    def last_cross(which):
        arrive(x2o.at[4, pl.ds(4 * which, 4)], r["x_q"].at[8 + which])
        total = None
        for j in range(4 * which, 4 * which + 4):
            left = r["m1"][j - 1] if j else x1[:, columns(last_head(own_last, c))]
            cr = dot_t(left, x2o[4, j])
            total = cr if total is None else total + cr
        r["d4"][...] = r["d4"][...] + total if which else total

    def exchange_sent(i):
        def sent(count):
            part = x2o.at[i // 2, pl.ds(4 * (i % 2), count)]
            rcopy(part, part, r["x_s"].at[i], r["x_q"].at[i], twin).wait_send()

        if i < 8:
            sent(4)
        else:
            pl.when(c == 1)(lambda: sent(4))
            pl.when(c == 0)(lambda: sent(3))

    load1 = pltpu.make_async_copy(r["x1_hbm"].at[0], x1, r["l_s"].at[0])
    load2 = pltpu.make_async_copy(r["x2_hbm"].at[0], x2, r["l_s"].at[1])
    load2.start()
    load1.start()
    barrier = pltpu.get_barrier_semaphore()
    peers = [sibling, twin, far]
    for d in range(1, 4):
        for c_ in (c, 1 - c):
            peers.append(dev((z + d) % 4, y, xh, c_))
            peers.append(dev(z, (y + d) % 4, xh, c_))
    for peer in peers:
        pl.semaphore_signal(barrier, inc=1, device_id=peer, device_id_type=MESH)
    pl.semaphore_wait(barrier, len(peers))
    exchange(0, FROM_HBM)
    load2.wait()
    exchange(FROM_HBM, BATCHES[0])
    load1.wait()
    collect()

    upper, diag = masks()
    eye = jnp.where(diag, 1.0, 0.0).astype(F32)
    row8 = iota((8, HD), 0)

    def gram(h):
        ch, zz, yy, p = places(h)
        cols = columns(h)
        ab = jnp.concatenate([x1[:, cols], x2[:, cols]], axis=1)
        g = dot_t(ab, ab)
        sums = jnp.dot(jnp.ones((8, ab.shape[0]), ab.dtype), ab, preferred_element_type=F32)
        g1_, cr, g2_ = g[:HD, :HD], g[:HD, HD:], g[HD:, HD:]
        packed = jnp.where(upper, g1_, g2_)
        dg = jnp.sum(jnp.where(diag, g2_, 0.0), axis=0, keepdims=True)
        aux = jnp.where(
            row8 == 0, sums[:, :HD],
            jnp.where(row8 == 1, sums[:, HD:], jnp.where(row8 == 2, jnp.broadcast_to(dg, (8, HD)), 0.0)),
        )
        r["pa"][ch, zz, p, 0:64] = packed[:64]
        r["pa"][ch, zz, p, 64:72] = aux
        r["pb"][ch, yy, p] = packed[64:]
        r["ca"][ch, zz, p] = cr[:64]
        r["cb"][ch, yy, p] = cr[64:]

    def cross(p, which):
        arrive(x2o.at[p, pl.ds(4 * which, 4)], r["x_q"].at[2 * p + which])
        for j in range(4 * which, 4 * which + 4):
            half, zz, h = part_head(p, j)
            yy = (zz + p) % 4
            cr = dot_t(x1[:, columns(h)], x2o[p, j])
            r["da"][p, half, zz] = cr[:64]
            r["db"][p, half, yy] = cr[64:]
            if j == 3:
                for name in LATE:
                    launch(
                        rcopy(
                            r[name].at[p, 1 - c], r[name + "_r1"].at[p], r[name + "_s"].at[p],
                            r[name + "_q"].at[p], sibling,
                        )
                    )

    def cross_s2(p):
        for name, axis in LATE.items():
            buf, r1 = r[name], r[name + "_r1"]
            u, v = uv(axis)
            arrive(r1.at[p], r[name + "_q"].at[p])
            for i in range(4):
                buf[p, c, i] = buf[p, c, i] + r1[p, i]
            for d in (1, 3, 2):
                to = (u + d) % 4
                launch(
                    rcopy(
                        buf.at[p, c, to], r[name + "_r2"].at[p, d - 1], r[name + "_s"].at[2 + 3 * (p + 1) + d - 1],
                        r[name + "_q"].at[2 + 3 * (p + 1) + d - 1], dev_uv(axis, to, v, xh),
                    )
                )

    def cross_s2_sum(p):
        for name, axis in LATE.items():
            buf, r2 = r[name], r[name + "_r2"]
            u, _ = uv(axis)
            for d in (1, 2, 3):
                arrive(r2.at[p, d - 1], r[name + "_q"].at[2 + 3 * (p + 1) + d - 1])
            r[name + "x_acc"][p] = (buf[p, c, u] + r2[p, 0]) + (r2[p, 1] + r2[p, 2])

    def last_s3():
        away = jnp.where(c == 0, y - z + 4, z - own_last + 4) % 4
        slot = away * 2 + 1 - xh
        launch(
            rcopy(
                r["d4"], r["r5"].at[slot], r["d4_s"].at[0], r["d4_q"].at[slot],
                dev(own_last, (own_last + 2 * c) % 4, 1, c),
            ),
            no(late_owner),
        )

    def last_total():
        for slot in range(1, 8):
            arrive(r["r5"].at[slot], r["d4_q"].at[slot])
        total = r["d4"][...] + r["r5"][1]
        for slot in range(2, 8):
            total = total + r["r5"][slot]
        return total

    def only_row0(row):
        return jnp.where(row8 == 0, jnp.broadcast_to(row, (8, HD)), 0.0)

    def mean_term(sums):
        mean1 = only_row0(r["aux"][0:1, :]) / tokens
        return dot_t(mean1, only_row0(sums) / tokens, HI)

    def similarity(raw, means, w2):
        white = mm(mm(r["w12"][0], raw / tokens - means), w2)
        sq = jnp.sum(jnp.sum(white * white, axis=1, keepdims=True), axis=0, keepdims=True)
        return jnp.broadcast_to(sq / HD, (1, HD))

    def whiten():
        top = s4_total("pa", True)
        low = s4_total("pb", True)
        aux = top[64:72]
        grams = unpack(top[:64], low, aux)
        ys, zs, scales = [], [], []
        for n in (0, 1):
            mean = only_row0(aux[n : n + 1, :]) / tokens
            cov = grams[n] / tokens - dot_t(mean, mean, HI) + RIDGE * eye
            sq = jnp.sum(jnp.sum(cov * cov, axis=1, keepdims=True), axis=0, keepdims=True)
            scale = jnp.sqrt(sq)
            scales.append(scale)
            ys.append(cov / scale)
        for it in range(ITERS):
            for n in (0, 1):
                if it == 0:
                    f = 1.5 * eye - 0.5 * ys[n]
                    zs.append(f)
                else:
                    f = 1.5 * eye - 0.5 * mm(zs[n], ys[n])
                    zs[n] = mm(f, zs[n])
                if it < ITERS - 1:
                    ys[n] = mm(ys[n], f)
        w1 = zs[0] / jnp.sqrt(scales[0])
        w2 = zs[1] / jnp.sqrt(scales[1])
        wp = jnp.where(upper, w1, w2)
        wd = jnp.sum(jnp.where(diag, w2, 0.0), axis=0, keepdims=True)
        r["wa"][c, z, own, 0:64] = wp[:64]
        r["wa"][c, z, own, 64:72] = jnp.broadcast_to(wd, (8, HD))
        r["wb"][c, y, own] = wp[64:]
        g1("wa")
        g1("wb")
        r["w12"][0] = w1
        r["w12"][1] = w2
        r["aux"][...] = aux
        r["w_out_x"][0:64] = fold(w2)
        r["w_out_x"][64:72] = jnp.where(row8 == 2, jnp.broadcast_to(wd, (8, HD)), aux)
    def both(p):
        cross(p, 0)
        cross(p, 1)

    loop(HALF, lambda i: gram((1 - c) * HALF + i), unroll=2)
    for name in CHAINS:
        s1(name)
    loop(HALF, lambda i: gram(c * HALF + i), unroll=2)
    for name in ("pa", "pb"):
        s1_sum(name)
        s2(name)
    for name in ("ca", "cb"):
        s1_sum(name)
    both(0)
    for name in ("pa", "pb"):
        s2_sum(name)
        s3(name, CHAINS[name][1], range(5))
    for name in ("pa", "pb"):
        s3_sum(name, True)
        s4(name, True)
    exchange(BATCHES[0], BATCHES[1])
    for name in ("ca", "cb"):
        s2(name)
    cross_s2(0)
    pl.when(owner)(whiten)
    exchange(BATCHES[1], BATCHES[2])
    for name in GATHERS:
        g1_arrive(name)
        g2(name)
    both(1)
    cross_s2(1)
    for name in ("ca", "cb"):
        s2_sum(name)
        s3(name, CHAINS[name][1], range(5))
    for name in GATHERS:
        g2_arrive(name)
        g3(name)
    collected(1)
    exchange(BATCHES[2], 8 * PARTS)

    @pl.when(owner)
    def _():
        rcopy(r["w_out_x"], r["w_in_x"], r["y_s"].at[0], r["y_q"].at[0], twin).start()

    both(2)
    cross_s2(2)
    cross_s2_sum(0)
    cross_s2_sum(1)

    lane_head = c * HALF + jnp.where(own == 4, 16 + z, head_of(z, own))
    lanes = iota((1, HD), 1)
    sa_mine = r["sa"].at[(c * 4 + z) * 5 + own]

    def own_similarity():
        raw = jnp.concatenate([s4_total("ca", True), s4_total("cb", True)], axis=0)
        sim = similarity(raw, mean_term(r["aux"][1:2, :]), r["w12"][1])
        sa_mine[...] = jnp.where(lanes == 64 * lay + lane_head, sim, 0.0)
        arrive(r["w_in_x"], r["y_q"].at[0])
        r["means"][...] = mean_term(r["w_in_x"][65:66])
        r["w2_other"][...] = unfold(r["w_in_x"][0:64], r["w_in_x"][66:67])

    def other_similarity(raw):
        sim = similarity(raw, r["means"][...], r["w2_other"][...])
        sa_mine[...] = jnp.where(lanes == 64 * (1 - lay) + lane_head, sim, sa_mine[...])
        steps = (2, 1, 3, 0)
        z_at = [(z + d) % 4 * 16 for d in range(4)]
        y_at = [(y + d) % 4 * 4 for d in range(4)]
        x_at = [(xh + d) % 2 * 2 for d in range(2)]
        c_at = [(c + d) % 2 for d in range(2)]
        for dx in (1, 0):
            for dz in steps:
                for dy in steps:
                    for dc in (1, 0):
                        if dx or dz or dy or dc:
                            to = z_at[dz] + y_at[dy] + (x_at[dx] + c_at[dc])
                            rcopy(sa_mine, sa_mine, r["sa_s"].at[0], r["sa_q"].at[0], (to, lay)).start()

    def emit(h):
        ch, zz, yy, p = places(h)
        w1, w2 = unpack(r["wa"][ch, zz, p, 0:64], r["wb"][ch, yy, p], r["wa"][ch, zz, p, 64:72])
        r["w"][0, h] = w1
        r["w"][1, h] = w2

    both(3)
    for name in GATHERS:
        g3_arrive(name)
        g4(name)
    cross_s2(3)
    cross_s2_sum(2)
    for name, axis in LATE.items():
        s3(name + "x", axis, range(3))
    for name in ("ca", "cb"):
        s3_sum(name, True)
    early = list(pending)
    pending.clear()
    for name in ("ca", "cb"):
        s4(name, True)
    cross_s2_sum(3)
    for name, axis in LATE.items():
        s3(name + "x", axis, (3,))
    for name in GATHERS:
        g4_arrive(name)
    loop(HEADS, emit, unroll=2)
    collected(0)
    drain(early)
    for i in range(2 * PARTS - 2):
        exchange_sent(i)
    last_cross(0)
    last_cross(1)
    last_s3()
    for name in LATE:
        s3_sum(name + "x", False)
        s4(name + "x", False)
    pl.when(owner)(own_similarity)

    @pl.when(early_owner)
    def _():
        other_similarity(jnp.concatenate([s4_total("dax", False), s4_total("dbx", False)], axis=0))

    @pl.when(late_owner)
    def _():
        other_similarity(last_total())

    pl.when(owner)(lambda: arrive(r["sa"].at[pl.ds(0, HEADS - 1)], r["sa_q"].at[0]))
    pl.when(no(owner))(lambda: arrive(r["sa"].at[pl.ds(0, HEADS)], r["sa_q"].at[0]))
    total = r["sa"][0]
    for i in range(1, HEADS):
        total = total + r["sa"][i]
    r["sim"][0:1, :] = total[:, 0:HEADS]
    r["sim"][1:2, :] = total[:, 64 : 64 + HEADS]

    drain(pending)
    for i in (2 * PARTS - 2, 2 * PARTS - 1):
        exchange_sent(i)

    @pl.when(owner)
    def _():
        for name in GATHERS:
            u, _ = uv(GATHERS[name][1])
            place = r[name].at[c, u, own]
            rcopy(place, place, r[name + "_s"].at[0], r[name + "_q"].at[0], far).wait_send()
        rcopy(r["w_out_x"], r["w_in_x"], r["y_s"].at[0], r["y_q"].at[0], twin).wait_send()
        sent = r["sa"].at[pl.ds(0, others)]
        rcopy(sent, sent, r["sa_s"].at[0], r["sa_q"].at[0], far).wait_send()


def gather_kernel(tokens, first_acts, second_acts):
    rows, width = first_acts.shape[1:]
    names = ["x1_hbm", "x2_hbm", "w", "sim"]
    scratch = []

    def add(name, spec):
        names.append(name)
        scratch.append(spec)

    dma = lambda n: pltpu.SemaphoreType.DMA((n,))
    for name in ("x1", "x2"):
        add(name, pltpu.VMEM((rows, width), first_acts.dtype))
    add("x2o", pltpu.VMEM((PARTS, 8, rows, HD), first_acts.dtype))
    for name, (n, _) in CHAINS.items():
        add(name, pltpu.VMEM((2, 4, 5, n, HD), F32))
        add(name + "_r1", pltpu.VMEM((4, 5, n, HD), F32))
        add(name + "_r2", pltpu.VMEM((3, 5, n, HD), F32))
    for name in LATE:
        add(name, pltpu.VMEM((PARTS - 1, 2, 4, 64, HD), F32))
        add(name + "_r1", pltpu.VMEM((PARTS - 1, 4, 64, HD), F32))
        add(name + "_r2", pltpu.VMEM((PARTS - 1, 3, 64, HD), F32))
        add(name + "_s", dma(17))
        add(name + "_q", dma(17))
    for name in ("m1", "m2"):
        add(name, pltpu.VMEM((7, rows, HD), first_acts.dtype))
    add("m3", pltpu.VMEM((2, rows, HD), first_acts.dtype))
    add("m3_s", dma(4))
    add("m3_q", dma(2))
    add("m_s", dma(16))
    add("m_q", dma(14))
    add("d4", pltpu.VMEM((HD, HD), F32))
    add("r5", pltpu.VMEM((8, HD, HD), F32))
    add("d4_s", dma(1))
    add("d4_q", dma(8))
    add("means", pltpu.VMEM((HD, HD), F32))
    for name, n in [(k, v[0]) for k, v in CHAINS.items()] + [(k + "x", 64) for k in LATE]:
        add(name + "_acc", pltpu.VMEM((5, n, HD), F32))
        add(name + "_r3", pltpu.VMEM((2, 3, n, HD), F32))
        add(name + "_t", pltpu.VMEM((2, n, HD), F32))
        add(name + "_r4", pltpu.VMEM((n, HD), F32))
        add(name + "_s", dma(10))
        add(name + "_q", dma(11))
    add("sa", pltpu.VMEM((64, 1, HD), F32))
    for name, (n, _) in GATHERS.items():
        add(name, pltpu.VMEM((2, 4, 5, n, HD), F32))
        add(name + "_s", dma(11))
        add(name + "_q", dma(10))
    add("sa_s", dma(1))
    add("sa_q", dma(1))
    add("w12", pltpu.VMEM((2, HD, HD), F32))
    add("aux", pltpu.VMEM((8, HD), F32))
    add("w_out_x", pltpu.VMEM((72, HD), F32))
    add("w_in_x", pltpu.VMEM((72, HD), F32))
    add("w2_other", pltpu.VMEM((HD, HD), F32))
    add("l_s", dma(2))
    add("x_s", dma(2 * PARTS))
    add("x_q", dma(2 * PARTS))
    add("y_s", dma(1))
    add("y_q", dma(1))
    add("none", dma(1))
    return pl.pallas_call(
        functools.partial(kernel, tokens, names),
        out_shape=(
            pltpu.VMEM((2, HEADS, HD, HD), F32),
            pltpu.VMEM((2, HEADS), F32),
        ),
        in_specs=[pl.BlockSpec(memory_space=pltpu.HBM)] * 2,
        out_specs=[pl.BlockSpec(memory_space=pltpu.VMEM)] * 2,
        scratch_shapes=scratch,
        compiler_params=pltpu.CompilerParams(
            collective_id=0, has_side_effects=True, vmem_limit_bytes=VMEM_LIMIT
        ),
    )(
        pltpu.with_memory_space_constraint(first_acts, pltpu.HBM),
        pltpu.with_memory_space_constraint(second_acts, pltpu.HBM),
    )


PIECES = 4


def store_kernel(w, sim, w_hbm, s_hbm, sems):
    step = HEADS // PIECES
    copies = [
        pltpu.make_async_copy(
            w.at[n, pl.ds(q * step, step)], w_hbm.at[n, 0, pl.ds(q * step, step)], sems.at[n * PIECES + q]
        )
        for n in range(2)
        for q in range(PIECES)
    ]
    copies.append(pltpu.make_async_copy(sim, s_hbm.at[0], sems.at[2 * PIECES]))
    for copy in copies:
        copy.start()
    for copy in copies:
        copy.wait()


def store(w, sim):
    vmem, hbm = pl.BlockSpec(memory_space=pltpu.VMEM), pl.BlockSpec(memory_space=pltpu.HBM)
    return pl.pallas_call(
        store_kernel,
        out_shape=(
            jax.ShapeDtypeStruct((2, 1, HEADS, HD, HD), F32),
            jax.ShapeDtypeStruct((1, 2, HEADS), F32),
        ),
        in_specs=[vmem] * 2,
        out_specs=(hbm, hbm),
        scratch_shapes=[pltpu.SemaphoreType.DMA((2 * PIECES + 1,))],
        compiler_params=pltpu.CompilerParams(vmem_limit_bytes=16 * 2**20),
    )(w, sim)


def solution(mesh):
    def whole(first_acts, second_acts):
        tokens = first_acts.shape[1] * lax.axis_size("tok")
        return store(*gather_kernel(tokens, first_acts, second_acts))

    in_specs = (P("lay", "tok", None), P("lay", "tok", None))
    out_specs = (P(None, "lay", None, None, None), P("lay", None, None))
    return jax.shard_map(whole, mesh=mesh, in_specs=in_specs, out_specs=out_specs, check_vma=False)
```

```python
import functools

import jax
import jax.numpy as jnp
from jax import lax
from jax.experimental import pallas as pl
from jax.experimental.pallas import tpu as pltpu
from jax.sharding import PartitionSpec as P

HEADS = 40
HD = 128
ITERS = 6
RIDGE = 0.05
HALF = HEADS // 2
PARTS = 5
FROM_HBM = 3
BATCHES = (15, 21, 32)
CARRIED = (3, 7)
VMEM_LIMIT = 48 * 2**20
F32 = jnp.float32
HI = lax.Precision.HIGHEST
MESH = pl.DeviceIdType.MESH

CHAINS = {"pa": (72, "z"), "pb": (64, "y"), "ca": (64, "z"), "cb": (64, "y")}
LATE = {"da": "z", "db": "y"}
GATHERS = {"wa": (72, "z"), "wb": (64, "y")}


def iota(shape, dim):
    return lax.broadcasted_iota(jnp.int32, shape, dim)


def dot_t(a, b, precision=None):
    return lax.dot_general(
        a, b, (((0,), (0,)), ((), ())), precision=precision, preferred_element_type=F32
    )


def mm(a, b):
    return jnp.dot(a, b, precision=HI, preferred_element_type=F32)


def masks():
    ri, ci = iota((HD, HD), 0), iota((HD, HD), 1)
    return ri <= ci, ri == ci


def unpack(top, low, aux):
    upper, diag = masks()
    p = jnp.concatenate([top, low], axis=0)
    pt = p.T
    first = jnp.where(upper, p, pt)
    second = jnp.where(upper, jnp.where(diag, aux[2:3, :], pt), p)
    return first, second


def fold(w):
    row, lane = iota((64, HD), 0), iota((64, HD), 1)
    lower = jnp.logical_and(lane < 64, row > lane)
    return jnp.where(lower, pltpu.roll(w[64:], 64, 1), w[:64])


def unfold(folded, diagonal):
    row, lane = iota((HD, HD), 0), iota((HD, HD), 1)
    q = jnp.concatenate([folded, pltpu.roll(folded, 64, 1)], axis=0)
    top = jnp.logical_and(row < 64, row <= lane)
    low = jnp.logical_and(lane >= 64, row > lane)
    out = jnp.where(jnp.logical_or(top, low), q, q.T)
    return jnp.where(jnp.logical_and(row == lane, row >= 64), diagonal, out)


def head_of(z, p):
    k = 4 * ((z + p) % 4) + z
    if isinstance(p, int):
        return 16 + z if p == 4 else k
    return jnp.where(p == 4, 16 + z, k)


def places(h):
    k = h % HALF
    z = k % 4
    half = h // HALF
    y = jnp.where(k < 16, k // 4, (z + 2 * half) % 4)
    p = jnp.where(k < 16, (k // 4 - z + 4) % 4, 4)
    return half, z, y, p


def kernel(tokens, names, *refs):
    r = dict(zip(names, refs))
    tok = lax.axis_index("tok")
    lay = lax.axis_index("lay")
    c = tok % 2
    xh = (tok // 2) % 2
    y = (tok // 4) % 4
    z = tok // 16

    def dev(z_, y_, xh_, c_):
        return (((z_ * 4 + y_) * 2 + xh_) * 2 + c_, lay)

    def uv(axis):
        return (z, y) if axis == "z" else (y, z)

    def dev_uv(axis, u, v, xh_):
        return dev(u, v, xh_, c) if axis == "z" else dev(v, u, xh_, c)

    sibling = dev(z, y, xh, 1 - c)
    twin = (tok, 1 - lay)
    far = dev(z, y, 1 - xh, c)

    on_diag = y == (z + 2 * c) % 4
    main = (y - z + 4) % 4
    owns_main = xh == main % 2
    owner = jnp.logical_or(owns_main, on_diag)
    own = jnp.where(owns_main, main, 4)
    late_owner = jnp.logical_and(on_diag, xh == 1)
    early_owner = owns_main
    extra_mine = jnp.where(owns_main, 0, 1)
    extra_give = jnp.where(owns_main, 1, 0)
    gives = jnp.logical_or(on_diag, jnp.logical_not(owns_main))
    no = jnp.logical_not

    def target(axis, p):
        u, _ = uv(axis)
        if p == 4:
            return (u + 2 * c) % 4
        return (u + p) % 4 if axis == "z" else (u - p + 4) % 4

    def rcopy(src, dst, ssem, rsem, device):
        return pltpu.make_async_remote_copy(
            src_ref=src, dst_ref=dst, send_sem=ssem, recv_sem=rsem,
            device_id=device, device_id_type=MESH,
        )

    others = lax.axis_size("tok") - 1
    def launch(copy, cond=None):
        if cond is None:
            copy.start()
        else:
            pl.when(cond)(lambda: copy.start())

    def left(ref, sem, cond=None):
        copy = rcopy(ref, ref, sem, r["l_s"].at[0], twin)
        if cond is None:
            copy.wait_send()
        else:
            pl.when(cond)(lambda: copy.wait_send())

    def arrive(ref, sem, cond=None):
        copy = rcopy(ref, ref, r["l_s"].at[0], sem, twin)
        if cond is None:
            copy.wait_recv()
        else:
            pl.when(cond)(lambda: copy.wait_recv())

    def loop(n, body, unroll=1):
        def step(i, carry):
            body(i)
            return carry

        lax.fori_loop(0, n, step, 0, unroll=unroll)

    def s1(name):
        launch(rcopy(r[name].at[1 - c], r[name + "_r1"], r[name + "_s"].at[0], r[name + "_q"].at[0], sibling))

    def s1_sum(name):
        buf, r1 = r[name], r[name + "_r1"]
        arrive(r1, r[name + "_q"].at[0])

        def body(i):
            for s in range(5):
                buf[c, i, s] = buf[c, i, s] + r1[i, s]

        loop(4, body)

    def s2(name, offsets=(1, 3, 2)):
        axis = CHAINS[name][1]
        u, v = uv(axis)
        for d in offsets:
            to = (u + d) % 4
            launch(
                rcopy(
                    r[name].at[c, to], r[name + "_r2"].at[d - 1], r[name + "_s"].at[1],
                    r[name + "_q"].at[1], dev_uv(axis, to, v, xh),
                )
            )

    def s2_sum(name):
        u, _ = uv(CHAINS[name][1])
        buf, r2, acc = r[name], r[name + "_r2"], r[name + "_acc"]
        arrive(r2, r[name + "_q"].at[1])
        for s in range(5):
            acc[s] = (buf[c, u, s] + r2[0, s]) + (r2[1, s] + r2[2, s])

    def s3(name, axis, slots):
        u, v = uv(axis)
        for p in slots:
            vo = target(axis, p)
            off = jnp.maximum((v - vo + 4) % 4, 1) - 1
            kind = p // 4
            launch(
                rcopy(
                    r[name + "_acc"].at[p], r[name + "_r3"].at[kind, off], r[name + "_s"].at[2],
                    r[name + "_q"].at[2 + kind], dev_uv(axis, u, vo, xh),
                ),
                v != vo,
            )

    def s3_sum(name, extra):
        acc, r3, part = r[name + "_acc"], r[name + "_r3"], r[name + "_t"]

        def add(kind, slot):
            arrive(r3.at[kind], r[name + "_q"].at[2 + kind])
            part[kind] = (acc[slot] + r3[kind, 0]) + (r3[kind, 1] + r3[kind, 2])

        add(0, main)
        if extra:
            pl.when(on_diag)(lambda: add(1, 4))

    def s4(name, extra):
        src = r[name + "_t"].at[extra_give] if extra else r[name + "_t"].at[0]
        cond = gives if extra else no(owns_main)
        launch(rcopy(src, r[name + "_r4"], r[name + "_s"].at[3], r[name + "_q"].at[4], far), cond)

    def s4_total(name, extra):
        arrive(r[name + "_r4"], r[name + "_q"].at[4])
        mine = r[name + "_t"][extra_mine] if extra else r[name + "_t"][0]
        return mine + r[name + "_r4"][...]

    def chain_left(name):
        acc = r[name + "_acc"]
        left(r[name + "_r1"], r[name + "_s"].at[0])
        left(r[name + "_r2"], r[name + "_s"].at[1])
        left(acc.at[pl.ds(0, 3)], r[name + "_s"].at[2], on_diag)
        left(acc.at[pl.ds(0, 4)], r[name + "_s"].at[2], no(on_diag))

    def given(name, cond):
        left(r[name + "_r4"], r[name + "_s"].at[3], cond)

    def g1(name):
        u, _ = uv(GATHERS[name][1])
        place = r[name].at[c, u, own]
        rcopy(place, place, r[name + "_s"].at[0], r[name + "_q"].at[0], far).start()

    def g1_arrive(name):
        u, _ = uv(GATHERS[name][1])
        arrive(r[name].at[c, u, jnp.where(owns_main, 4, main)], r[name + "_q"].at[0], gives)

    def g2(name):
        axis = GATHERS[name][1]
        u, v = uv(axis)
        for d in (1, 3, 2):
            for kind in (0, 1):
                slot = 4 if kind else main
                place = r[name].at[c, u, slot]
                launch(
                    rcopy(
                        place, place, r[name + "_s"].at[1], r[name + "_q"].at[1],
                        dev_uv(axis, u, (v + d) % 4, xh),
                    ),
                    on_diag if kind else None,
                )

    def g2_arrive(name):
        u, _ = uv(GATHERS[name][1])
        arrive(r[name].at[c, u, pl.ds(0, 3)], r[name + "_q"].at[1], on_diag)
        arrive(r[name].at[c, u, pl.ds(0, 4)], r[name + "_q"].at[1], no(on_diag))

    def g3(name):
        axis = GATHERS[name][1]
        u, v = uv(axis)
        place = r[name].at[c, u]
        for d in (1, 3, 2):
            launch(
                rcopy(
                    place, place, r[name + "_s"].at[2], r[name + "_q"].at[2],
                    dev_uv(axis, (u + d) % 4, v, xh),
                )
            )

    def g3_arrive(name):
        arrive(r[name].at[c, pl.ds(0, 3)], r[name + "_q"].at[2])

    def g4(name):
        place = r[name].at[c]
        launch(rcopy(place, place, r[name + "_s"].at[3], r[name + "_q"].at[3], sibling))

    def g4_arrive(name):
        arrive(r[name].at[1 - c], r[name + "_q"].at[3])

    def gather_left(name):
        buf, sems = r[name], r[name + "_s"]
        left(buf.at[c, 0, 0], sems.at[0], owner)
        left(buf.at[c, pl.ds(0, 2), pl.ds(0, 3)], sems.at[1], on_diag)
        left(buf.at[c, 0, pl.ds(0, 3)], sems.at[1], no(on_diag))
        left(buf.at[c, pl.ds(0, 3)], sems.at[2])
        left(buf.at[c], sems.at[3])

    x1, x2, x2o = r["x1"], r["x2"], r["x2o"]

    def part_head(p, j):
        half = (1 - c) if j < 4 else c
        return half, j % 4, half * HALF + head_of(j % 4, p)

    own_last = jnp.where(c == 0, z, (y + 2) % 4)

    def last_head(z_, c_):
        return c_ * HALF + 16 + z_

    def columns(h):
        return pl.ds(pl.multiple_of(h * HD, HD), HD)

    def exchange(lo, hi):
        for n in range(lo, hi):
            p, j = n // 8, n % 8
            _, _, h = part_head(p, j)
            src = r["x2_hbm"].at[0, :, columns(h)] if n < FROM_HBM else x2.at[:, columns(h)]
            if p == 4:
                src = x2.at[:, columns(last_head(own_last, c))] if j == 0 else r["m2"].at[j - 1]
            sem = 2 * p + j // 4
            copy = rcopy(src, x2o.at[p, j], r["x_s"].at[p // 4], r["x_q"].at[sem], twin)
            if p == 4 and j in CARRIED:
                pl.when(c == 1)(lambda copy=copy: copy.start())
            else:
                copy.start()
            if n == 8 * PARTS - 5:
                for i, k in enumerate(CARRIED):
                    launch(
                        rcopy(
                            r["m3"].at[i], x2o.at[4, k], r["x_s"].at[1], r["x_q"].at[8 + k // 4],
                            (jnp.maximum(tok, 1) - 1, 1 - lay),
                        ),
                        c == 1,
                    )

    def collect():
        for d in (1, 3, 2, 0):
            for c_ in (0, 1):
                if c_ == 0:
                    w_, to, other = (z + d) % 4, dev((z + d) % 4, y, xh, 0), c
                else:
                    w_, to, other = (y + d + 2) % 4, dev(z, (y + d) % 4, xh, 1), 1 - c
                slot = jnp.maximum(2 * d + other, 1) - 1
                cols = columns(last_head(w_, c_))
                for n, x in ((1, x2), (0, x1)):
                    cond = None if d else other == 1
                    carried = n == 1 and c_ == 0 and 2 * d + 1 in CARRIED
                    if carried:
                        i = CARRIED.index(2 * d + 1)
                        launch(
                            rcopy(
                                x.at[:, cols], r["m3"].at[i], r["m_s"].at[1], r["m_q"].at[2],
                                dev(w_, y, xh, 1),
                            ),
                            c == 1,
                        )
                        cond = c == 0
                    launch(
                        rcopy(
                            x.at[:, cols], r["m%d" % (n + 1)].at[slot], r["m_s"].at[n],
                            r["m_q"].at[n], to,
                        ),
                        cond,
                    )

    def collected(n):
        if n == 0:
            arrive(r["m1"], r["m_q"].at[0])
        else:
            arrive(r["m2"], r["m_q"].at[1], c == 1)
            arrive(r["m2"].at[pl.ds(0, 7 - len(CARRIED))], r["m_q"].at[1], c == 0)
            arrive(r["m3"], r["m_q"].at[2], c == 1)

    def last_cross(which):
        arrive(x2o.at[4, pl.ds(4 * which, 4)], r["x_q"].at[8 + which])
        total = None
        for j in range(4 * which, 4 * which + 4):
            left = r["m1"][j - 1] if j else x1[:, columns(last_head(own_last, c))]
            cr = dot_t(left, x2o[4, j])
            total = cr if total is None else total + cr
        r["d4"][...] = r["d4"][...] + total if which else total

    def exchange_left(last):
        if last:
            left(x2o.at[pl.ds(0, 2), pl.ds(0, 5)], r["x_s"].at[1], c == 1)
            left(x2o.at[0, pl.ds(0, 6)], r["x_s"].at[1], c == 0)
        else:
            left(x2o.at[pl.ds(0, 4)], r["x_s"].at[0])

    load1 = pltpu.make_async_copy(r["x1_hbm"].at[0], x1, r["l_s"].at[0])
    load2 = pltpu.make_async_copy(r["x2_hbm"].at[0], x2, r["l_s"].at[1])
    load2.start()
    load1.start()
    barrier = pltpu.get_barrier_semaphore()
    peers = [sibling, twin, far]
    for d in range(1, 4):
        for c_ in (c, 1 - c):
            peers.append(dev((z + d) % 4, y, xh, c_))
            peers.append(dev(z, (y + d) % 4, xh, c_))
    for peer in peers:
        pl.semaphore_signal(barrier, inc=1, device_id=peer, device_id_type=MESH)
    pl.semaphore_wait(barrier, len(peers))
    exchange(0, FROM_HBM)
    load2.wait()
    exchange(FROM_HBM, BATCHES[0])
    load1.wait()
    collect()

    upper, diag = masks()
    eye = jnp.where(diag, 1.0, 0.0).astype(F32)
    row8 = iota((8, HD), 0)

    def gram(h):
        ch, zz, yy, p = places(h)
        cols = columns(h)
        ab = jnp.concatenate([x1[:, cols], x2[:, cols]], axis=1)
        g = dot_t(ab, ab)
        sums = jnp.dot(jnp.ones((8, ab.shape[0]), ab.dtype), ab, preferred_element_type=F32)
        g1_, cr, g2_ = g[:HD, :HD], g[:HD, HD:], g[HD:, HD:]
        packed = jnp.where(upper, g1_, g2_)
        dg = jnp.sum(jnp.where(diag, g2_, 0.0), axis=0, keepdims=True)
        aux = jnp.where(
            row8 == 0, sums[:, :HD],
            jnp.where(row8 == 1, sums[:, HD:], jnp.where(row8 == 2, jnp.broadcast_to(dg, (8, HD)), 0.0)),
        )
        r["pa"][ch, zz, p, 0:64] = packed[:64]
        r["pa"][ch, zz, p, 64:72] = aux
        r["pb"][ch, yy, p] = packed[64:]
        r["ca"][ch, zz, p] = cr[:64]
        r["cb"][ch, yy, p] = cr[64:]

    def cross(p, which):
        arrive(x2o.at[p, pl.ds(4 * which, 4)], r["x_q"].at[2 * p + which])
        for j in range(4 * which, 4 * which + 4):
            half, zz, h = part_head(p, j)
            yy = (zz + p) % 4
            cr = dot_t(x1[:, columns(h)], x2o[p, j])
            r["da"][p, half, zz] = cr[:64]
            r["db"][p, half, yy] = cr[64:]
            if j == 3:
                for name in LATE:
                    launch(
                        rcopy(
                            r[name].at[p, 1 - c], r[name + "_r1"].at[p], r["late_s"].at[0],
                            r["late_q"].at[p], sibling,
                        )
                    )

    def cross_s2(p):
        arrive(r["da_r1"].at[pl.ds(0, 2)], r["late_q"].at[p])
        for name, axis in LATE.items():
            buf, r1 = r[name], r[name + "_r1"]
            u, v = uv(axis)
            for i in range(4):
                buf[p, c, i] = buf[p, c, i] + r1[p, i]
            for d in (1, 3, 2):
                to = (u + d) % 4
                launch(
                    rcopy(
                        buf.at[p, c, to], r[name + "_r2"].at[p, d - 1], r["late_s"].at[1],
                        r["late_q"].at[4 + p], dev_uv(axis, to, v, xh),
                    )
                )

    def cross_s2_sum(p):
        arrive(r["da_r2"].at[pl.ds(0, 2)], r["late_q"].at[4 + p])
        for name, axis in LATE.items():
            buf, r2 = r[name], r[name + "_r2"]
            u, _ = uv(axis)
            r[name + "x_acc"][p] = (buf[p, c, u] + r2[p, 0]) + (r2[p, 1] + r2[p, 2])

    def last_s3():
        away = jnp.where(c == 0, y - z + 4, z - own_last + 4) % 4
        slot = jnp.maximum(away * 2 + 1 - xh, 1)
        launch(
            rcopy(
                r["d4"], r["r5"].at[slot - 1], r["d4_s"].at[0], r["d4_q"].at[0],
                dev(own_last, (own_last + 2 * c) % 4, 1, c),
            ),
            no(late_owner),
        )

    def last_total():
        arrive(r["r5"], r["d4_q"].at[0])
        total = r["d4"][...] + r["r5"][0]
        for slot in range(1, 7):
            total = total + r["r5"][slot]
        return total

    def only_row0(row):
        return jnp.where(row8 == 0, jnp.broadcast_to(row, (8, HD)), 0.0)

    def mean_term(sums):
        mean1 = only_row0(r["aux"][0:1, :]) / tokens
        return dot_t(mean1, only_row0(sums) / tokens, HI)

    def similarity(raw, means, w2):
        white = mm(mm(r["w12"][0], raw / tokens - means), w2)
        sq = jnp.sum(jnp.sum(white * white, axis=1, keepdims=True), axis=0, keepdims=True)
        return jnp.broadcast_to(sq / HD, (1, HD))

    def whiten():
        top = s4_total("pa", True)
        low = s4_total("pb", True)
        aux = top[64:72]
        grams = unpack(top[:64], low, aux)
        ys, zs, scales = [], [], []
        for n in (0, 1):
            mean = only_row0(aux[n : n + 1, :]) / tokens
            cov = grams[n] / tokens - dot_t(mean, mean, HI) + RIDGE * eye
            sq = jnp.sum(jnp.sum(cov * cov, axis=1, keepdims=True), axis=0, keepdims=True)
            scale = jnp.sqrt(sq)
            scales.append(scale)
            ys.append(cov / scale)
        for it in range(ITERS):
            for n in (0, 1):
                if it == 0:
                    f = 1.5 * eye - 0.5 * ys[n]
                    zs.append(f)
                else:
                    f = 1.5 * eye - 0.5 * mm(zs[n], ys[n])
                    zs[n] = mm(f, zs[n])
                if it < ITERS - 1:
                    ys[n] = mm(ys[n], f)
        w1 = zs[0] / jnp.sqrt(scales[0])
        w2 = zs[1] / jnp.sqrt(scales[1])
        wp = jnp.where(upper, w1, w2)
        wd = jnp.sum(jnp.where(diag, w2, 0.0), axis=0, keepdims=True)
        r["wa"][c, z, own, 0:64] = wp[:64]
        r["wa"][c, z, own, 64:72] = jnp.broadcast_to(wd, (8, HD))
        r["wb"][c, y, own] = wp[64:]
        g1("wa")
        g1("wb")
        r["w12"][0] = w1
        r["w12"][1] = w2
        r["aux"][...] = aux
        r["w_out_x"][0:64] = fold(w2)
        r["w_out_x"][64:72] = jnp.where(row8 == 2, jnp.broadcast_to(wd, (8, HD)), aux)
    def both(p):
        cross(p, 0)
        cross(p, 1)

    loop(HALF, lambda i: gram((1 - c) * HALF + i), unroll=2)
    for name in CHAINS:
        s1(name)
    loop(HALF, lambda i: gram(c * HALF + i), unroll=2)
    for name in ("pa", "pb"):
        s1_sum(name)
        s2(name)
    for name in ("ca", "cb"):
        s1_sum(name)
    both(0)
    for name in ("pa", "pb"):
        s2_sum(name)
        s3(name, CHAINS[name][1], range(5))
    for name in ("pa", "pb"):
        s3_sum(name, True)
        s4(name, True)
    exchange(BATCHES[0], BATCHES[1])
    for name in ("ca", "cb"):
        s2(name)
    cross_s2(0)
    pl.when(owner)(whiten)
    exchange(BATCHES[1], BATCHES[2])
    for name in GATHERS:
        g1_arrive(name)
        g2(name)
    both(1)
    cross_s2(1)
    for name in ("ca", "cb"):
        s2_sum(name)
        s3(name, CHAINS[name][1], range(5))
    for name in GATHERS:
        g2_arrive(name)
        g3(name)
    collected(1)
    exchange(BATCHES[2], 8 * PARTS)

    @pl.when(owner)
    def _():
        rcopy(r["w_out_x"], r["w_in_x"], r["y_s"].at[0], r["y_q"].at[0], twin).start()

    both(2)
    cross_s2(2)
    cross_s2_sum(0)
    cross_s2_sum(1)

    lane_head = c * HALF + jnp.where(own == 4, 16 + z, head_of(z, own))
    lanes = iota((1, HD), 1)
    sa_mine = r["sa"].at[(c * 4 + z) * 5 + own]

    def own_similarity():
        raw = jnp.concatenate([s4_total("ca", True), s4_total("cb", True)], axis=0)
        sim = similarity(raw, mean_term(r["aux"][1:2, :]), r["w12"][1])
        sa_mine[...] = jnp.where(lanes == 64 * lay + lane_head, sim, 0.0)
        arrive(r["w_in_x"], r["y_q"].at[0])
        r["means"][...] = mean_term(r["w_in_x"][65:66])
        r["w2_other"][...] = unfold(r["w_in_x"][0:64], r["w_in_x"][66:67])

    def other_similarity(raw):
        sim = similarity(raw, r["means"][...], r["w2_other"][...])
        sa_mine[...] = jnp.where(lanes == 64 * (1 - lay) + lane_head, sim, sa_mine[...])
        steps = (2, 1, 3, 0)
        z_at = [(z + d) % 4 * 16 for d in range(4)]
        y_at = [(y + d) % 4 * 4 for d in range(4)]
        x_at = [(xh + d) % 2 * 2 for d in range(2)]
        c_at = [(c + d) % 2 for d in range(2)]
        for dx in (1, 0):
            for dz in steps:
                for dy in steps:
                    for dc in (1, 0):
                        if dx or dz or dy or dc:
                            to = z_at[dz] + y_at[dy] + (x_at[dx] + c_at[dc])
                            rcopy(sa_mine, sa_mine, r["sa_s"].at[0], r["sa_q"].at[0], (to, lay)).start()

    def emit(h):
        ch, zz, yy, p = places(h)
        w1, w2 = unpack(r["wa"][ch, zz, p, 0:64], r["wb"][ch, yy, p], r["wa"][ch, zz, p, 64:72])
        r["w"][0, h] = w1
        r["w"][1, h] = w2

    both(3)
    for name in GATHERS:
        g3_arrive(name)
        g4(name)
    cross_s2(3)
    cross_s2_sum(2)
    for name, axis in LATE.items():
        s3(name + "x", axis, range(3))
    for name in ("ca", "cb"):
        s3_sum(name, True)
    for name in ("ca", "cb"):
        s4(name, True)
    cross_s2_sum(3)
    for name, axis in LATE.items():
        s3(name + "x", axis, (3,))
    for name in GATHERS:
        g4_arrive(name)
    loop(HEADS, emit, unroll=2)
    collected(0)
    for name in CHAINS:
        chain_left(name)
    for name in ("pa", "pb"):
        given(name, gives)
    for name in GATHERS:
        gather_left(name)
    for n in (0, 1):
        left(r["m1"], r["m_s"].at[n])
    left(r["da"], r["late_s"].at[0])
    left(r["da"].at[pl.ds(0, 3)], r["late_s"].at[1])
    exchange_left(False)
    last_cross(0)
    last_cross(1)
    last_s3()
    for name in LATE:
        s3_sum(name + "x", False)
        s4(name + "x", False)
    pl.when(owner)(own_similarity)

    @pl.when(early_owner)
    def _():
        other_similarity(jnp.concatenate([s4_total("dax", False), s4_total("dbx", False)], axis=0))

    @pl.when(late_owner)
    def _():
        other_similarity(last_total())

    pl.when(owner)(lambda: arrive(r["sa"].at[pl.ds(0, HEADS - 1)], r["sa_q"].at[0]))
    pl.when(no(owner))(lambda: arrive(r["sa"].at[pl.ds(0, HEADS)], r["sa_q"].at[0]))
    total = r["sa"][0]
    for i in range(1, HEADS):
        total = total + r["sa"][i]
    r["sim"][0:1, :] = total[:, 0:HEADS]
    r["sim"][1:2, :] = total[:, 64 : 64 + HEADS]

    exchange_left(True)
    for name in ("ca", "cb"):
        given(name, gives)
    for name in LATE:
        left(r[name + "x_acc"].at[pl.ds(0, 3)], r[name + "x_s"].at[2])
        given(name + "x", no(owns_main))
    left(r["d4"], r["d4_s"].at[0], no(late_owner))
    left(r["w_out_x"], r["y_s"].at[0], owner)
    left(r["sa"].at[pl.ds(0, others)], r["sa_s"].at[0], owner)


def gather_kernel(tokens, first_acts, second_acts):
    rows, width = first_acts.shape[1:]
    names = ["x1_hbm", "x2_hbm", "w", "sim"]
    scratch = []

    def add(name, spec):
        names.append(name)
        scratch.append(spec)

    dma = lambda n: pltpu.SemaphoreType.DMA((n,))
    for name in ("x1", "x2"):
        add(name, pltpu.VMEM((rows, width), first_acts.dtype))
    add("x2o", pltpu.VMEM((PARTS, 8, rows, HD), first_acts.dtype))
    for name, (n, _) in CHAINS.items():
        add(name, pltpu.VMEM((2, 4, 5, n, HD), F32))
        add(name + "_r1", pltpu.VMEM((4, 5, n, HD), F32))
        add(name + "_r2", pltpu.VMEM((3, 5, n, HD), F32))
    for name in LATE:
        add(name, pltpu.VMEM((PARTS - 1, 2, 4, 64, HD), F32))
        add(name + "_r1", pltpu.VMEM((PARTS - 1, 4, 64, HD), F32))
        add(name + "_r2", pltpu.VMEM((PARTS - 1, 3, 64, HD), F32))
    add("late_s", dma(2))
    add("late_q", dma(8))
    for name in ("m1", "m2"):
        add(name, pltpu.VMEM((7, rows, HD), first_acts.dtype))
    add("m3", pltpu.VMEM((2, rows, HD), first_acts.dtype))
    add("m_s", dma(2))
    add("m_q", dma(3))
    add("d4", pltpu.VMEM((HD, HD), F32))
    add("r5", pltpu.VMEM((7, HD, HD), F32))
    add("d4_s", dma(1))
    add("d4_q", dma(1))
    add("means", pltpu.VMEM((HD, HD), F32))
    for name, n in [(k, v[0]) for k, v in CHAINS.items()] + [(k + "x", 64) for k in LATE]:
        add(name + "_acc", pltpu.VMEM((5, n, HD), F32))
        add(name + "_r3", pltpu.VMEM((2, 3, n, HD), F32))
        add(name + "_t", pltpu.VMEM((2, n, HD), F32))
        add(name + "_r4", pltpu.VMEM((n, HD), F32))
        add(name + "_s", dma(4))
        add(name + "_q", dma(5))
    add("sa", pltpu.VMEM((64, 1, HD), F32))
    for name, (n, _) in GATHERS.items():
        add(name, pltpu.VMEM((2, 4, 5, n, HD), F32))
        add(name + "_s", dma(4))
        add(name + "_q", dma(4))
    add("sa_s", dma(1))
    add("sa_q", dma(1))
    add("w12", pltpu.VMEM((2, HD, HD), F32))
    add("aux", pltpu.VMEM((8, HD), F32))
    add("w_out_x", pltpu.VMEM((72, HD), F32))
    add("w_in_x", pltpu.VMEM((72, HD), F32))
    add("w2_other", pltpu.VMEM((HD, HD), F32))
    add("l_s", dma(2))
    add("x_s", dma(2))
    add("x_q", dma(2 * PARTS))
    add("y_s", dma(1))
    add("y_q", dma(1))
    return pl.pallas_call(
        functools.partial(kernel, tokens, names),
        out_shape=(
            pltpu.VMEM((2, HEADS, HD, HD), F32),
            pltpu.VMEM((2, HEADS), F32),
        ),
        in_specs=[pl.BlockSpec(memory_space=pltpu.HBM)] * 2,
        out_specs=[pl.BlockSpec(memory_space=pltpu.VMEM)] * 2,
        scratch_shapes=scratch,
        compiler_params=pltpu.CompilerParams(
            collective_id=0, has_side_effects=True, vmem_limit_bytes=VMEM_LIMIT
        ),
    )(
        pltpu.with_memory_space_constraint(first_acts, pltpu.HBM),
        pltpu.with_memory_space_constraint(second_acts, pltpu.HBM),
    )


PIECES = 4


def store_kernel(w, sim, w_hbm, s_hbm, sems):
    step = HEADS // PIECES
    copies = [
        pltpu.make_async_copy(
            w.at[n, pl.ds(q * step, step)], w_hbm.at[n, 0, pl.ds(q * step, step)], sems.at[n * PIECES + q]
        )
        for n in range(2)
        for q in range(PIECES)
    ]
    copies.append(pltpu.make_async_copy(sim, s_hbm.at[0], sems.at[2 * PIECES]))
    for copy in copies:
        copy.start()
    for copy in copies:
        copy.wait()


def store(w, sim):
    vmem, hbm = pl.BlockSpec(memory_space=pltpu.VMEM), pl.BlockSpec(memory_space=pltpu.HBM)
    return pl.pallas_call(
        store_kernel,
        out_shape=(
            jax.ShapeDtypeStruct((2, 1, HEADS, HD, HD), F32),
            jax.ShapeDtypeStruct((1, 2, HEADS), F32),
        ),
        in_specs=[vmem] * 2,
        out_specs=(hbm, hbm),
        scratch_shapes=[pltpu.SemaphoreType.DMA((2 * PIECES + 1,))],
        compiler_params=pltpu.CompilerParams(vmem_limit_bytes=16 * 2**20),
    )(w, sim)


def solution(mesh):
    def whole(first_acts, second_acts):
        tokens = first_acts.shape[1] * lax.axis_size("tok")
        return store(*gather_kernel(tokens, first_acts, second_acts))

    in_specs = (P("lay", "tok", None), P("lay", "tok", None))
    out_specs = (P(None, "lay", None, None, None), P("lay", None, None))
    return jax.shard_map(whole, mesh=mesh, in_specs=in_specs, out_specs=out_specs, check_vma=False)
```

```python
import functools

import jax
import jax.numpy as jnp
from jax import lax
from jax.experimental import pallas as pl
from jax.experimental.pallas import tpu as pltpu
from jax.sharding import PartitionSpec as P

HEADS = 40
HD = 128
ITERS = 6
RIDGE = 0.05
HALF = HEADS // 2
PARTS = 5
FROM_HBM = 3
BATCHES = (15, 21, 32)
CARRIED = (3, 7)
VMEM_LIMIT = 48 * 2**20
F32 = jnp.float32
HI = lax.Precision.HIGHEST
MESH = pl.DeviceIdType.MESH

CHAINS = {"pa": (72, "z"), "pb": (64, "y"), "ca": (64, "z"), "cb": (64, "y")}
LATE = {"da": "z", "db": "y"}
GATHERS = {"wa": (72, "z"), "wb": (64, "y")}


def iota(shape, dim):
    return lax.broadcasted_iota(jnp.int32, shape, dim)


def dot_t(a, b, precision=None):
    return lax.dot_general(
        a, b, (((0,), (0,)), ((), ())), precision=precision, preferred_element_type=F32
    )


def mm(a, b):
    return jnp.dot(a, b, precision=HI, preferred_element_type=F32)


def masks():
    ri, ci = iota((HD, HD), 0), iota((HD, HD), 1)
    return ri <= ci, ri == ci


def unpack(top, low, aux):
    upper, diag = masks()
    p = jnp.concatenate([top, low], axis=0)
    pt = p.T
    first = jnp.where(upper, p, pt)
    second = jnp.where(upper, jnp.where(diag, aux[2:3, :], pt), p)
    return first, second


def fold(w):
    row, lane = iota((64, HD), 0), iota((64, HD), 1)
    lower = jnp.logical_and(lane < 64, row > lane)
    return jnp.where(lower, pltpu.roll(w[64:], 64, 1), w[:64])


def unfold(folded, diagonal):
    row, lane = iota((HD, HD), 0), iota((HD, HD), 1)
    q = jnp.concatenate([folded, pltpu.roll(folded, 64, 1)], axis=0)
    top = jnp.logical_and(row < 64, row <= lane)
    low = jnp.logical_and(lane >= 64, row > lane)
    out = jnp.where(jnp.logical_or(top, low), q, q.T)
    return jnp.where(jnp.logical_and(row == lane, row >= 64), diagonal, out)


def head_of(z, p):
    k = 4 * ((z + p) % 4) + z
    if isinstance(p, int):
        return 16 + z if p == 4 else k
    return jnp.where(p == 4, 16 + z, k)


def places(h):
    k = h % HALF
    z = k % 4
    half = h // HALF
    y = jnp.where(k < 16, k // 4, (z + 2 * half) % 4)
    p = jnp.where(k < 16, (k // 4 - z + 4) % 4, 4)
    return half, z, y, p


def kernel(tokens, names, *refs):
    r = dict(zip(names, refs))
    tok = lax.axis_index("tok")
    lay = lax.axis_index("lay")
    c = tok % 2
    xh = (tok // 2) % 2
    y = (tok // 4) % 4
    z = tok // 16

    def dev(z_, y_, xh_, c_):
        return (((z_ * 4 + y_) * 2 + xh_) * 2 + c_, lay)

    def uv(axis):
        return (z, y) if axis == "z" else (y, z)

    def dev_uv(axis, u, v, xh_):
        return dev(u, v, xh_, c) if axis == "z" else dev(v, u, xh_, c)

    sibling = dev(z, y, xh, 1 - c)
    twin = (tok, 1 - lay)
    far = dev(z, y, 1 - xh, c)

    on_diag = y == (z + 2 * c) % 4
    main = (y - z + 4) % 4
    owns_main = xh == main % 2
    owner = jnp.logical_or(owns_main, on_diag)
    own = jnp.where(owns_main, main, 4)
    late_owner = jnp.logical_and(on_diag, xh == 1)
    early_owner = owns_main
    extra_mine = jnp.where(owns_main, 0, 1)
    extra_give = jnp.where(owns_main, 1, 0)
    gives = jnp.logical_or(on_diag, jnp.logical_not(owns_main))
    no = jnp.logical_not

    def target(axis, p):
        u, _ = uv(axis)
        if p == 4:
            return (u + 2 * c) % 4
        return (u + p) % 4 if axis == "z" else (u - p + 4) % 4

    def rcopy(src, dst, ssem, rsem, device):
        return pltpu.make_async_remote_copy(
            src_ref=src, dst_ref=dst, send_sem=ssem, recv_sem=rsem,
            device_id=device, device_id_type=MESH,
        )

    others = lax.axis_size("tok") - 1
    def launch(copy, cond=None):
        if cond is None:
            copy.start()
        else:
            pl.when(cond)(lambda: copy.start())

    def left(ref, sem, cond=None):
        copy = rcopy(ref, ref, sem, r["l_s"].at[0], twin)
        if cond is None:
            copy.wait_send()
        else:
            pl.when(cond)(lambda: copy.wait_send())

    def arrive(ref, sem, cond=None):
        copy = rcopy(ref, ref, r["l_s"].at[0], sem, twin)
        if cond is None:
            copy.wait_recv()
        else:
            pl.when(cond)(lambda: copy.wait_recv())

    def loop(n, body, unroll=1):
        def step(i, carry):
            body(i)
            return carry

        lax.fori_loop(0, n, step, 0, unroll=unroll)

    def s1(name):
        launch(rcopy(r[name].at[1 - c], r[name + "_r1"], r[name + "_s"].at[0], r[name + "_q"].at[0], sibling))

    def s1_sum(name):
        buf, r1 = r[name], r[name + "_r1"]
        arrive(r1, r[name + "_q"].at[0])

        def body(i):
            for s in range(5):
                buf[c, i, s] = buf[c, i, s] + r1[i, s]

        loop(4, body)

    def s2(name, offsets=(1, 3, 2)):
        axis = CHAINS[name][1]
        u, v = uv(axis)
        for d in offsets:
            to = (u + d) % 4
            launch(
                rcopy(
                    r[name].at[c, to], r[name + "_r2"].at[d - 1], r[name + "_s"].at[1],
                    r[name + "_q"].at[1], dev_uv(axis, to, v, xh),
                )
            )

    def s2_sum(name):
        u, _ = uv(CHAINS[name][1])
        buf, r2, acc = r[name], r[name + "_r2"], r[name + "_acc"]
        arrive(r2, r[name + "_q"].at[1])
        for s in range(5):
            acc[s] = (buf[c, u, s] + r2[0, s]) + (r2[1, s] + r2[2, s])

    def s3(name, axis, slots):
        u, v = uv(axis)
        for p in slots:
            vo = target(axis, p)
            off = jnp.maximum((v - vo + 4) % 4, 1) - 1
            kind = p // 4
            launch(
                rcopy(
                    r[name + "_acc"].at[p], r[name + "_r3"].at[kind, off], r[name + "_s"].at[2],
                    r[name + "_q"].at[2 + kind], dev_uv(axis, u, vo, xh),
                ),
                v != vo,
            )

    def s3_sum(name, extra):
        acc, r3, part = r[name + "_acc"], r[name + "_r3"], r[name + "_t"]

        def add(kind, slot):
            arrive(r3.at[kind], r[name + "_q"].at[2 + kind])
            part[kind] = (acc[slot] + r3[kind, 0]) + (r3[kind, 1] + r3[kind, 2])

        add(0, main)
        if extra:
            pl.when(on_diag)(lambda: add(1, 4))

    def s4(name, extra):
        src = r[name + "_t"].at[extra_give] if extra else r[name + "_t"].at[0]
        cond = gives if extra else no(owns_main)
        launch(rcopy(src, r[name + "_r4"], r[name + "_s"].at[3], r[name + "_q"].at[4], far), cond)

    def s4_total(name, extra):
        arrive(r[name + "_r4"], r[name + "_q"].at[4])
        mine = r[name + "_t"][extra_mine] if extra else r[name + "_t"][0]
        return mine + r[name + "_r4"][...]

    def chain_left(name):
        acc = r[name + "_acc"]
        left(r[name + "_r1"], r[name + "_s"].at[0])
        left(r[name + "_r2"], r[name + "_s"].at[1])
        left(acc.at[pl.ds(0, 3)], r[name + "_s"].at[2], on_diag)
        left(acc.at[pl.ds(0, 4)], r[name + "_s"].at[2], no(on_diag))

    def given(name, cond):
        left(r[name + "_r4"], r[name + "_s"].at[3], cond)

    def g1(name):
        u, _ = uv(GATHERS[name][1])
        place = r[name].at[c, u, own]
        rcopy(place, place, r[name + "_s"].at[0], r[name + "_q"].at[0], far).start()

    def g1_arrive(name):
        u, _ = uv(GATHERS[name][1])
        arrive(r[name].at[c, u, jnp.where(owns_main, 4, main)], r[name + "_q"].at[0], gives)

    def g2(name):
        axis = GATHERS[name][1]
        u, v = uv(axis)
        for d in (1, 3, 2):
            for kind in (0, 1):
                slot = 4 if kind else main
                place = r[name].at[c, u, slot]
                launch(
                    rcopy(
                        place, place, r[name + "_s"].at[1], r[name + "_q"].at[1],
                        dev_uv(axis, u, (v + d) % 4, xh),
                    ),
                    on_diag if kind else None,
                )

    def g2_arrive(name):
        u, _ = uv(GATHERS[name][1])
        arrive(r[name].at[c, u, pl.ds(0, 3)], r[name + "_q"].at[1], on_diag)
        arrive(r[name].at[c, u, pl.ds(0, 4)], r[name + "_q"].at[1], no(on_diag))

    def g3(name):
        axis = GATHERS[name][1]
        u, v = uv(axis)
        place = r[name].at[c, u]
        for d in (1, 3, 2):
            launch(
                rcopy(
                    place, place, r[name + "_s"].at[2], r[name + "_q"].at[2],
                    dev_uv(axis, (u + d) % 4, v, xh),
                )
            )

    def g3_arrive(name):
        arrive(r[name].at[c, pl.ds(0, 3)], r[name + "_q"].at[2])

    def g4(name):
        place = r[name].at[c]
        launch(rcopy(place, place, r[name + "_s"].at[3], r[name + "_q"].at[3], sibling))

    def g4_arrive(name):
        arrive(r[name].at[1 - c], r[name + "_q"].at[3])

    def gather_left(name):
        buf, sems = r[name], r[name + "_s"]
        left(buf.at[c, 0, 0], sems.at[0], owner)
        left(buf.at[c, pl.ds(0, 2), pl.ds(0, 3)], sems.at[1], on_diag)
        left(buf.at[c, 0, pl.ds(0, 3)], sems.at[1], no(on_diag))
        left(buf.at[c, pl.ds(0, 3)], sems.at[2])
        left(buf.at[c], sems.at[3])

    x1, x2, x2o = r["x1"], r["x2"], r["x2o"]

    def part_head(p, j):
        half = (1 - c) if j < 4 else c
        return half, j % 4, half * HALF + head_of(j % 4, p)

    own_last = jnp.where(c == 0, z, (y + 2) % 4)

    def last_head(z_, c_):
        return c_ * HALF + 16 + z_

    def columns(h):
        return pl.ds(pl.multiple_of(h * HD, HD), HD)

    def exchange(lo, hi):
        for n in range(lo, hi):
            p, j = n // 8, n % 8
            _, _, h = part_head(p, j)
            src = r["x2_hbm"].at[0, :, columns(h)] if n < FROM_HBM else x2.at[:, columns(h)]
            if p == 4:
                src = x2.at[:, columns(last_head(own_last, c))] if j == 0 else r["m2"].at[j - 1]
            sem = 2 * p + j // 4
            copy = rcopy(src, x2o.at[p, j], r["x_s"].at[p // 4], r["x_q"].at[sem], twin)
            if p == 4 and j in CARRIED:
                pl.when(c == 1)(lambda copy=copy: copy.start())
            else:
                copy.start()
            if n == 8 * PARTS - 5:
                for i, k in enumerate(CARRIED):
                    launch(
                        rcopy(
                            r["m3"].at[i], x2o.at[4, k], r["x_s"].at[1], r["x_q"].at[8 + k // 4],
                            (jnp.maximum(tok, 1) - 1, 1 - lay),
                        ),
                        c == 1,
                    )

    def collect():
        for d in (1, 3, 2, 0):
            for c_ in (0, 1):
                if c_ == 0:
                    w_, to, other = (z + d) % 4, dev((z + d) % 4, y, xh, 0), c
                else:
                    w_, to, other = (y + d + 2) % 4, dev(z, (y + d) % 4, xh, 1), 1 - c
                slot = jnp.maximum(2 * d + other, 1) - 1
                cols = columns(last_head(w_, c_))
                for n, x in ((1, x2), (0, x1)):
                    cond = None if d else other == 1
                    carried = n == 1 and c_ == 0 and 2 * d + 1 in CARRIED
                    if carried:
                        i = CARRIED.index(2 * d + 1)
                        launch(
                            rcopy(
                                x.at[:, cols], r["m3"].at[i], r["m_s"].at[1], r["m_q"].at[2],
                                dev(w_, y, xh, 1),
                            ),
                            c == 1,
                        )
                        cond = c == 0
                    launch(
                        rcopy(
                            x.at[:, cols], r["m%d" % (n + 1)].at[slot], r["m_s"].at[n],
                            r["m_q"].at[n], to,
                        ),
                        cond,
                    )

    def collected(n):
        if n == 0:
            arrive(r["m1"], r["m_q"].at[0])
        else:
            arrive(r["m2"], r["m_q"].at[1], c == 1)
            arrive(r["m2"].at[pl.ds(0, 7 - len(CARRIED))], r["m_q"].at[1], c == 0)
            arrive(r["m3"], r["m_q"].at[2], c == 1)

    def last_cross(which):
        arrive(x2o.at[4, pl.ds(4 * which, 4)], r["x_q"].at[8 + which])
        total = None
        for j in range(4 * which, 4 * which + 4):
            left = r["m1"][j - 1] if j else x1[:, columns(last_head(own_last, c))]
            cr = dot_t(left, x2o[4, j])
            total = cr if total is None else total + cr
        r["d4"][...] = r["d4"][...] + total if which else total

    def exchange_left(last):
        if last:
            left(x2o.at[pl.ds(0, 2), pl.ds(0, 5)], r["x_s"].at[1], c == 1)
            left(x2o.at[0, pl.ds(0, 6)], r["x_s"].at[1], c == 0)
        else:
            left(x2o.at[pl.ds(0, 4)], r["x_s"].at[0])

    load1 = pltpu.make_async_copy(r["x1_hbm"].at[0], x1, r["l_s"].at[0])
    load2 = pltpu.make_async_copy(r["x2_hbm"].at[0], x2, r["l_s"].at[1])
    load2.start()
    load1.start()
    barrier = pltpu.get_barrier_semaphore()
    peers = [sibling, twin, far]
    for d in range(1, 4):
        for c_ in (c, 1 - c):
            peers.append(dev((z + d) % 4, y, xh, c_))
            peers.append(dev(z, (y + d) % 4, xh, c_))
    for peer in peers:
        pl.semaphore_signal(barrier, inc=1, device_id=peer, device_id_type=MESH)
    pl.semaphore_wait(barrier, len(peers))
    exchange(0, FROM_HBM)
    load2.wait()
    exchange(FROM_HBM, BATCHES[0])
    load1.wait()
    collect()

    upper, diag = masks()
    eye = jnp.where(diag, 1.0, 0.0).astype(F32)
    row8 = iota((8, HD), 0)

    def gram(h):
        ch, zz, yy, p = places(h)
        cols = columns(h)
        ab = jnp.concatenate([x1[:, cols], x2[:, cols]], axis=1)
        g = dot_t(ab, ab)
        sums = jnp.dot(jnp.ones((8, ab.shape[0]), ab.dtype), ab, preferred_element_type=F32)
        g1_, cr, g2_ = g[:HD, :HD], g[:HD, HD:], g[HD:, HD:]
        packed = jnp.where(upper, g1_, g2_)
        dg = jnp.sum(jnp.where(diag, g2_, 0.0), axis=0, keepdims=True)
        aux = jnp.where(
            row8 == 0, sums[:, :HD],
            jnp.where(row8 == 1, sums[:, HD:], jnp.where(row8 == 2, jnp.broadcast_to(dg, (8, HD)), 0.0)),
        )
        r["pa"][ch, zz, p, 0:64] = packed[:64]
        r["pa"][ch, zz, p, 64:72] = aux
        r["pb"][ch, yy, p] = packed[64:]
        r["ca"][ch, zz, p] = cr[:64]
        r["cb"][ch, yy, p] = cr[64:]

    def cross(p, which):
        arrive(x2o.at[p, pl.ds(4 * which, 4)], r["x_q"].at[2 * p + which])
        for j in range(4 * which, 4 * which + 4):
            half, zz, h = part_head(p, j)
            yy = (zz + p) % 4
            cr = dot_t(x1[:, columns(h)], x2o[p, j])
            r["da"][p, half, zz] = cr[:64]
            r["db"][p, half, yy] = cr[64:]
            if j == 3:
                for name in LATE:
                    launch(
                        rcopy(
                            r[name].at[p, 1 - c], r[name + "_r1"].at[p], r["late_s"].at[0],
                            r["late_q"].at[p], sibling,
                        )
                    )

    def cross_s2(p):
        arrive(r["da_r1"].at[pl.ds(0, 2)], r["late_q"].at[p])
        for name, axis in LATE.items():
            buf, r1 = r[name], r[name + "_r1"]
            u, v = uv(axis)
            for i in range(4):
                buf[p, c, i] = buf[p, c, i] + r1[p, i]
            for d in (1, 3, 2):
                to = (u + d) % 4
                launch(
                    rcopy(
                        buf.at[p, c, to], r[name + "_r2"].at[p, d - 1], r["late_s"].at[1],
                        r["late_q"].at[4 + p], dev_uv(axis, to, v, xh),
                    )
                )

    def cross_s2_sum(p):
        arrive(r["da_r2"].at[pl.ds(0, 2)], r["late_q"].at[4 + p])
        for name, axis in LATE.items():
            buf, r2 = r[name], r[name + "_r2"]
            u, _ = uv(axis)
            r[name + "x_acc"][p] = (buf[p, c, u] + r2[p, 0]) + (r2[p, 1] + r2[p, 2])

    def last_s3():
        away = jnp.where(c == 0, y - z + 4, z - own_last + 4) % 4
        slot = jnp.maximum(away * 2 + 1 - xh, 1)
        launch(
            rcopy(
                r["d4"], r["r5"].at[slot - 1], r["d4_s"].at[0], r["d4_q"].at[0],
                dev(own_last, (own_last + 2 * c) % 4, 1, c),
            ),
            no(late_owner),
        )

    def last_total():
        arrive(r["r5"], r["d4_q"].at[0])
        total = r["d4"][...] + r["r5"][0]
        for slot in range(1, 7):
            total = total + r["r5"][slot]
        return total

    def only_row0(row):
        return jnp.where(row8 == 0, jnp.broadcast_to(row, (8, HD)), 0.0)

    def mean_term(sums):
        mean1 = only_row0(r["aux"][0:1, :]) / tokens
        return dot_t(mean1, only_row0(sums) / tokens, HI)

    def similarity(raw, means, w2):
        white = mm(mm(r["w12"][0], raw / tokens - means), w2)
        sq = jnp.sum(jnp.sum(white * white, axis=1, keepdims=True), axis=0, keepdims=True)
        return jnp.broadcast_to(sq / HD, (1, HD))

    def whiten():
        top = s4_total("pa", True)
        low = s4_total("pb", True)
        aux = top[64:72]
        grams = unpack(top[:64], low, aux)
        ys, zs, scales = [], [], []
        for n in (0, 1):
            mean = only_row0(aux[n : n + 1, :]) / tokens
            cov = grams[n] / tokens - dot_t(mean, mean, HI) + RIDGE * eye
            sq = jnp.sum(jnp.sum(cov * cov, axis=1, keepdims=True), axis=0, keepdims=True)
            scale = jnp.sqrt(sq)
            scales.append(scale)
            ys.append(cov / scale)
        for it in range(ITERS):
            for n in (0, 1):
                if it == 0:
                    f = 1.5 * eye - 0.5 * ys[n]
                    zs.append(f)
                else:
                    f = 1.5 * eye - 0.5 * mm(zs[n], ys[n])
                    zs[n] = mm(f, zs[n])
                if it < ITERS - 1:
                    ys[n] = mm(ys[n], f)
        w1 = zs[0] / jnp.sqrt(scales[0])
        w2 = zs[1] / jnp.sqrt(scales[1])
        wp = jnp.where(upper, w1, w2)
        wd = jnp.sum(jnp.where(diag, w2, 0.0), axis=0, keepdims=True)
        r["wa"][c, z, own, 0:64] = wp[:64]
        r["wa"][c, z, own, 64:72] = jnp.broadcast_to(wd, (8, HD))
        r["wb"][c, y, own] = wp[64:]
        g1("wa")
        g1("wb")
        r["w12"][0] = w1
        r["w12"][1] = w2
        r["aux"][...] = aux
        r["w_out_x"][0:64] = fold(w2)
        r["w_out_x"][64:72] = jnp.where(row8 == 2, jnp.broadcast_to(wd, (8, HD)), aux)
    def both(p):
        cross(p, 0)
        cross(p, 1)

    loop(HALF, lambda i: gram((1 - c) * HALF + i), unroll=2)
    for name in CHAINS:
        s1(name)
    loop(HALF, lambda i: gram(c * HALF + i), unroll=2)
    for name in ("pa", "pb"):
        s1_sum(name)
        s2(name)
    for name in ("ca", "cb"):
        s1_sum(name)
    both(0)
    for name in ("pa", "pb"):
        s2_sum(name)
        s3(name, CHAINS[name][1], range(5))
    for name in ("pa", "pb"):
        s3_sum(name, True)
        s4(name, True)
    exchange(BATCHES[0], BATCHES[1])
    for name in ("ca", "cb"):
        s2(name)
    cross_s2(0)
    pl.when(owner)(whiten)
    exchange(BATCHES[1], BATCHES[2])
    for name in GATHERS:
        g1_arrive(name)
        g2(name)
    both(1)
    cross_s2(1)
    for name in ("ca", "cb"):
        s2_sum(name)
        s3(name, CHAINS[name][1], range(5))
    for name in GATHERS:
        g2_arrive(name)
        g3(name)
    collected(1)
    exchange(BATCHES[2], 8 * PARTS)

    @pl.when(owner)
    def _():
        rcopy(r["w_out_x"], r["w_in_x"], r["y_s"].at[0], r["y_q"].at[0], twin).start()

    both(2)
    cross_s2(2)
    cross_s2_sum(0)
    cross_s2_sum(1)

    lane_head = c * HALF + jnp.where(own == 4, 16 + z, head_of(z, own))
    lanes = iota((1, HD), 1)
    sa_mine = r["sa"].at[(c * 4 + z) * 5 + own]

    def own_similarity():
        raw = jnp.concatenate([s4_total("ca", True), s4_total("cb", True)], axis=0)
        sim = similarity(raw, mean_term(r["aux"][1:2, :]), r["w12"][1])
        sa_mine[...] = jnp.where(lanes == 64 * lay + lane_head, sim, 0.0)
        arrive(r["w_in_x"], r["y_q"].at[0])
        r["means"][...] = mean_term(r["w_in_x"][65:66])
        r["w2_other"][...] = unfold(r["w_in_x"][0:64], r["w_in_x"][66:67])

    def other_similarity(raw):
        sim = similarity(raw, r["means"][...], r["w2_other"][...])
        sa_mine[...] = jnp.where(lanes == 64 * (1 - lay) + lane_head, sim, sa_mine[...])
        steps = (2, 1, 3, 0)
        z_at = [(z + d) % 4 * 16 for d in range(4)]
        y_at = [(y + d) % 4 * 4 for d in range(4)]
        x_at = [(xh + d) % 2 * 2 for d in range(2)]
        c_at = [(c + d) % 2 for d in range(2)]
        for dx in (1, 0):
            for dz in steps:
                for dy in steps:
                    for dc in (1, 0):
                        if dx or dz or dy or dc:
                            to = z_at[dz] + y_at[dy] + (x_at[dx] + c_at[dc])
                            rcopy(sa_mine, sa_mine, r["sa_s"].at[0], r["sa_q"].at[0], (to, lay)).start()

    def emit(h):
        ch, zz, yy, p = places(h)
        w1, w2 = unpack(r["wa"][ch, zz, p, 0:64], r["wb"][ch, yy, p], r["wa"][ch, zz, p, 64:72])
        r["w"][0, h] = w1
        r["w"][1, h] = w2

    both(3)
    for name in GATHERS:
        g3_arrive(name)
        g4(name)
    cross_s2(3)
    cross_s2_sum(2)
    for name, axis in LATE.items():
        s3(name + "x", axis, range(3))
    for name in ("ca", "cb"):
        s3_sum(name, True)
    for name in ("ca", "cb"):
        s4(name, True)
    cross_s2_sum(3)
    for name, axis in LATE.items():
        s3(name + "x", axis, (3,))
    for name in GATHERS:
        g4_arrive(name)
    loop(HALF, emit, unroll=2)
    collected(0)
    for name in CHAINS:
        chain_left(name)
    for name in ("pa", "pb"):
        given(name, gives)
    for name in GATHERS:
        gather_left(name)
    for n in (0, 1):
        left(r["m1"], r["m_s"].at[n])
    left(r["da"], r["late_s"].at[0])
    left(r["da"].at[pl.ds(0, 3)], r["late_s"].at[1])
    exchange_left(False)
    last_cross(0)
    last_cross(1)
    last_s3()
    for name in LATE:
        s3_sum(name + "x", False)
        s4(name + "x", False)
    loop(HALF, lambda i: emit(HALF + i), unroll=2)
    pl.when(owner)(own_similarity)

    @pl.when(early_owner)
    def _():
        other_similarity(jnp.concatenate([s4_total("dax", False), s4_total("dbx", False)], axis=0))

    @pl.when(late_owner)
    def _():
        other_similarity(last_total())

    pl.when(owner)(lambda: arrive(r["sa"].at[pl.ds(0, HEADS - 1)], r["sa_q"].at[0]))
    pl.when(no(owner))(lambda: arrive(r["sa"].at[pl.ds(0, HEADS)], r["sa_q"].at[0]))
    total = r["sa"][0]
    for i in range(1, HEADS):
        total = total + r["sa"][i]
    r["sim"][0:1, :] = total[:, 0:HEADS]
    r["sim"][1:2, :] = total[:, 64 : 64 + HEADS]

    exchange_left(True)
    for name in ("ca", "cb"):
        given(name, gives)
    for name in LATE:
        left(r[name + "x_acc"].at[pl.ds(0, 3)], r[name + "x_s"].at[2])
        given(name + "x", no(owns_main))
    left(r["d4"], r["d4_s"].at[0], no(late_owner))
    left(r["w_out_x"], r["y_s"].at[0], owner)
    left(r["sa"].at[pl.ds(0, others)], r["sa_s"].at[0], owner)


def gather_kernel(tokens, first_acts, second_acts):
    rows, width = first_acts.shape[1:]
    names = ["x1_hbm", "x2_hbm", "w", "sim"]
    scratch = []

    def add(name, spec):
        names.append(name)
        scratch.append(spec)

    dma = lambda n: pltpu.SemaphoreType.DMA((n,))
    for name in ("x1", "x2"):
        add(name, pltpu.VMEM((rows, width), first_acts.dtype))
    add("x2o", pltpu.VMEM((PARTS, 8, rows, HD), first_acts.dtype))
    for name, (n, _) in CHAINS.items():
        add(name, pltpu.VMEM((2, 4, 5, n, HD), F32))
        add(name + "_r1", pltpu.VMEM((4, 5, n, HD), F32))
        add(name + "_r2", pltpu.VMEM((3, 5, n, HD), F32))
    for name in LATE:
        add(name, pltpu.VMEM((PARTS - 1, 2, 4, 64, HD), F32))
        add(name + "_r1", pltpu.VMEM((PARTS - 1, 4, 64, HD), F32))
        add(name + "_r2", pltpu.VMEM((PARTS - 1, 3, 64, HD), F32))
    add("late_s", dma(2))
    add("late_q", dma(8))
    for name in ("m1", "m2"):
        add(name, pltpu.VMEM((7, rows, HD), first_acts.dtype))
    add("m3", pltpu.VMEM((2, rows, HD), first_acts.dtype))
    add("m_s", dma(2))
    add("m_q", dma(3))
    add("d4", pltpu.VMEM((HD, HD), F32))
    add("r5", pltpu.VMEM((7, HD, HD), F32))
    add("d4_s", dma(1))
    add("d4_q", dma(1))
    add("means", pltpu.VMEM((HD, HD), F32))
    for name, n in [(k, v[0]) for k, v in CHAINS.items()] + [(k + "x", 64) for k in LATE]:
        add(name + "_acc", pltpu.VMEM((5, n, HD), F32))
        add(name + "_r3", pltpu.VMEM((2, 3, n, HD), F32))
        add(name + "_t", pltpu.VMEM((2, n, HD), F32))
        add(name + "_r4", pltpu.VMEM((n, HD), F32))
        add(name + "_s", dma(4))
        add(name + "_q", dma(5))
    add("sa", pltpu.VMEM((64, 1, HD), F32))
    for name, (n, _) in GATHERS.items():
        add(name, pltpu.VMEM((2, 4, 5, n, HD), F32))
        add(name + "_s", dma(4))
        add(name + "_q", dma(4))
    add("sa_s", dma(1))
    add("sa_q", dma(1))
    add("w12", pltpu.VMEM((2, HD, HD), F32))
    add("aux", pltpu.VMEM((8, HD), F32))
    add("w_out_x", pltpu.VMEM((72, HD), F32))
    add("w_in_x", pltpu.VMEM((72, HD), F32))
    add("w2_other", pltpu.VMEM((HD, HD), F32))
    add("l_s", dma(2))
    add("x_s", dma(2))
    add("x_q", dma(2 * PARTS))
    add("y_s", dma(1))
    add("y_q", dma(1))
    return pl.pallas_call(
        functools.partial(kernel, tokens, names),
        out_shape=(
            pltpu.VMEM((2, HEADS, HD, HD), F32),
            pltpu.VMEM((2, HEADS), F32),
        ),
        in_specs=[pl.BlockSpec(memory_space=pltpu.HBM)] * 2,
        out_specs=[pl.BlockSpec(memory_space=pltpu.VMEM)] * 2,
        scratch_shapes=scratch,
        compiler_params=pltpu.CompilerParams(
            collective_id=0, has_side_effects=True, vmem_limit_bytes=VMEM_LIMIT
        ),
    )(
        pltpu.with_memory_space_constraint(first_acts, pltpu.HBM),
        pltpu.with_memory_space_constraint(second_acts, pltpu.HBM),
    )


PIECES = 1


def store_kernel(w, sim, w_hbm, s_hbm, sems):
    step = HEADS // PIECES
    copies = [
        pltpu.make_async_copy(
            w.at[n, pl.ds(q * step, step)], w_hbm.at[n, 0, pl.ds(q * step, step)], sems.at[n * PIECES + q]
        )
        for n in range(2)
        for q in range(PIECES)
    ]
    copies.append(pltpu.make_async_copy(sim, s_hbm.at[0], sems.at[2 * PIECES]))
    for copy in copies:
        copy.start()
    for copy in copies:
        copy.wait()


def store(w, sim):
    vmem, hbm = pl.BlockSpec(memory_space=pltpu.VMEM), pl.BlockSpec(memory_space=pltpu.HBM)
    return pl.pallas_call(
        store_kernel,
        out_shape=(
            jax.ShapeDtypeStruct((2, 1, HEADS, HD, HD), F32),
            jax.ShapeDtypeStruct((1, 2, HEADS), F32),
        ),
        in_specs=[vmem] * 2,
        out_specs=(hbm, hbm),
        scratch_shapes=[pltpu.SemaphoreType.DMA((2 * PIECES + 1,))],
        compiler_params=pltpu.CompilerParams(vmem_limit_bytes=16 * 2**20),
    )(w, sim)


def solution(mesh):
    def whole(first_acts, second_acts):
        tokens = first_acts.shape[1] * lax.axis_size("tok")
        return store(*gather_kernel(tokens, first_acts, second_acts))

    in_specs = (P("lay", "tok", None), P("lay", "tok", None))
    out_specs = (P(None, "lay", None, None, None), P("lay", None, None))
    return jax.shard_map(whole, mesh=mesh, in_specs=in_specs, out_specs=out_specs, check_vma=False)
```
